32 devices in a mesh: dp: 4 (over x, core), tm: 2 (over y), height: 4 (over z).
Axes of the slice: x: 2, y: 2, z: 4, core: 2. Of those that a mesh axis runs over, the one named last changes fastest.
Arguments:
- latent: bfloat16 [16, 8, 16, 512], P(('dp', 'tm'), None, None, 'height'), parts along dimension 0, may hold values from -6 to 6
- gain_latent: float32 [512], P('height'), may hold values from 0.25 to 1.75
- shift_latent: float32 [512], P('height'), may hold values from -3 to 3
- conv_latent: bfloat16 [13824, 512], P('tm', 'height'), may hold values from -0.0546875 to 0.0546875
- up_weight: bfloat16 [512, 2048], P('height'), may hold values from -0.25 to 0.25
- gain_block: float32 [256], replicated, may hold values from 0.25 to 1.75
- shift_block: float32 [256], replicated, may hold values from -3 to 3
- conv_block: bfloat16 [6912, 256], P(('tm', 'height')), may hold values from -0.078125 to 0.078125
- cotangent: bfloat16 [32, 16, 32, 256], P(('dp', 'tm'), 'height'), parts along dimension 0, may hold values from -6 to 6
Outputs:
- decoded: bfloat16 [32, 16, 32, 256], P(('dp', 'tm'), 'height'), parts along dimension 0
- grad_upsampled: bfloat16 [32, 16, 32, 256], P(('dp', 'tm'), 'height'), parts along dimension 0
- grad_weight: float32 [9216, 256], P(('dp', 'tm', 'height')), parts along dimension 0
- grad_gain: float32 [1024], P('dp'), parts along dimension 0
- grad_shift: float32 [1024], P('dp'), parts along dimension 0
The draws below stay inside these ranges and needn't reach their ends.
There are 4 independent parts, one for each index of `dp`. The reference program is written for one: setup_inputs(seed, part) draws one part's arguments, and reference() takes and returns one part's arrays. A program takes and returns all parts, laid end to end along the dimension named above; an argument that names none is the same for every part. Nothing has to cross between parts.
All inputs are finite; a program needn't handle non-finite values.
Results may differ from the reference program's by a relative error of at most 0.009.
Values may be sent and summed in bfloat16 or wider, within the bound.
A program may use at most 128 MiB of HBM per device.

```python
import jax
import jax.numpy as jnp
from jax import lax

C1 = 512
C2 = 256
GROUPS = 32
W1 = 16
H1 = 8
FRAMES = 4
FRAMES_UP = 8
ROWS_UP = 16
COLS_UP = 32
N_TM = 2
N_HEIGHT = 4


def level_of(rng, shape, pieces, least, high):
    gain = 1.0
    for position, shards_of in pieces:
        steps = jax.random.uniform(jax.random.fold_in(jax.random.fold_in(rng, 6), position), (shards_of,), jnp.float32, least / len(pieces), high / len(pieces))
        gain = gain * jnp.repeat(jnp.exp(steps), shape[position] // shards_of).reshape((-1,) + (1,) * (len(shape) - 1 - position))
    return gain


def noise(own_key, shape, scale, bound, split=(), kind=jnp.bfloat16):
    array = scale * jax.random.normal(own_key, shape, jnp.float32)
    if split:
        array = array * level_of(own_key, shape, split, -0.22, 0.18)
    return jnp.clip(array, -bound, bound).astype(kind)


def setup_inputs(seed: int = 0, part: int = 0) -> dict:
    streams_of = jax.random.split(jax.random.key(seed), 10)
    part_keys = jax.random.split(jax.random.fold_in(streams_of[9], part), 10)
    return {
        "latent": noise(part_keys[0], (FRAMES, H1, W1, C1), 1.0, 6.0, ((0, 2), (3, 4))),
        "gain_latent": jnp.clip(1.0 + 0.15 * jax.random.normal(streams_of[1], (C1,), jnp.float32), 0.25, 1.75),
        "shift_latent": noise(streams_of[2], (C1,), 0.5, 3.0, ((0, 4),), jnp.float32),
        "conv_latent": noise(streams_of[3], (27 * C1, C1), (27 * C1) ** -0.5, 0.0546875, ((0, 2), (1, 4))),
        "up_weight": noise(streams_of[4], (C1, 8 * C2), C1 ** -0.5, 0.25, ((0, 4),)),
        "gain_block": jnp.clip(1.0 + 0.15 * jax.random.normal(streams_of[5], (C2,), jnp.float32), 0.25, 1.75),
        "shift_block": noise(streams_of[6], (C2,), 0.5, 3.0, (), jnp.float32),
        "conv_block": noise(streams_of[7], (27 * C2, C2), (27 * C2) ** -0.5, 0.078125, ((0, 8),)),
        "cotangent": noise(part_keys[8], (FRAMES_UP, ROWS_UP, COLS_UP, C2), 1.0, 6.0, ((0, 2), (1, 4))),
    }


epsilon = 1e-06

def moments(values, groups):
    grouped = values.reshape(-1, groups, values.shape[-1] // groups)
    count_cells = grouped.shape[0] * grouped.shape[2]
    mean_value = lax.optimization_barrier(jnp.sum(grouped, axis=(0, 2))) / count_cells
    mean_square = lax.optimization_barrier(jnp.sum(grouped * grouped, axis=(0, 2))) / count_cells
    inverse = lax.rsqrt(mean_square - mean_value * mean_value + epsilon)
    return (mean_value, inverse)

def standardize(values, mean_value, inverse, groups):
    shape_full = values.shape
    grouped = values.reshape(shape_full[:-1] + (groups, shape_full[-1] // groups))
    return ((grouped - mean_value[:, None]) * inverse[:, None]).reshape(shape_full)

def causal_taps(padded, weight, frames, rows, cols):
    channels_in = padded.shape[-1]
    summed = jnp.zeros((frames * rows * cols, weight.shape[1]), jnp.float32)
    for lag_step in range(3):
        for row_step in range(3):
            for col_step in range(3):
                tap_index = (lag_step * 3 + row_step) * 3 + col_step
                window = padded[lag_step:lag_step + frames, row_step:row_step + rows, col_step:col_step + cols]
                kernel = weight[tap_index * channels_in:(tap_index + 1) * channels_in]
                summed = summed + jnp.dot(window.reshape(-1, channels_in), kernel, preferred_element_type=jnp.float32)
    return summed.reshape(frames, rows, cols, weight.shape[1])

def transposed_taps(padded, weight, frames, rows, cols):
    channels_out = padded.shape[-1]
    channels_in = weight.shape[0] // 27
    summed = jnp.zeros((frames * rows * cols, channels_in), jnp.float32)
    for lag_step in range(3):
        for row_step in range(3):
            for col_step in range(3):
                tap_index = (lag_step * 3 + row_step) * 3 + col_step
                window = padded[2 - lag_step:2 - lag_step + frames, 2 - row_step:2 - row_step + rows, 2 - col_step:2 - col_step + cols]
                kernel = weight[tap_index * channels_in:(tap_index + 1) * channels_in]
                summed = summed + lax.dot_general(window.reshape(-1, channels_out), kernel, (((1,), (1,)), ((), ())), preferred_element_type=jnp.float32)
    return summed.reshape(frames, rows, cols, channels_in)

def weight_terms(padded, grads, frames, rows, cols):
    channels_in = padded.shape[-1]
    flat_grads = grads.reshape(-1, grads.shape[-1])
    blocks = []
    for row_step in range(3):
        for col_step in range(3):
            window = padded[2:2 + frames, row_step:row_step + rows, col_step:col_step + cols]
            blocks.append(lax.dot_general(window.reshape(-1, channels_in), flat_grads, (((0,), (0,)), ((), ())), preferred_element_type=jnp.float32))
    return jnp.concatenate(blocks, 0)

def reference(latent, gain_latent, shift_latent, conv_latent, up_weight, gain_block, shift_block, conv_block, cotangent):
    latent_f32 = latent.astype(jnp.float32)
    mean_latent, inverse_latent = moments(latent_f32, GROUPS)
    normed = standardize(latent_f32, mean_latent, inverse_latent, GROUPS) * gain_latent + shift_latent
    active = jax.nn.silu(normed).astype(jnp.bfloat16)
    frames_latent, rows_latent, cols_latent = (latent.shape[0], latent.shape[1], latent.shape[2])
    padded = jnp.pad(active, ((2, 0), (1, 1), (1, 1), (0, 0)))
    mixed = causal_taps(padded, conv_latent, frames_latent, rows_latent, cols_latent)
    refined = (latent_f32 + mixed).astype(jnp.bfloat16)
    expanded = jnp.dot(refined.reshape(-1, C1), up_weight, preferred_element_type=jnp.float32)
    spread = expanded.reshape(frames_latent, rows_latent, cols_latent, 2, 2, 2, C2)
    spread = spread.transpose(0, 3, 1, 4, 2, 5, 6)
    upsampled = spread.reshape(2 * frames_latent, 2 * rows_latent, 2 * cols_latent, C2).astype(jnp.bfloat16)
    frames_block, rows_block, cols_block = (upsampled.shape[0], upsampled.shape[1], upsampled.shape[2])
    up_f32 = upsampled.astype(jnp.float32)
    mean_block, inverse_block = moments(up_f32, GROUPS)
    standard = standardize(up_f32, mean_block, inverse_block, GROUPS)
    normed_block = standard * gain_block + shift_block
    active_block = jax.nn.silu(normed_block).astype(jnp.bfloat16)
    padded_block = jnp.pad(active_block, ((2, 0), (1, 1), (1, 1), (0, 0)))
    mixed_block = causal_taps(padded_block, conv_block, frames_block, rows_block, cols_block)
    decoded = (up_f32 + mixed_block).astype(jnp.bfloat16)
    grad_padded = jnp.pad(cotangent, ((0, 2), (1, 1), (1, 1), (0, 0)))
    grad_active = transposed_taps(grad_padded, conv_block, frames_block, rows_block, cols_block)
    frames_dev = frames_block // N_TM
    rows_dev = rows_block // N_HEIGHT
    zero_index = jnp.zeros((), jnp.int32)

    def add_device(carried, device):
        time_start = device // N_HEIGHT * frames_dev
        row_start = device % N_HEIGHT * rows_dev
        region = lax.dynamic_slice(padded_block, (time_start, row_start, zero_index, zero_index), (frames_dev + 2, rows_dev + 2, cols_block + 2, C2))
        grads = lax.dynamic_slice(cotangent, (time_start, row_start, zero_index, zero_index), (frames_dev, rows_dev, cols_block, C2))
        term = weight_terms(region, grads, frames_dev, rows_dev, cols_block)
        return (carried + term, None)
    grad_weight, unused = lax.scan(add_device, jnp.zeros((9 * C2, C2), jnp.float32), jnp.arange(N_TM * N_HEIGHT, dtype=jnp.int32))
    sigmoid = jax.nn.sigmoid(normed_block)
    grad_normed = grad_active * sigmoid * (1.0 + normed_block * (1.0 - sigmoid))
    flat_grad = grad_normed.reshape(-1, C2)
    flat_standard = standard.reshape(-1, C2)
    grad_shift = lax.optimization_barrier(jnp.sum(flat_grad, axis=0))
    grad_gain = lax.optimization_barrier(jnp.sum(flat_grad * flat_standard, axis=0))
    per_block = C2 // GROUPS
    count_block = flat_grad.shape[0] * per_block
    first_mean = lax.optimization_barrier(jnp.sum((gain_block * grad_shift).reshape(GROUPS, per_block), axis=1)) / count_block
    second_mean = lax.optimization_barrier(jnp.sum((gain_block * grad_gain).reshape(GROUPS, per_block), axis=1)) / count_block
    grouped_grad = (grad_normed * gain_block).reshape(-1, GROUPS, per_block)
    grouped_standard = standard.reshape(-1, GROUPS, per_block)
    corrected = (grouped_grad - first_mean[:, None] - grouped_standard * second_mean[:, None]) * inverse_block[:, None]
    grad_upsampled = (cotangent.astype(jnp.float32) + corrected.reshape(cotangent.shape)).astype(jnp.bfloat16)
    return (decoded, grad_upsampled, grad_weight, grad_gain, grad_shift)
```

```python
import functools

import jax
import jax.numpy as jnp
from jax import lax
from jax.experimental import pallas as pl
from jax.experimental.pallas import tpu as pltpu
from jax.sharding import PartitionSpec as P

C1 = 512
GROUPS = 32


epsilon = 1e-06


def shifted(block, axis, distance):
    devices = range(lax.axis_size(axis))
    route = [(i - distance, i) for i in devices if i - distance in devices]
    return lax.ppermute(block, axis, route)


def extended_2(cells, sides, width):
    for axis, dim in sides:
        count = lax.axis_size(axis)
        ends = count - 1
        head = lax.slice_in_dim(cells, 0, width, axis=dim)
        tail = lax.slice_in_dim(cells, cells.shape[dim] - width, cells.shape[dim], axis=dim)
        cells = jnp.concatenate(
            [
                lax.ppermute(tail, axis, [(i, (i + 1) % count) for i in range(ends)]),
                cells,
                lax.ppermute(head, axis, [((i + 1) % count, i) for i in range(ends)]),
            ],
            axis=dim,
        )
    return cells


def standardize(values, mean_value, inverse, groups):
    shape_full = values.shape
    grouped = values.reshape(shape_full[:-1] + (groups, shape_full[-1] // groups))
    return ((grouped - mean_value[:, None]) * inverse[:, None]).reshape(shape_full)


def causal_taps(padded, weight, frames, rows, cols):
    channels_in = padded.shape[-1]
    summed = jnp.zeros((frames * rows * cols, weight.shape[1]), jnp.float32)
    for lag_step in range(3):
        for row_step in range(3):
            for col_step in range(3):
                tap_index = (lag_step * 3 + row_step) * 3 + col_step
                window = padded[
                    lag_step : lag_step + frames,
                    row_step : row_step + rows,
                    col_step : col_step + cols,
                ]
                kernel = weight[tap_index * channels_in : (tap_index + 1) * channels_in]
                summed = summed + jnp.dot(
                    window.reshape(-1, channels_in), kernel, preferred_element_type=jnp.float32
                )
    return summed.reshape(frames, rows, cols, weight.shape[1])


def transposed_taps(padded, weight, frames, rows, cols):
    channels_out = padded.shape[-1]
    channels_in = weight.shape[0] // 27
    summed = jnp.zeros((frames * rows * cols, channels_in), jnp.float32)
    for lag_step in range(3):
        for row_step in range(3):
            for col_step in range(3):
                tap_index = (lag_step * 3 + row_step) * 3 + col_step
                window = padded[
                    2 - lag_step : 2 - lag_step + frames,
                    2 - row_step : 2 - row_step + rows,
                    2 - col_step : 2 - col_step + cols,
                ]
                kernel = weight[tap_index * channels_in : (tap_index + 1) * channels_in]
                summed = summed + lax.dot_general(
                    window.reshape(-1, channels_out),
                    kernel,
                    (((1,), (1,)), ((), ())),
                    preferred_element_type=jnp.float32,
                )
    return summed.reshape(frames, rows, cols, channels_in)


def weight_terms(padded, grads, frames, rows, cols):
    channels_in = padded.shape[-1]
    flat_grads = grads.reshape(-1, grads.shape[-1])
    blocks = []
    for row_step in range(3):
        for col_step in range(3):
            window = padded[2 : 2 + frames, row_step : row_step + rows, col_step : col_step + cols]
            blocks.append(
                lax.dot_general(
                    window.reshape(-1, channels_in),
                    flat_grads,
                    (((0,), (0,)), ((), ())),
                    preferred_element_type=jnp.float32,
                )
            )
    return jnp.concatenate(blocks, 0)


def local(
    latent,
    gain_latent,
    shift_latent,
    conv_latent,
    up_weight,
    gain_block,
    shift_block,
    conv_block,
    cotangent,
):
    per_group = C1 // GROUPS
    groups_here = latent.shape[-1] // per_group
    latent_f32 = latent.astype(jnp.float32)
    grouped = latent_f32.reshape(-1, groups_here, per_group)
    first_sums = jnp.sum(grouped, axis=(0, 2))
    second_sums = jnp.sum(grouped * grouped, axis=(0, 2))
    first_totals, second_totals = lax.psum((first_sums, second_sums), "tm")
    count_latent = grouped.shape[0] * per_group * lax.axis_size("tm")
    mean_latent = first_totals / count_latent
    inverse_latent = lax.rsqrt(second_totals / count_latent - mean_latent * mean_latent + epsilon)
    normed = (
        standardize(latent_f32, mean_latent, inverse_latent, groups_here) * gain_latent
        + shift_latent
    )
    active = jax.nn.silu(normed).astype(jnp.bfloat16)
    earlier = shifted(active, "tm", 1)
    extended = jnp.concatenate([earlier, active], 0)
    all_channels = lax.all_gather(extended, "height", axis=3, tiled=True)
    padded = jnp.pad(all_channels, ((0, 0), (1, 1), (1, 1), (0, 0)))
    latent_weight = lax.all_gather(conv_latent, "tm", axis=0, tiled=True)
    frames_latent, rows_latent, cols_latent = (latent.shape[0], latent.shape[1], latent.shape[2])
    mixed = causal_taps(padded, latent_weight, frames_latent, rows_latent, cols_latent)
    refined = (latent_f32 + mixed).astype(jnp.bfloat16)
    band_rows = rows_latent // lax.axis_size("height")
    own_band = lax.all_to_all(refined, "height", split_axis=1, concat_axis=3, tiled=True)
    flat_band = own_band.reshape(-1, own_band.shape[-1])
    expanded = jnp.dot(
        flat_band,
        lax.all_gather(up_weight, "height", axis=0, tiled=True),
        preferred_element_type=jnp.float32,
    )
    channels_block = up_weight.shape[1] // 8
    spread = expanded.reshape(frames_latent, band_rows, cols_latent, 2, 2, 2, channels_block)
    spread = spread.transpose(0, 3, 1, 4, 2, 5, 6)
    upsampled = spread.reshape(
        2 * frames_latent, 2 * band_rows, 2 * cols_latent, channels_block
    ).astype(jnp.bfloat16)
    frames_block, rows_block, cols_block = (
        upsampled.shape[0],
        upsampled.shape[1],
        upsampled.shape[2],
    )
    up_f32 = upsampled.astype(jnp.float32)
    per_block = channels_block // GROUPS
    grouped_block = up_f32.reshape(-1, GROUPS, per_block)
    block_first = jnp.sum(grouped_block, axis=(0, 2))
    block_second = jnp.sum(grouped_block * grouped_block, axis=(0, 2))
    block_first, block_second = lax.psum((block_first, block_second), ("tm", "height"))
    count_block = grouped_block.shape[0] * per_block * lax.axis_size("tm") * lax.axis_size("height")
    mean_block = block_first / count_block
    inverse_block = lax.rsqrt(block_second / count_block - mean_block * mean_block + epsilon)
    standard = standardize(up_f32, mean_block, inverse_block, GROUPS)
    normed_block = standard * gain_block + shift_block
    active_block = jax.nn.silu(normed_block).astype(jnp.bfloat16)
    before = shifted(active_block[-2:], "tm", 1)
    ext_block = jnp.concatenate([before, active_block], 0)
    beside_all = extended_2(ext_block, (("height", 1),), 1)
    padded_block = jnp.pad(beside_all, ((0, 0), (0, 0), (1, 1), (0, 0)))
    block_weight = lax.all_gather(conv_block, ("tm", "height"), axis=0, tiled=True)
    mixed_block = causal_taps(padded_block, block_weight, frames_block, rows_block, cols_block)
    decoded = (up_f32 + mixed_block).astype(jnp.bfloat16)
    after = shifted(cotangent[:2], "tm", -1)
    grad_ext = jnp.concatenate([cotangent, after], 0)
    grad_around = extended_2(grad_ext, (("height", 1),), 1)
    grad_padded = jnp.pad(grad_around, ((0, 0), (0, 0), (1, 1), (0, 0)))
    grad_active = transposed_taps(grad_padded, block_weight, frames_block, rows_block, cols_block)
    local_terms = weight_terms(padded_block, cotangent, frames_block, rows_block, cols_block)
    grad_weight = lax.psum_scatter(local_terms, ("tm", "height"), scatter_dimension=0, tiled=True)
    sigmoid = jax.nn.sigmoid(normed_block)
    grad_normed = grad_active * sigmoid * (1.0 + normed_block * (1.0 - sigmoid))
    flat_grad = grad_normed.reshape(-1, channels_block)
    flat_standard = standard.reshape(-1, channels_block)
    grad_shift, grad_gain = lax.psum(
        (jnp.sum(flat_grad, axis=0), jnp.sum(flat_grad * flat_standard, axis=0)), ("tm", "height")
    )
    first_mean = jnp.sum((gain_block * grad_shift).reshape(GROUPS, per_block), axis=1) / count_block
    second_mean = jnp.sum((gain_block * grad_gain).reshape(GROUPS, per_block), axis=1) / count_block
    grouped_grad = (grad_normed * gain_block).reshape(-1, GROUPS, per_block)
    grouped_standard = standard.reshape(-1, GROUPS, per_block)
    corrected = (
        grouped_grad - first_mean[:, None] - grouped_standard * second_mean[:, None]
    ) * inverse_block[:, None]
    grad_upsampled = (cotangent.astype(jnp.float32) + corrected.reshape(cotangent.shape)).astype(
        jnp.bfloat16
    )
    return (decoded, grad_upsampled, grad_weight, grad_gain, grad_shift)


MESH = pl.DeviceIdType.MESH
F32 = jnp.float32
BF16 = jnp.bfloat16


def group_matrix(channels, per):
    row = lax.broadcasted_iota(jnp.int32, (channels, channels), 0) // per
    col = lax.broadcasted_iota(jnp.int32, (channels, channels), 1) // per
    return (row == col).astype(F32)


def over_groups(rows, per):
    return jnp.dot(
        rows,
        group_matrix(rows.shape[-1], per),
        precision=lax.Precision.HIGHEST,
        preferred_element_type=F32,
    )


def column_shift(cells, cols, step):
    count = cells.shape[0]
    column = lax.broadcasted_iota(jnp.int32, cells.shape, 0) % cols
    edge = 0 if step == 1 else cols - 1
    return jnp.where(column == edge, 0.0, pltpu.roll(cells, step % count, 0))


def two_rows(first, second):
    width = first.shape[-1]
    row = lax.broadcasted_iota(jnp.int32, (8, width), 0)
    return jnp.where(row == 0, first, jnp.where(row == 1, second, 0.0))


def block_kernel(sizes, n_send, *refs):
    (T, H, Fl, Rl, Cl, CH, C2, F, R, C) = sizes
    (
        latent, gain_l, shift_l, w_l, up_w, gain_b, shift_b, w_b, cot,
        decoded, grad_up, grad_w, grad_gs,
        lbuf, gall, sall, wl, abuf, part, partf, parts_in, stat2, stat3, upw, wb,
        ub, std, ab, cb, cot3, gw, gy, gs, gz, acc, tmp, lace, send_sem, recv_sem, local_sem,
    ) = refs
    d, t, h = lax.axis_index("dp"), lax.axis_index("tm"), lax.axis_index("height")
    N = T * H
    FL = T * Fl
    U = H * CH // T
    band = Rl // H
    q = lax.rem(d, 4)
    half, side = lax.rem(q, 2), q // 2
    pair = d + 1 - 2 * half
    across = d + 2 - 4 * side
    used = [0]
    sent = []

    def at(kt, kh):
        return (d, lax.rem(t + kt, T), lax.rem(h + kh, H))

    def copy(src, dst, device):
        k = used[0]
        used[0] += 1
        return pltpu.make_async_remote_copy(
            src_ref=src, dst_ref=dst, send_sem=send_sem.at[k], recv_sem=recv_sem.at[k],
            device_id=device, device_id_type=MESH,
        )

    def go(src, dst, device):
        made = copy(src, dst, device)
        made.start()
        sent.append(made)
        return made

    def scope(name):
        return jax.named_scope(name)

    def recv(name, *made):
        with scope(name):
            for m in made:
                m.wait_recv()

    peers = [(kt, kh) for kt in range(T) for kh in range(H) if kt or kh]
    far = [kh for kh in range(H // 2, H)] + [kh for kh in range(1, H // 2)]
    shard = w_b.shape[0]

    def local_copy(k, src, dst):
        made = pltpu.make_async_copy(src, dst, local_sem.at[k])
        made.start()
        return made

    own_l = local_copy(0, latent, lbuf.at[t, h])
    cb[...] = jnp.zeros(cb.shape, BF16)
    barrier = pltpu.get_barrier_semaphore()
    for kt, kh in peers:
        pl.semaphore_signal(barrier, inc=1, device_id=at(kt, kh), device_id_type=MESH)
    pl.semaphore_signal(barrier, inc=1, device_id=(pair, t, h), device_id_type=MESH)
    pl.semaphore_signal(barrier, inc=1, device_id=(across, t, h), device_id_type=MESH)
    own_up = local_copy(1, up_w, upw.at[pl.ds(pl.multiple_of(h * CH, CH), CH)])
    own_w = local_copy(2, w_b, wb.at[pl.ds(pl.multiple_of((t * H + h) * shard, shard), shard)])
    own_wl = local_copy(3, w_l, wl)
    abuf[...] = jnp.zeros(abuf.shape, BF16)
    ab[...] = jnp.zeros(ab.shape, BF16)
    own_c = local_copy(4, cot, cb.at[pl.ds(0, F), pl.ds(1, R)])
    gall[h] = gain_l[...]
    sall[h] = shift_l[...]
    own_l.wait()
    with scope("w_barrier"):
        pl.semaphore_wait(barrier, N + 1)

    mine = lbuf.at[t, h]
    lz = {kh: go(mine, mine, at(0, kh)) for kh in far}
    gz_in = [go(gain_l, gall.at[h], at(0, kh)) for kh in range(1, H)]
    gz_in += [go(shift_l, sall.at[h], at(0, kh)) for kh in range(1, H)]
    ly = [go(mine, mine, at(kt, 0)) for kt in range(1, T)]

    up_rows, up_cols = CH // T, 8 * C2 // 4

    def up_piece(gt, gh, quarter):
        return upw.at[
            pl.ds(pl.multiple_of(gh * CH + gt * up_rows, up_rows), up_rows),
            pl.ds(pl.multiple_of(quarter * up_cols, up_cols), up_cols),
        ]

    own_up.wait()
    uz = {kh: go(up_piece(t, h, q), up_piece(t, h, q), at(0, kh)) for kh in far}

    def back(kh):
        return lax.rem(h + H - kh, H)

    for kh in range(1, H):
        recv("w_lz", lz[kh])
        got = lbuf.at[t, back(kh)]
        for kt in range(1, T):
            ly.append(go(got, got, at(kt, 0)))

    ux, upair, uy = [], [], []

    def up_on(gt, gh):
        piece = up_piece(gt, gh, q)
        ux.append((gt, gh, go(piece, piece, (across, t, h))))
        upair.append(go(piece, piece, (pair, t, h)))

    for kh in range(1, H):
        recv("w_uz", uz[kh])
        piece = up_piece(t, back(kh), q)
        for kt in range(1, T):
            uy.append((kt, kh, go(piece, piece, at(kt, 0))))
        up_on(t, back(kh))

    recv("w_ly", *ly)
    recv("w_gain", *gz_in)

    per_l = H * CH // GROUPS
    cells_l = FL * Rl * Cl
    count_l = cells_l * per_l
    xs, rows = [], []
    for k in range(H):
        x = lbuf[:, k].astype(F32).reshape(cells_l, CH)
        rows += [jnp.sum(x, 0, keepdims=True), jnp.sum(x * x, 0, keepdims=True)]
    total = over_groups(jnp.concatenate(rows, 0), per_l) / count_l
    for k in range(H):
        mean = total[2 * k : 2 * k + 1]
        inv = lax.rsqrt(total[2 * k + 1 : 2 * k + 2] - mean * mean + epsilon)
        x = lbuf[:, k].astype(F32).reshape(cells_l, CH)
        v = (x - mean) * inv * gall[k] + sall[k]
        lane = k * CH % U
        abuf[k * CH // U, 2 : 2 + FL, 1 : 1 + Rl, :, lane : lane + CH] = (
            (v * jax.nn.sigmoid(v)).astype(BF16).reshape(FL, Rl, Cl, CH)
        )

    own_wl.wait()

    def window(chunk, tap):
        lag, dr = tap // 9, (tap // 3) % 3
        return abuf[chunk, pl.ds(lag, FL), pl.ds(dr, Rl)].reshape(cells_l, U)

    def w_rows(chunk, tap):
        return wl[pl.ds(pl.multiple_of((tap * T + chunk - 27 * t) * U, U), U), :]

    with scope("c_latent"):
        sums = None
        for g in range(4):
            tap = jnp.where(t == 0, 3 * g, 15 + 3 * g)
            for chunk in range(T):
                k3 = jnp.concatenate([w_rows(chunk, tap + dc) for dc in range(3)], 1)
                term = jnp.dot(window(chunk, tap), k3, preferred_element_type=F32)
                sums = term if sums is None else sums + term
        alone = jnp.where(t == 0, 12, 14)
        k2 = jnp.concatenate([w_rows(t, alone), w_rows(t, 13)], 1)
        both = jnp.dot(window(t, alone), k2, preferred_element_type=F32)
        lone = both[:, :CH] + jnp.dot(
            window(1 - t, alone), w_rows(1 - t, alone), preferred_element_type=F32
        )
        first = sums[:, :CH] + jnp.where(t == 0, lone, 0.0)
        last = sums[:, 2 * CH :] + jnp.where(t == 0, 0.0, lone)
        mixed = (
            column_shift(first, Cl, 1) + sums[:, CH : 2 * CH] + both[:, CH:]
            + column_shift(last, Cl, -1)
        )
        partf[...] = mixed.reshape(FL, Rl, Cl, CH)
        partf[pl.ds(t * Fl, Fl)] += lbuf[t, h].astype(F32)
        part[...] = partf[...].astype(BF16)
    p_in = []
    for kt, kh in [(kt, kh) for kh in far + [0] for kt in range(T) if kt or kh]:
        dev = at(kt, kh)
        p_in.append(
            go(part.at[pl.ds(dev[1] * Fl, Fl), pl.ds(dev[2] * band, band)],
               parts_in.at[kt * H + kh], dev)
        )

    own_w.wait()
    own_c.wait()
    w_half = shard // 2

    def w_piece(gt, gh, piece_side):
        start = pl.multiple_of((gt * H + gh) * shard + piece_side * w_half, w_half)
        return wb.at[pl.ds(start, w_half), pl.ds(pl.multiple_of(half * (C2 // 2), C2 // 2), C2 // 2)]

    w_mine = w_piece(t, h, side)
    wz = {kh: go(w_mine, w_mine, at(0, kh)) for kh in far}
    wy = [(kt, 0, go(w_mine, w_mine, at(kt, 0))) for kt in range(1, T)]
    wx, wpair = [], []

    def w_on(gt, gh):
        piece = w_piece(gt, gh, side)
        wx.append((gt, gh, go(piece, piece, (across, t, h))))
        wpair.append(go(piece, piece, (pair, t, h)))

    def halo(buffer, f0, f_two, two_at, step):
        made = []
        ok_t_send = (t < T - 1) if step == 1 else (t > 0)
        ok_t_recv = (t > 0) if step == 1 else (t < T - 1)
        kt = step % T

        def part_of(fs, n_f, r0, n_r):
            return buffer.at[pl.ds(fs, n_f), pl.ds(r0, n_r)]

        for kt_, kh_, ok_s, ok_r, src, dst in (
            (kt, 0, ok_t_send, ok_t_recv, part_of(f_two, 2, 1, R), part_of(two_at, 2, 1, R)),
            (0, 1, h < H - 1, h > 0, part_of(f0, F, R, 1), part_of(f0, F, 0, 1)),
            (0, H - 1, h > 0, h < H - 1, part_of(f0, F, 1, 1), part_of(f0, F, R + 1, 1)),
            (kt, 1, ok_t_send & (h < H - 1), ok_t_recv & (h > 0),
             part_of(f_two, 2, R, 1), part_of(two_at, 2, 0, 1)),
            (kt, H - 1, ok_t_send & (h > 0), ok_t_recv & (h < H - 1),
             part_of(f_two, 2, 1, 1), part_of(two_at, 2, R + 1, 1)),
        ):
            c = copy(src, dst, at(kt_, kh_))
            pl.when(ok_s)(c.start)
            made.append((c, ok_s, ok_r))
        return made

    cot_halo = halo(cb, 0, 0, F, -1)

    for kt, kh, made in uy:
        recv("w_uy", made)
        up_on(lax.rem(t + T - kt, T), back(kh))
    for gt, gh, made in ux:
        recv("w_ux", made)
        piece = up_piece(gt, gh, lax.rem(q + 2, 4))
        upair.append(go(piece, piece, (pair, t, h)))
    recv("w_upair", *upair)
    recv("w_parts", *p_in)

    cells_b = Fl * band * Cl
    with scope("c_up"):
        parts_own = partf[pl.ds(t * Fl, Fl), pl.ds(h * band, band)]
        expanded = jnp.zeros((cells_b, 8 * C2), F32)
        for kh in range(H):
            value = parts_own if kh == 0 else parts_in[kh].astype(F32)
            for kt in range(1, T):
                value = value + parts_in[kt * H + kh].astype(F32)
            refined = value.reshape(cells_b, CH).astype(BF16)
            source = back(kh)
            expanded = expanded + jnp.dot(
                refined, upw[pl.ds(pl.multiple_of(source * CH, CH), CH), :],
                preferred_element_type=F32,
            )
        expanded = expanded.astype(BF16).astype(F32)
        for f in range(Fl):
            for r in range(band):
                for p in range(2):
                    for qq in range(2):
                        for s in range(2):
                            first = (f * band + r) * Cl
                            col = ((p * 2 + qq) * 2 + s) * C2
                            for n in range(C2 // 128):
                                lace[
                                    n, pl.ds(((2 * f + p) * R + 2 * r + qq) * C + s, Cl, stride=2), :
                                ] = expanded[first : first + Cl, col + n * 128 : col + (n + 1) * 128]

        cells = F * R * C
        me = t * H + h
        up = jnp.concatenate([lace[n] for n in range(C2 // 128)], axis=1)
        stat2[me] = two_rows(jnp.sum(up, 0, keepdims=True), jnp.sum(up * up, 0, keepdims=True))
        ub[2 : 2 + F, 1 : 1 + R] = up.astype(BF16).reshape(F, R, C, C2)
    s2 = [go(stat2.at[me], stat2.at[me], at(kt, kh)) for kt, kh in peers]
    up_halo = halo(ub, 2, F, 0, 1)

    for kh in range(1, H):
        recv("w_wz", wz[kh])
        piece = w_piece(t, back(kh), side)
        for kt in range(1, T):
            wy.append((kt, kh, go(piece, piece, at(kt, 0))))
        w_on(t, back(kh))
    with scope("w_cothalo"):
        for made, _, ok in cot_halo:
            pl.when(ok)(made.wait_recv)
    wide = cb[0:F].astype(F32).reshape(F * (R + 2) * C, C2)
    cot3[:, :, :, 0:C2] = column_shift(wide, C, -1).astype(BF16).reshape(F, R + 2, C, C2)
    cot3[:, :, :, C2 : 2 * C2] = cb[0:F]
    cot3[:, :, :, 2 * C2 :] = column_shift(wide, C, 1).astype(BF16).reshape(F, R + 2, C, C2)

    recv("w_s2", *s2)
    per_b = C2 // GROUPS
    count_b = cells * per_b * N
    total = stat2[0]
    for k in range(1, N):
        total = total + stat2[k]
    total = over_groups(total, per_b) / count_b
    mean_b = total[0:1]
    inv_b = lax.rsqrt(total[1:2] - mean_b * mean_b + epsilon)

    def activate(values):
        normed = (values - mean_b) * inv_b * gain_b[...] + shift_b[...]
        return (normed * jax.nn.sigmoid(normed)).astype(BF16)

    with scope("c_gw"):
        own = activate(ub[2 : 2 + F, 1 : 1 + R].astype(F32).reshape(cells, C2))
        ab[2 : 2 + F, 1 : 1 + R] = own.reshape(F, R, C, C2)
        for dr in range(3):
            term = lax.dot_general(
                own, cot3[:, 2 - dr : 2 - dr + R].reshape(cells, 3 * C2),
                (((0,), (0,)), ((), ())), preferred_element_type=F32,
            )
            for dc in range(3):
                gw[(dr * 3 + dc) * C2 : (dr * 3 + dc + 1) * C2, :] = (
                    term[:, dc * C2 : (dc + 1) * C2].astype(BF16)
                )
    out_rows = 9 * C2 // N
    y_rows = out_rows * H

    def g_rows(gt, gh):
        return gw.at[pl.ds(pl.multiple_of((gt * H + gh) * out_rows, out_rows), out_rows)]

    def ahead(kh):
        return lax.rem(h + kh, H)

    g_y = []
    for kh in far + [0]:
        for kt in range(1, T):
            dev = at(kt, 0)
            g_y.append((kh, kt, go(g_rows(dev[1], ahead(kh)), gy.at[kt, kh], dev)))

    for kt, kh, made in wy:
        recv("w_wy", made)
        w_on(lax.rem(t + T - kt, T), back(kh))
    with scope("w_uphalo"):
        for made, _, ok in up_halo:
            pl.when(ok)(made.wait_recv)
    with scope("c_halo"):
        for rows_at, n_rows, ok in ((0, 1, h > 0), (R + 1, 1, h < H - 1)):
            @pl.when(ok)
            def _():
                v = ub[2 : 2 + F, rows_at : rows_at + n_rows].astype(F32).reshape(F * n_rows * C, C2)
                ab[2 : 2 + F, rows_at : rows_at + n_rows] = activate(v).reshape(F, n_rows, C, C2)
        for rows_at, n_rows, ok in (
            (1, R, t > 0), (0, 1, (t > 0) & (h > 0)), (R + 1, 1, (t > 0) & (h < H - 1))
        ):
            @pl.when(ok)
            def _():
                v = ub[0:2, rows_at : rows_at + n_rows].astype(F32).reshape(2 * n_rows * C, C2)
                ab[0:2, rows_at : rows_at + n_rows] = activate(v).reshape(2, n_rows, C, C2)

    for gt, gh, made in wx:
        recv("w_wx", made)
        piece = w_piece(gt, gh, 1 - side)
        wpair.append(go(piece, piece, (pair, t, h)))

    g_z = {}

    def g_on(kh):
        total = None
        for made_kh, kt, made in g_y:
            if made_kh == kh:
                recv("w_gy", made)
                term = gy[kt, kh].astype(F32)
                total = term if total is None else total + term
        start = pl.multiple_of((t * H + ahead(kh)) * out_rows, out_rows)
        total = total + gw[pl.ds(start, out_rows), :].astype(F32)
        if kh == 0:
            grad_w[...] = total
        else:
            gs[kh] = total.astype(BF16)
            g_z[kh] = go(gs.at[kh], gz.at[kh], at(0, kh))

    recv("w_wpair", *wpair)

    acc[...] = jnp.zeros(acc.shape, F32)

    def grad_tap(j, _):
        lag, dr = j // 3, j % 3
        win = cb[pl.ds(2 - lag, F), pl.ds(2 - dr, R)].reshape(cells, C2)
        for dc in range(3):
            rows = wb[pl.ds(pl.multiple_of((j * 3 + dc) * C2, C2), C2), :]
            acc[dc] += lax.dot_general(
                win, rows, (((1,), (1,)), ((), ())), preferred_element_type=F32
            )
        return 0

    with scope("c_gradtap"):
        lax.fori_loop(0, 9, grad_tap, 0)
    grad_active = column_shift(acc[0], C, -1) + acc[1] + column_shift(acc[2], C, 1)
    standard = (ub[2 : 2 + F, 1 : 1 + R].astype(F32).reshape(cells, C2) - mean_b) * inv_b
    std[...] = standard
    normed = standard * gain_b[...] + shift_b[...]
    sigmoid = jax.nn.sigmoid(normed)
    grad_normed = grad_active * sigmoid * (1.0 + normed * (1.0 - sigmoid))
    stat3[me] = two_rows(
        jnp.sum(grad_normed * standard, 0, keepdims=True), jnp.sum(grad_normed, 0, keepdims=True)
    )
    s3 = [go(stat3.at[me], stat3.at[me], at(kt, kh)) for kt, kh in peers]
    tmp[...] = grad_normed * gain_b[...]
    for kh in far:
        g_on(kh)

    acc[0] = jnp.zeros((cells, C2), F32)
    acc[1] = ub[2 : 2 + F, 1 : 1 + R].astype(F32).reshape(cells, C2)
    acc[2] = jnp.zeros((cells, C2), F32)

    def tap(j, _):
        lag, dr = j // 3, j % 3
        win = ab[pl.ds(lag, F), pl.ds(dr, R)].reshape(cells, C2)
        for dc in range(3):
            rows = wb[pl.ds(pl.multiple_of((j * 3 + dc) * C2, C2), C2), :]
            acc[dc] += jnp.dot(win, rows, preferred_element_type=F32)
        return 0

    with scope("c_tap"):
        lax.fori_loop(0, 9, tap, 0)
    decoded[...] = (
        (column_shift(acc[0], C, 1) + acc[1] + column_shift(acc[2], C, -1))
        .astype(BF16).reshape(F, R, C, C2)
    )
    g_on(0)

    recv("w_s3", *s3)
    total = stat3[0]
    for k in range(1, N):
        total = total + stat3[k]
    grad_gs[...] = total
    means = over_groups(total * gain_b[...], per_b) / count_b
    corrected = (tmp[...] - means[1:2] - std[...] * means[0:1]) * inv_b
    grad_up[...] = (
        cb[0:F, 1 : 1 + R].astype(F32).reshape(cells, C2) + corrected
    ).astype(BF16).reshape(F, R, C, C2)

    recv("w_gz", *g_z.values())
    result = grad_w[...]
    for kh in range(1, H):
        result = result + gz[kh].astype(F32)
    grad_w[...] = result

    with scope("w_send"):
        for made in sent:
            made.wait_send()
        for made, ok, _ in cot_halo + up_halo:
            pl.when(ok)(made.wait_send)
    assert used[0] <= n_send


def local_block(shape, *args):
    (latent, gain_l, shift_l, w_l, up_w, gain_b, shift_b, w_b, cot) = args
    T, H = shape["tm"], shape["height"]
    Fl, Rl, Cl, CH = latent.shape
    F, R, C, C2 = cot.shape
    N = T * H
    U = H * CH // T
    fits = (
        shape["dp"] % 4 == 0 and T == 2
        and CH % 128 == 0 and U % CH == 0
        and w_b.shape[0] % 32 == 0 and (CH // T) % 16 == 0
        and (9 * C2) % (16 * N) == 0 and C2 % 256 == 0
        and Cl % 16 == 0 and w_l.shape[0] == 27 * U and F >= 2
    )
    if not fits:
        return local(*args)
    sizes = (T, H, Fl, Rl, Cl, CH, C2, F, R, C)
    n_send = 200
    FL = T * Fl
    band = Rl // H
    cells = F * R * C
    out_rows = 9 * C2 // N
    vmem = pl.BlockSpec(memory_space=pltpu.VMEM)
    hbm = pl.BlockSpec(memory_space=pl.ANY)
    flops = 2 * (FL * Rl * Cl * w_l.size + 2 * cells * 27 * C2 * C2 + cells * 9 * C2 * C2)
    outs = pl.pallas_call(
        functools.partial(block_kernel, sizes, n_send),
        out_shape=(
            jax.ShapeDtypeStruct(cot.shape, BF16),
            jax.ShapeDtypeStruct(cot.shape, BF16),
            jax.ShapeDtypeStruct((out_rows, C2), F32),
            jax.ShapeDtypeStruct((8, C2), F32),
        ),
        in_specs=[hbm, vmem, vmem, hbm, hbm, vmem, vmem, hbm, hbm],
        out_specs=(vmem,) * 4,
        scratch_shapes=[
            pltpu.VMEM((T, H, Fl, Rl, Cl, CH), BF16),
            pltpu.VMEM((H, 1, CH), F32),
            pltpu.VMEM((H, 1, CH), F32),
            pltpu.VMEM(w_l.shape, BF16),
            pltpu.VMEM((T, FL + 2, Rl + 2, Cl, U), BF16),
            pltpu.VMEM((FL, Rl, Cl, CH), BF16),
            pltpu.VMEM((FL, Rl, Cl, CH), F32),
            pltpu.VMEM((N, Fl, band, Cl, CH), BF16),
            pltpu.VMEM((N, 8, C2), F32),
            pltpu.VMEM((N, 8, C2), F32),
            pltpu.VMEM((H * CH, 8 * C2), BF16),
            pltpu.VMEM((27 * C2, C2), BF16),
            pltpu.VMEM((F + 2, R + 2, C, C2), BF16),
            pltpu.VMEM((cells, C2), F32),
            pltpu.VMEM((F + 2, R + 2, C, C2), BF16),
            pltpu.VMEM((F + 2, R + 2, C, C2), BF16),
            pltpu.VMEM((F, R + 2, C, 3 * C2), BF16),
            pltpu.VMEM((9 * C2, C2), BF16),
            pltpu.VMEM((T, H, out_rows, C2), BF16),
            pltpu.VMEM((H, out_rows, C2), BF16),
            pltpu.VMEM((H, out_rows, C2), BF16),
            pltpu.VMEM((3, cells, C2), F32),
            pltpu.VMEM((cells, C2), F32),
            pltpu.VMEM((C2 // 128, cells, 128), F32),
            pltpu.SemaphoreType.DMA((n_send,)),
            pltpu.SemaphoreType.DMA((n_send,)),
            pltpu.SemaphoreType.DMA((5,)),
        ],
        compiler_params=pltpu.CompilerParams(
            collective_id=0, has_side_effects=True, vmem_limit_bytes=60 * 1024 * 1024
        ),
        cost_estimate=pl.CostEstimate(flops=flops, bytes_accessed=1 << 23, transcendentals=0),
    )(
        latent, gain_l.reshape(1, -1), shift_l.reshape(1, -1), w_l, up_w,
        gain_b.reshape(1, -1), shift_b.reshape(1, -1), w_b, cot,
    )
    decoded, grad_up, grad_w, grad_gs = outs
    return decoded, grad_up, grad_w, grad_gs[0], grad_gs[1]


def solution(mesh):
    return jax.shard_map(
        functools.partial(local_block, dict(mesh.shape)),
        mesh=mesh,
        in_specs=(
            P(("dp", "tm"), None, None, "height"),
            P("height"),
            P("height"),
            P("tm", "height"),
            P("height", None),
            P(),
            P(),
            P(("tm", "height"), None),
            P(("dp", "tm"), "height", None, None),
        ),
        out_specs=(
            P(("dp", "tm"), "height", None, None),
            P(("dp", "tm"), "height", None, None),
            P(("dp", "tm", "height"), None),
            P("dp"),
            P("dp"),
        ),
        check_vma=False,
    )
```

```python
import functools

import jax
import jax.numpy as jnp
from jax import lax
from jax.experimental import pallas as pl
from jax.experimental.pallas import tpu as pltpu
from jax.sharding import PartitionSpec as P

C1 = 512
GROUPS = 32


epsilon = 1e-06


def shifted(block, axis, distance):
    devices = range(lax.axis_size(axis))
    route = [(i - distance, i) for i in devices if i - distance in devices]
    return lax.ppermute(block, axis, route)


def extended_2(cells, sides, width):
    for axis, dim in sides:
        count = lax.axis_size(axis)
        ends = count - 1
        head = lax.slice_in_dim(cells, 0, width, axis=dim)
        tail = lax.slice_in_dim(cells, cells.shape[dim] - width, cells.shape[dim], axis=dim)
        cells = jnp.concatenate(
            [
                lax.ppermute(tail, axis, [(i, (i + 1) % count) for i in range(ends)]),
                cells,
                lax.ppermute(head, axis, [((i + 1) % count, i) for i in range(ends)]),
            ],
            axis=dim,
        )
    return cells


def standardize(values, mean_value, inverse, groups):
    shape_full = values.shape
    grouped = values.reshape(shape_full[:-1] + (groups, shape_full[-1] // groups))
    return ((grouped - mean_value[:, None]) * inverse[:, None]).reshape(shape_full)


def causal_taps(padded, weight, frames, rows, cols):
    channels_in = padded.shape[-1]
    summed = jnp.zeros((frames * rows * cols, weight.shape[1]), jnp.float32)
    for lag_step in range(3):
        for row_step in range(3):
            for col_step in range(3):
                tap_index = (lag_step * 3 + row_step) * 3 + col_step
                window = padded[
                    lag_step : lag_step + frames,
                    row_step : row_step + rows,
                    col_step : col_step + cols,
                ]
                kernel = weight[tap_index * channels_in : (tap_index + 1) * channels_in]
                summed = summed + jnp.dot(
                    window.reshape(-1, channels_in), kernel, preferred_element_type=jnp.float32
                )
    return summed.reshape(frames, rows, cols, weight.shape[1])


def transposed_taps(padded, weight, frames, rows, cols):
    channels_out = padded.shape[-1]
    channels_in = weight.shape[0] // 27
    summed = jnp.zeros((frames * rows * cols, channels_in), jnp.float32)
    for lag_step in range(3):
        for row_step in range(3):
            for col_step in range(3):
                tap_index = (lag_step * 3 + row_step) * 3 + col_step
                window = padded[
                    2 - lag_step : 2 - lag_step + frames,
                    2 - row_step : 2 - row_step + rows,
                    2 - col_step : 2 - col_step + cols,
                ]
                kernel = weight[tap_index * channels_in : (tap_index + 1) * channels_in]
                summed = summed + lax.dot_general(
                    window.reshape(-1, channels_out),
                    kernel,
                    (((1,), (1,)), ((), ())),
                    preferred_element_type=jnp.float32,
                )
    return summed.reshape(frames, rows, cols, channels_in)


def weight_terms(padded, grads, frames, rows, cols):
    channels_in = padded.shape[-1]
    flat_grads = grads.reshape(-1, grads.shape[-1])
    blocks = []
    for row_step in range(3):
        for col_step in range(3):
            window = padded[2 : 2 + frames, row_step : row_step + rows, col_step : col_step + cols]
            blocks.append(
                lax.dot_general(
                    window.reshape(-1, channels_in),
                    flat_grads,
                    (((0,), (0,)), ((), ())),
                    preferred_element_type=jnp.float32,
                )
            )
    return jnp.concatenate(blocks, 0)


def local(
    latent,
    gain_latent,
    shift_latent,
    conv_latent,
    up_weight,
    gain_block,
    shift_block,
    conv_block,
    cotangent,
):
    per_group = C1 // GROUPS
    groups_here = latent.shape[-1] // per_group
    latent_f32 = latent.astype(jnp.float32)
    grouped = latent_f32.reshape(-1, groups_here, per_group)
    first_sums = jnp.sum(grouped, axis=(0, 2))
    second_sums = jnp.sum(grouped * grouped, axis=(0, 2))
    first_totals, second_totals = lax.psum((first_sums, second_sums), "tm")
    count_latent = grouped.shape[0] * per_group * lax.axis_size("tm")
    mean_latent = first_totals / count_latent
    inverse_latent = lax.rsqrt(second_totals / count_latent - mean_latent * mean_latent + epsilon)
    normed = (
        standardize(latent_f32, mean_latent, inverse_latent, groups_here) * gain_latent
        + shift_latent
    )
    active = jax.nn.silu(normed).astype(jnp.bfloat16)
    earlier = shifted(active, "tm", 1)
    extended = jnp.concatenate([earlier, active], 0)
    all_channels = lax.all_gather(extended, "height", axis=3, tiled=True)
    padded = jnp.pad(all_channels, ((0, 0), (1, 1), (1, 1), (0, 0)))
    latent_weight = lax.all_gather(conv_latent, "tm", axis=0, tiled=True)
    frames_latent, rows_latent, cols_latent = (latent.shape[0], latent.shape[1], latent.shape[2])
    mixed = causal_taps(padded, latent_weight, frames_latent, rows_latent, cols_latent)
    refined = (latent_f32 + mixed).astype(jnp.bfloat16)
    band_rows = rows_latent // lax.axis_size("height")
    own_band = lax.all_to_all(refined, "height", split_axis=1, concat_axis=3, tiled=True)
    flat_band = own_band.reshape(-1, own_band.shape[-1])
    expanded = jnp.dot(
        flat_band,
        lax.all_gather(up_weight, "height", axis=0, tiled=True),
        preferred_element_type=jnp.float32,
    )
    channels_block = up_weight.shape[1] // 8
    spread = expanded.reshape(frames_latent, band_rows, cols_latent, 2, 2, 2, channels_block)
    spread = spread.transpose(0, 3, 1, 4, 2, 5, 6)
    upsampled = spread.reshape(
        2 * frames_latent, 2 * band_rows, 2 * cols_latent, channels_block
    ).astype(jnp.bfloat16)
    frames_block, rows_block, cols_block = (
        upsampled.shape[0],
        upsampled.shape[1],
        upsampled.shape[2],
    )
    up_f32 = upsampled.astype(jnp.float32)
    per_block = channels_block // GROUPS
    grouped_block = up_f32.reshape(-1, GROUPS, per_block)
    block_first = jnp.sum(grouped_block, axis=(0, 2))
    block_second = jnp.sum(grouped_block * grouped_block, axis=(0, 2))
    block_first, block_second = lax.psum((block_first, block_second), ("tm", "height"))
    count_block = grouped_block.shape[0] * per_block * lax.axis_size("tm") * lax.axis_size("height")
    mean_block = block_first / count_block
    inverse_block = lax.rsqrt(block_second / count_block - mean_block * mean_block + epsilon)
    standard = standardize(up_f32, mean_block, inverse_block, GROUPS)
    normed_block = standard * gain_block + shift_block
    active_block = jax.nn.silu(normed_block).astype(jnp.bfloat16)
    before = shifted(active_block[-2:], "tm", 1)
    ext_block = jnp.concatenate([before, active_block], 0)
    beside_all = extended_2(ext_block, (("height", 1),), 1)
    padded_block = jnp.pad(beside_all, ((0, 0), (0, 0), (1, 1), (0, 0)))
    block_weight = lax.all_gather(conv_block, ("tm", "height"), axis=0, tiled=True)
    mixed_block = causal_taps(padded_block, block_weight, frames_block, rows_block, cols_block)
    decoded = (up_f32 + mixed_block).astype(jnp.bfloat16)
    after = shifted(cotangent[:2], "tm", -1)
    grad_ext = jnp.concatenate([cotangent, after], 0)
    grad_around = extended_2(grad_ext, (("height", 1),), 1)
    grad_padded = jnp.pad(grad_around, ((0, 0), (0, 0), (1, 1), (0, 0)))
    grad_active = transposed_taps(grad_padded, block_weight, frames_block, rows_block, cols_block)
    local_terms = weight_terms(padded_block, cotangent, frames_block, rows_block, cols_block)
    grad_weight = lax.psum_scatter(local_terms, ("tm", "height"), scatter_dimension=0, tiled=True)
    sigmoid = jax.nn.sigmoid(normed_block)
    grad_normed = grad_active * sigmoid * (1.0 + normed_block * (1.0 - sigmoid))
    flat_grad = grad_normed.reshape(-1, channels_block)
    flat_standard = standard.reshape(-1, channels_block)
    grad_shift, grad_gain = lax.psum(
        (jnp.sum(flat_grad, axis=0), jnp.sum(flat_grad * flat_standard, axis=0)), ("tm", "height")
    )
    first_mean = jnp.sum((gain_block * grad_shift).reshape(GROUPS, per_block), axis=1) / count_block
    second_mean = jnp.sum((gain_block * grad_gain).reshape(GROUPS, per_block), axis=1) / count_block
    grouped_grad = (grad_normed * gain_block).reshape(-1, GROUPS, per_block)
    grouped_standard = standard.reshape(-1, GROUPS, per_block)
    corrected = (
        grouped_grad - first_mean[:, None] - grouped_standard * second_mean[:, None]
    ) * inverse_block[:, None]
    grad_upsampled = (cotangent.astype(jnp.float32) + corrected.reshape(cotangent.shape)).astype(
        jnp.bfloat16
    )
    return (decoded, grad_upsampled, grad_weight, grad_gain, grad_shift)


MESH = pl.DeviceIdType.MESH
VMEM_LIMIT = 32 * 1024 * 1024
W_EARLY = 2
F32 = jnp.float32
BF16 = jnp.bfloat16


def group_matrix(channels, per):
    row = lax.broadcasted_iota(jnp.int32, (channels, channels), 0) // per
    col = lax.broadcasted_iota(jnp.int32, (channels, channels), 1) // per
    return (row == col).astype(F32)


def over_groups(rows, per):
    return jnp.dot(
        rows,
        group_matrix(rows.shape[-1], per),
        precision=lax.Precision.HIGHEST,
        preferred_element_type=F32,
    )


def column_shift(cells, cols, step):
    count = cells.shape[0]
    column = lax.broadcasted_iota(jnp.int32, cells.shape, 0) % cols
    edge = 0 if step == 1 else cols - 1
    return jnp.where(column == edge, 0.0, pltpu.roll(cells, step % count, 0))


def two_rows(first, second):
    width = first.shape[-1]
    row = lax.broadcasted_iota(jnp.int32, (8, width), 0)
    return jnp.where(row == 0, first, jnp.where(row == 1, second, 0.0))


def block_kernel(sizes, n_send, n_recv, *refs):
    (T, H, Fl, Rl, Cl, CH, C2, F, R, C) = sizes
    (
        latent, gain_in, shift_in, w_l, up_w, gain_b_in, shift_b_in, w_b, cot,
        decoded, grad_up, grad_w, grad_gs,
        lbuf, gall, gain_b, shift_b, wl, abuf, part, partf, parts_in, stat2, stat3, upw, wb,
        ub, std, ab, cb, cot3, gw, gy, gs, gz, tmp, lace, send_sem, recv_sem, local_sem,
    ) = refs
    d, t, h = lax.axis_index("dp"), lax.axis_index("tm"), lax.axis_index("height")
    N = T * H
    FL = T * Fl
    U = H * CH // T
    band = Rl // H
    q = lax.rem(d, 4)
    half, side = lax.rem(q, 2), q // 2
    pair = d + 1 - 2 * half
    across = d + 2 - 4 * side
    counts = [0, 0]

    def new_send():
        counts[0] += 1
        return send_sem.at[counts[0] - 1]

    def new_recv(n=1):
        counts[1] += n
        return recv_sem.at[counts[1] - 1] if n == 1 else counts[1] - n

    def at(kt, kh):
        return (d, lax.rem(t + kt, T), lax.rem(h + kh, H))

    def copy(src, dst, device, s_sem, r_sem):
        return pltpu.make_async_remote_copy(
            src_ref=src, dst_ref=dst, send_sem=s_sem, recv_sem=r_sem,
            device_id=device, device_id_type=MESH,
        )

    def go(*what):
        copy(*what).start()

    pair_dev, across_dev = (pair, t, h), (across, t, h)
    left = []

    def got(name, ref, r_sem):
        with scope(name):
            copy(ref, ref, pair_dev, send_sem.at[0], r_sem).wait_recv()

    def left_all(ref, s_sem):
        left.append((ref, s_sem))

    def scope(name):
        return jax.named_scope(name)

    peers = [(kt, kh) for kh in [*range(H // 2, H), *range(1, H // 2), 0] for kt in range(T) if kt or kh]
    shard = w_b.shape[0]

    def local_copy(k, src, dst):
        made = pltpu.make_async_copy(src, dst, local_sem.at[k])
        made.start()
        return made

    def near(i):
        where = 0
        for hh in range(H):
            order = sorted((o for o in range(H) if o != hh), key=lambda o: (abs(o - hh), -o))
            where = where + jnp.where(h == hh, order[i], 0)
        return where

    nearest = [near(i) for i in range(H - 1)]

    class Along:
        def __init__(self, s_sem):
            self.s, self.base = s_sem, new_recv(H - 1)

        def send(self, i, src, dst):
            to = nearest[i]
            r = recv_sem.at[self.base + lax.rem(to - h + H, H) - 1]
            go(src, dst, (d, t, to), self.s, r)

        def wait(self, name, i, ref):
            got(name, ref, recv_sem.at[self.base + lax.rem(h - nearest[i] + H, H) - 1])

    own_l = local_copy(0, latent, lbuf.at[t, h])
    cb[...] = jnp.zeros(cb.shape, BF16)
    barrier = pltpu.get_barrier_semaphore()
    for kt, kh in peers:
        pl.semaphore_signal(barrier, inc=1, device_id=at(kt, kh), device_id_type=MESH)
    pl.semaphore_signal(barrier, inc=1, device_id=pair_dev, device_id_type=MESH)
    pl.semaphore_signal(barrier, inc=1, device_id=across_dev, device_id_type=MESH)
    own_w = local_copy(2, w_b, wb.at[pl.ds(pl.multiple_of((t * H + h) * shard, shard), shard)])
    own_g = [
        local_copy(5, gain_in, gall.at[h, pl.ds(0, 1)]),
        local_copy(6, shift_in, gall.at[h, pl.ds(1, 1)]),
        local_copy(7, gain_b_in, gain_b), local_copy(8, shift_b_in, shift_b),
    ]
    own_up = local_copy(1, up_w, upw.at[pl.ds(pl.multiple_of(h * CH, CH), CH)])
    own_c = local_copy(4, cot, cb.at[pl.ds(0, F), pl.ds(1, R)])
    own_wl = local_copy(3, w_l, wl)
    abuf[...] = jnp.zeros(abuf.shape, BF16)
    ab[...] = jnp.zeros(ab.shape, BF16)
    own_l.wait()
    with scope("w_barrier"):
        pl.semaphore_wait(barrier, N + 1)

    yes = at(1, 0)
    w_half = shard // 2
    half_cols = pl.ds(pl.multiple_of(half * (C2 // 2), C2 // 2), C2 // 2)

    def w_piece(gt, gh, piece_side):
        start = pl.multiple_of((gt * H + gh) * shard + piece_side * w_half, w_half)
        return wb.at[pl.ds(start, w_half), half_cols]

    def w_both(gt, gh):
        return wb.at[pl.ds(pl.multiple_of((gt * H + gh) * shard, shard), shard), half_cols]

    up_rows, up_cols = CH // T, 2 * C2

    def up_piece(gt, gh, n=1):
        first = 2 * half + (side if n == 1 else 0)
        return upw.at[
            pl.ds(pl.multiple_of(gh * CH + gt * up_rows, up_rows), up_rows),
            pl.ds(pl.multiple_of(first * up_cols, up_cols), n * up_cols),
        ]

    mine = lbuf.at[t, h]
    lz = Along(new_send())
    ly_s, ly_r = new_send(), new_recv()
    for i in range(H - 1):
        lz.send(i, mine, mine)
    go(mine, mine, yes, ly_s, ly_r)
    own_w.wait()
    w_s = new_send()
    w_mine = w_piece(t, h, side)
    wy_r = [new_recv() for _ in range(H)]
    go(w_mine, w_mine, yes, w_s, wy_r[H - 1])
    for made in own_g:
        made.wait()
    gain_s, gain_r = new_send(), new_recv()
    for kh in range(1, H):
        go(gall.at[h], gall.at[h], at(0, kh), gain_s, gain_r)
    own_up.wait()
    u_s = new_send()
    uz = Along(u_s)
    for i in range(H - 1):
        uz.send(i, up_piece(t, h), up_piece(t, h))

    for i in range(H - 1):
        piece = lbuf.at[t, nearest[i]]
        lz.wait("w_lz", i, piece)
        go(piece, piece, yes, ly_s, ly_r)
    left_all(lbuf.at[0, pl.ds(0, H - 1)], lz.s)
    left_all(lbuf.at[0], ly_s)
    left_all(gall.at[pl.ds(0, H - 1)], gain_s)

    wx_r, wx_at = [], []
    wpair_r = new_recv()

    def w_across(gt, gh):
        wx_r.append(new_recv())
        wx_at.append((gt, gh))
        go(w_piece(gt, gh, side), w_piece(gt, gh, side), across_dev, w_s, wx_r[-1])

    def w_pair(k):
        gt, gh = wx_at[k]
        got("w_wx", w_piece(gt, gh, 1 - side), wx_r[k])
        go(w_both(gt, gh), w_both(gt, gh), pair_dev, w_s, wpair_r)

    got("w_wy0", w_piece(1 - t, h, side), wy_r[H - 1])
    w_across(1 - t, h)

    def halo(buffer, f0, f_two, two_at, step):
        made = []
        ok_t_send = (t < T - 1) if step == 1 else (t > 0)
        ok_t_recv = (t > 0) if step == 1 else (t < T - 1)
        kt = step % T

        def part_of(fs, n_f, r0, n_r):
            return buffer.at[pl.ds(fs, n_f), pl.ds(r0, n_r)]

        for kt_, kh_, ok_s, ok_r, src, dst in (
            (kt, 0, ok_t_send, ok_t_recv, part_of(f_two, 2, 1, R), part_of(two_at, 2, 1, R)),
            (0, 1, h < H - 1, h > 0, part_of(f0, F, R, 1), part_of(f0, F, 0, 1)),
            (0, H - 1, h > 0, h < H - 1, part_of(f0, F, 1, 1), part_of(f0, F, R + 1, 1)),
            (kt, 1, ok_t_send & (h < H - 1), ok_t_recv & (h > 0),
             part_of(f_two, 2, R, 1), part_of(two_at, 2, 0, 1)),
            (kt, H - 1, ok_t_send & (h > 0), ok_t_recv & (h < H - 1),
             part_of(f_two, 2, 1, 1), part_of(two_at, 2, R + 1, 1)),
        ):
            c = copy(src, dst, at(kt_, kh_), new_send(), new_recv())
            pl.when(ok_s)(c.start)
            made.append((c, ok_s, ok_r))
        return made

    uy_r = [new_recv() for _ in range(H - 1)]
    ux_r = [new_recv(), new_recv()]
    upair_r = new_recv()
    for i in range(H - 1):
        piece = up_piece(t, nearest[i])
        uz.wait("w_uz", i, piece)
        go(piece, piece, yes, u_s, uy_r[i])
        go(piece, piece, across_dev, u_s, ux_r[0])

    got("w_ly", lbuf.at[0], ly_r)
    got("w_gain", gall.at[pl.ds(0, H - 1)], gain_r)
    wz = Along(w_s)
    own_c.wait()
    for i in range(W_EARLY):
        wz.send(i, w_mine, w_mine)
    cot_halo = halo(cb, 0, 0, F, -1)

    per_l = H * CH // GROUPS
    cells_l = FL * Rl * Cl
    count_l = cells_l * per_l
    xs, rows = [], []
    for k in range(H):
        x = lbuf[:, k].astype(F32).reshape(cells_l, CH)
        rows += [jnp.sum(x, 0, keepdims=True), jnp.sum(x * x, 0, keepdims=True)]
    total = over_groups(jnp.concatenate(rows, 0), per_l) / count_l
    for k in range(H):
        mean = total[2 * k : 2 * k + 1]
        inv = lax.rsqrt(total[2 * k + 1 : 2 * k + 2] - mean * mean + epsilon)
        x = lbuf[:, k].astype(F32).reshape(cells_l, CH)
        v = (x - mean) * inv * gall[k, 0:1] + gall[k, 1:2]
        lane = k * CH % U
        abuf[k * CH // U, 2 : 2 + FL, 1 : 1 + Rl, :, lane : lane + CH] = (
            (v * jax.nn.sigmoid(v)).astype(BF16).reshape(FL, Rl, Cl, CH)
        )

    own_wl.wait()

    def window(chunk, tap):
        lag, dr = tap // 9, (tap // 3) % 3
        return abuf[chunk, pl.ds(lag, FL), pl.ds(dr, Rl)].reshape(cells_l, U)

    def w_rows(chunk, tap):
        return wl[pl.ds(pl.multiple_of((tap * T + chunk - 27 * t) * U, U), U), :]

    with scope("c_latent"):
        sums = None
        for g in range(4):
            tap = jnp.where(t == 0, 3 * g, 15 + 3 * g)
            for chunk in range(T):
                k3 = jnp.concatenate([w_rows(chunk, tap + dc) for dc in range(3)], 1)
                term = jnp.dot(window(chunk, tap), k3, preferred_element_type=F32)
                sums = term if sums is None else sums + term
        alone = jnp.where(t == 0, 12, 14)
        k2 = jnp.concatenate([w_rows(t, alone), w_rows(t, 13)], 1)
        both = jnp.dot(window(t, alone), k2, preferred_element_type=F32)
        lone = both[:, :CH] + jnp.dot(
            window(1 - t, alone), w_rows(1 - t, alone), preferred_element_type=F32
        )
        first = sums[:, :CH] + jnp.where(t == 0, lone, 0.0)
        last = sums[:, 2 * CH :] + jnp.where(t == 0, 0.0, lone)
        mixed = (
            column_shift(first, Cl, 1) + sums[:, CH : 2 * CH] + both[:, CH:]
            + column_shift(last, Cl, -1)
        )
        partf[...] = mixed.reshape(FL, Rl, Cl, CH)
        partf[pl.ds(t * Fl, Fl)] += lbuf[t, h].astype(F32)
        part[...] = partf[...].astype(BF16)
    p_s, p_r = new_send(), new_recv()
    for kt, kh in peers:
        dev = at(kt, kh)
        go(part.at[pl.ds(dev[1] * Fl, Fl), pl.ds(dev[2] * band, band)],
           parts_in.at[kt * H + kh], dev, p_s, p_r)
    for i in range(W_EARLY, H - 1):
        wz.send(i, w_mine, w_mine)

    def w_height(i):
        piece = w_piece(t, nearest[i], side)
        wz.wait("w_wz", i, piece)
        go(piece, piece, yes, w_s, wy_r[i])
        w_across(t, nearest[i])

    for i in range(H - 1):
        piece = up_piece(1 - t, nearest[i])
        got("w_uy", piece, uy_r[i])
        go(piece, piece, across_dev, u_s, ux_r[1])
    w_height(0)
    for k in range(2):
        gt = t if k == 0 else 1 - t
        got("w_ux", upw.at[pl.ds(0, (H - 1) * up_rows), pl.ds(0, up_cols)], ux_r[k])
        for i in range(H - 1):
            piece = up_piece(gt, nearest[i], 2)
            go(piece, piece, pair_dev, u_s, upair_r)
    for i in range(1, W_EARLY):
        w_height(i)
    got("w_upair", upw.at[pl.ds(0, (H - 1) * CH), pl.ds(0, 4 * C2)], upair_r)
    got("w_parts", parts_in.at[pl.ds(1, N - 1)], p_r)
    left_all(parts_in.at[pl.ds(1, N - 1)], p_s)
    left_all(upw.at[pl.ds(0, (H - 1) * CH)], u_s)

    cells_b = Fl * band * Cl
    with scope("c_up"):
        parts_own = partf[pl.ds(t * Fl, Fl), pl.ds(h * band, band)]
        expanded = jnp.zeros((cells_b, 8 * C2), F32)
        for kh in range(H):
            value = parts_own if kh == 0 else parts_in[kh].astype(F32)
            for kt in range(1, T):
                value = value + parts_in[kt * H + kh].astype(F32)
            refined = value.reshape(cells_b, CH).astype(BF16)
            source = lax.rem(h + H - kh, H)
            expanded = expanded + jnp.dot(
                refined, upw[pl.ds(pl.multiple_of(source * CH, CH), CH), :],
                preferred_element_type=F32,
            )
        expanded = expanded.astype(BF16).astype(F32)
        for f in range(Fl):
            for r in range(band):
                for p in range(2):
                    for qq in range(2):
                        for s in range(2):
                            first = (f * band + r) * Cl
                            col = ((p * 2 + qq) * 2 + s) * C2
                            for n in range(C2 // 128):
                                lace[
                                    n, pl.ds(((2 * f + p) * R + 2 * r + qq) * C + s, Cl, stride=2), :
                                ] = expanded[first : first + Cl, col + n * 128 : col + (n + 1) * 128]

        cells = F * R * C
        me = t * H + h
        up = jnp.concatenate([lace[n] for n in range(C2 // 128)], axis=1)
        stat2[me] = two_rows(jnp.sum(up, 0, keepdims=True), jnp.sum(up * up, 0, keepdims=True))
        ub[2 : 2 + F, 1 : 1 + R] = up.astype(BF16).reshape(F, R, C, C2)
    s2_s, s2_r = new_send(), new_recv()
    for kt, kh in peers:
        go(stat2.at[me], stat2.at[me], at(kt, kh), s2_s, s2_r)
    left_all(stat2.at[pl.ds(0, N - 1)], s2_s)
    up_halo = halo(ub, 2, F, 0, 1)

    for i in range(W_EARLY, H - 1):
        w_height(i)
    with scope("w_cothalo"):
        for made, _, ok in cot_halo:
            pl.when(ok)(made.wait_recv)
    wide = cb[0:F].astype(F32).reshape(F * (R + 2) * C, C2)
    cot3[:, :, :, 0:C2] = column_shift(wide, C, -1).astype(BF16).reshape(F, R + 2, C, C2)
    cot3[:, :, :, C2 : 2 * C2] = cb[0:F]
    cot3[:, :, :, 2 * C2 :] = column_shift(wide, C, 1).astype(BF16).reshape(F, R + 2, C, C2)

    got("w_s2", stat2.at[pl.ds(0, N - 1)], s2_r)
    per_b = C2 // GROUPS
    count_b = cells * per_b * N
    total = stat2[0]
    for k in range(1, N):
        total = total + stat2[k]
    total = over_groups(total, per_b) / count_b
    mean_b = total[0:1]
    inv_b = lax.rsqrt(total[1:2] - mean_b * mean_b + epsilon)

    def activate(values):
        normed = (values - mean_b) * inv_b * gain_b[...] + shift_b[...]
        return (normed * jax.nn.sigmoid(normed)).astype(BF16)

    with scope("c_gw"):
        own = activate(ub[2 : 2 + F, 1 : 1 + R].astype(F32).reshape(cells, C2))
        ab[2 : 2 + F, 1 : 1 + R] = own.reshape(F, R, C, C2)
        for dr in range(3):
            term = lax.dot_general(
                own, cot3[:, 2 - dr : 2 - dr + R].reshape(cells, 3 * C2),
                (((0,), (0,)), ((), ())), preferred_element_type=F32,
            )
            for dc in range(3):
                gw[(dr * 3 + dc) * C2 : (dr * 3 + dc + 1) * C2, :] = (
                    term[:, dc * C2 : (dc + 1) * C2].astype(BF16)
                )
    out_rows = 9 * C2 // N
    y_rows = out_rows * H

    def g_rows(gt, gh):
        return gw.at[pl.ds(pl.multiple_of((gt * H + gh) * out_rows, out_rows), out_rows)]

    def ahead(kh):
        return lax.rem(h + kh, H)

    order = [*range(H // 2, H), *range(1, H // 2), 0]
    gy_s, gz_s, gz_r = new_send(), new_send(), new_recv()
    gy_r = {kh: new_recv() for kh in order}
    for kh in order:
        go(g_rows(1 - t, ahead(kh)), gy.at[kh], yes, gy_s, gy_r[kh])
    left_all(gy, gy_s)

    for i in range(H - 1):
        got("w_wy", w_piece(1 - t, nearest[i], side), wy_r[i])
        w_across(1 - t, nearest[i])
    with scope("w_uphalo"):
        for made, _, ok in up_halo:
            pl.when(ok)(made.wait_recv)
    with scope("c_halo"):
        for rows_at, n_rows, ok in ((0, 1, h > 0), (R + 1, 1, h < H - 1)):
            @pl.when(ok)
            def _():
                v = ub[2 : 2 + F, rows_at : rows_at + n_rows].astype(F32).reshape(F * n_rows * C, C2)
                ab[2 : 2 + F, rows_at : rows_at + n_rows] = activate(v).reshape(F, n_rows, C, C2)
        for rows_at, n_rows, ok in (
            (1, R, t > 0), (0, 1, (t > 0) & (h > 0)), (R + 1, 1, (t > 0) & (h < H - 1))
        ):
            @pl.when(ok)
            def _():
                v = ub[0:2, rows_at : rows_at + n_rows].astype(F32).reshape(2 * n_rows * C, C2)
                ab[0:2, rows_at : rows_at + n_rows] = activate(v).reshape(2, n_rows, C, C2)

    def g_on(kh):
        got("w_gy", gy.at[kh], gy_r[kh])
        start = pl.multiple_of((t * H + ahead(kh)) * out_rows, out_rows)
        total = gy[kh].astype(F32) + gw[pl.ds(start, out_rows), :].astype(F32)
        if kh == 0:
            grad_w[...] = total
        else:
            gs[kh] = total.astype(BF16)
            go(gs.at[kh], gz.at[kh], at(0, kh), gz_s, gz_r)

    for k in range(len(wx_at) - 2):
        w_pair(k)
    for k, kh in enumerate(order[:-1]):
        if k < 2:
            w_pair(len(wx_at) - 2 + k)
        g_on(kh)
    left_all(gs.at[pl.ds(1, H - 1)], gz_s)
    got("w_wpair", wb.at[pl.ds(0, (N - 1) * shard), pl.ds(0, C2 // 2)], wpair_r)
    left_all(wb.at[pl.ds(0, (2 * (H - 1) + 1 + 3 * (N - 1)) * w_half // 2)], w_s)

    with scope("c_gradtap"):
        wide = None
        for j in range(9):
            lag, dr = j // 3, j % 3
            win = cb[2 - lag : 2 - lag + F, 2 - dr : 2 - dr + R].reshape(cells, C2)
            term = lax.dot_general(
                win, wb[j * 3 * C2 : (j + 1) * 3 * C2, :], (((1,), (1,)), ((), ())),
                preferred_element_type=F32,
            )
            wide = term if wide is None else wide + term
        grad_active = (
            column_shift(wide[:, :C2], C, -1) + wide[:, C2 : 2 * C2]
            + column_shift(wide[:, 2 * C2 :], C, 1)
        )
    standard = (ub[2 : 2 + F, 1 : 1 + R].astype(F32).reshape(cells, C2) - mean_b) * inv_b
    std[...] = standard
    normed = standard * gain_b[...] + shift_b[...]
    sigmoid = jax.nn.sigmoid(normed)
    grad_normed = grad_active * sigmoid * (1.0 + normed * (1.0 - sigmoid))
    stat3[me] = two_rows(
        jnp.sum(grad_normed * standard, 0, keepdims=True), jnp.sum(grad_normed, 0, keepdims=True)
    )
    s3_s, s3_r = new_send(), new_recv()
    for kt, kh in peers:
        go(stat3.at[me], stat3.at[me], at(kt, kh), s3_s, s3_r)
    left_all(stat3.at[pl.ds(0, N - 1)], s3_s)
    tmp[...] = grad_normed * gain_b[...]

    with scope("c_tap"):
        wide = None
        for j in range(9):
            lag, dr = j // 3, j % 3
            win = ab[lag : lag + F, dr : dr + R].reshape(cells, C2)
            k3 = jnp.concatenate(
                [wb[(j * 3 + dc) * C2 : (j * 3 + dc + 1) * C2, :] for dc in range(3)], 1
            )
            term = jnp.dot(win, k3, preferred_element_type=F32)
            wide = term if wide is None else wide + term
        decoded[...] = (
            (column_shift(wide[:, :C2], C, 1) + wide[:, C2 : 2 * C2]
             + column_shift(wide[:, 2 * C2 :], C, -1)
             + ub[2 : 2 + F, 1 : 1 + R].astype(F32).reshape(cells, C2))
            .astype(BF16).reshape(F, R, C, C2)
        )
    g_on(0)

    got("w_s3", stat3.at[pl.ds(0, N - 1)], s3_r)
    total = stat3[0]
    for k in range(1, N):
        total = total + stat3[k]
    grad_gs[...] = total
    means = over_groups(total * gain_b[...], per_b) / count_b
    corrected = (tmp[...] - means[1:2] - std[...] * means[0:1]) * inv_b
    grad_up[...] = (
        cb[0:F, 1 : 1 + R].astype(F32).reshape(cells, C2) + corrected
    ).astype(BF16).reshape(F, R, C, C2)

    got("w_gz", gz.at[pl.ds(1, H - 1)], gz_r)
    result = grad_w[...]
    for kh in range(1, H):
        result = result + gz[kh].astype(F32)
    grad_w[...] = result

    with scope("w_send"):
        for ref, s_sem in left:
            copy(ref, ref, pair_dev, s_sem, recv_sem.at[0]).wait_send()
        for made, ok, _ in cot_halo + up_halo:
            pl.when(ok)(made.wait_send)
    assert counts == [n_send, n_recv], counts


def finish_kernel(decoded, grad_up, grad_w, grad_gs, out_d, out_u, out_w, out_g, out_s, sems):
    moves = [
        pltpu.make_async_copy(src, dst, sems.at[k])
        for k, (src, dst) in enumerate((
            (decoded, out_d), (grad_up, out_u), (grad_w, out_w),
            (grad_gs.at[pl.ds(0, 1)], out_g), (grad_gs.at[pl.ds(1, 1)], out_s),
        ))
    ]
    for move in moves:
        move.start()
    for move in moves:
        move.wait()


def stay(array):
    return pltpu.with_memory_space_constraint(array, pltpu.HBM)


def local_block(shape, *args):
    (latent, gain_l, shift_l, w_l, up_w, gain_b, shift_b, w_b, cot) = args
    T, H = shape["tm"], shape["height"]
    Fl, Rl, Cl, CH = latent.shape
    F, R, C, C2 = cot.shape
    N = T * H
    U = H * CH // T
    fits = (
        shape["dp"] % 4 == 0 and T == 2
        and CH % 128 == 0 and U % CH == 0
        and w_b.shape[0] % 32 == 0 and (CH // T) % 16 == 0
        and (9 * C2) % (16 * N) == 0 and C2 % 256 == 0
        and Cl % 16 == 0 and w_l.shape[0] == 27 * U and F >= 2
    )
    if not fits:
        return local(*args)
    sizes = (T, H, Fl, Rl, Cl, CH, C2, F, R, C)
    n_send = 20
    n_recv = 20 + 4 * (H - 1) + 2 * H + N - 1
    FL = T * Fl
    band = Rl // H
    cells = F * R * C
    out_rows = 9 * C2 // N
    vmem = pl.BlockSpec(memory_space=pltpu.VMEM)
    hbm = pl.BlockSpec(memory_space=pltpu.HBM)
    flops = 2 * (FL * Rl * Cl * w_l.size + 2 * cells * 27 * C2 * C2 + cells * 9 * C2 * C2)
    outs = pl.pallas_call(
        functools.partial(block_kernel, sizes, n_send, n_recv),
        out_shape=(
            jax.ShapeDtypeStruct(cot.shape, BF16),
            jax.ShapeDtypeStruct(cot.shape, BF16),
            jax.ShapeDtypeStruct((out_rows, C2), F32),
            jax.ShapeDtypeStruct((8, C2), F32),
        ),
        in_specs=[hbm] * 9,
        out_specs=(vmem,) * 4,
        scratch_shapes=[
            pltpu.VMEM((T, H, Fl, Rl, Cl, CH), BF16),
            pltpu.VMEM((H, 2, CH), F32),
            pltpu.VMEM((1, C2), F32),
            pltpu.VMEM((1, C2), F32),
            pltpu.VMEM(w_l.shape, BF16),
            pltpu.VMEM((T, FL + 2, Rl + 2, Cl, U), BF16),
            pltpu.VMEM((FL, Rl, Cl, CH), BF16),
            pltpu.VMEM((FL, Rl, Cl, CH), F32),
            pltpu.VMEM((N, Fl, band, Cl, CH), BF16),
            pltpu.VMEM((N, 8, C2), F32),
            pltpu.VMEM((N, 8, C2), F32),
            pltpu.VMEM((H * CH, 8 * C2), BF16),
            pltpu.VMEM((27 * C2, C2), BF16),
            pltpu.VMEM((F + 2, R + 2, C, C2), BF16),
            pltpu.VMEM((cells, C2), F32),
            pltpu.VMEM((F + 2, R + 2, C, C2), BF16),
            pltpu.VMEM((F + 2, R + 2, C, C2), BF16),
            pltpu.VMEM((F, R + 2, C, 3 * C2), BF16),
            pltpu.VMEM((9 * C2, C2), BF16),
            pltpu.VMEM((H, out_rows, C2), BF16),
            pltpu.VMEM((H, out_rows, C2), BF16),
            pltpu.VMEM((H, out_rows, C2), BF16),
            pltpu.VMEM((cells, C2), F32),
            pltpu.VMEM((C2 // 128, cells, 128), F32),
            pltpu.SemaphoreType.DMA((n_send,)),
            pltpu.SemaphoreType.DMA((n_recv,)),
            pltpu.SemaphoreType.DMA((9,)),
        ],
        compiler_params=pltpu.CompilerParams(
            collective_id=0, has_side_effects=True, vmem_limit_bytes=VMEM_LIMIT
        ),
        cost_estimate=pl.CostEstimate(flops=flops, bytes_accessed=1 << 23, transcendentals=0),
    )(
        stay(latent), stay(gain_l.reshape(1, -1)), stay(shift_l.reshape(1, -1)), stay(w_l), stay(up_w),
        stay(gain_b.reshape(1, -1)), stay(shift_b.reshape(1, -1)), stay(w_b), stay(cot),
    )
    row = jax.ShapeDtypeStruct((1, C2), F32)
    done = pl.pallas_call(
        finish_kernel,
        out_shape=tuple(jax.ShapeDtypeStruct(a.shape, a.dtype) for a in outs[:3]) + (row, row),
        in_specs=[vmem] * 4,
        out_specs=(hbm,) * 5,
        scratch_shapes=[pltpu.SemaphoreType.DMA((5,))],
        compiler_params=pltpu.CompilerParams(vmem_limit_bytes=1 << 20),
        cost_estimate=pl.CostEstimate(flops=0, bytes_accessed=1 << 20, transcendentals=0),
    )(*outs)
    return done[0], done[1], done[2], done[3].reshape(C2), done[4].reshape(C2)


def solution(mesh):
    return jax.shard_map(
        functools.partial(local_block, dict(mesh.shape)),
        mesh=mesh,
        in_specs=(
            P(("dp", "tm"), None, None, "height"),
            P("height"),
            P("height"),
            P("tm", "height"),
            P("height", None),
            P(),
            P(),
            P(("tm", "height"), None),
            P(("dp", "tm"), "height", None, None),
        ),
        out_specs=(
            P(("dp", "tm"), "height", None, None),
            P(("dp", "tm"), "height", None, None),
            P(("dp", "tm", "height"), None),
            P("dp"),
            P("dp"),
        ),
        check_vma=False,
    )
```

```python
import functools

import jax
import jax.numpy as jnp
from jax import lax
from jax.experimental import pallas as pl
from jax.experimental.pallas import tpu as pltpu
from jax.sharding import PartitionSpec as P

C1 = 512
GROUPS = 32


epsilon = 1e-06


def shifted(block, axis, distance):
    devices = range(lax.axis_size(axis))
    route = [(i - distance, i) for i in devices if i - distance in devices]
    return lax.ppermute(block, axis, route)


def extended_2(cells, sides, width):
    for axis, dim in sides:
        count = lax.axis_size(axis)
        ends = count - 1
        head = lax.slice_in_dim(cells, 0, width, axis=dim)
        tail = lax.slice_in_dim(cells, cells.shape[dim] - width, cells.shape[dim], axis=dim)
        cells = jnp.concatenate(
            [
                lax.ppermute(tail, axis, [(i, (i + 1) % count) for i in range(ends)]),
                cells,
                lax.ppermute(head, axis, [((i + 1) % count, i) for i in range(ends)]),
            ],
            axis=dim,
        )
    return cells


def standardize(values, mean_value, inverse, groups):
    shape_full = values.shape
    grouped = values.reshape(shape_full[:-1] + (groups, shape_full[-1] // groups))
    return ((grouped - mean_value[:, None]) * inverse[:, None]).reshape(shape_full)


def causal_taps(padded, weight, frames, rows, cols):
    channels_in = padded.shape[-1]
    summed = jnp.zeros((frames * rows * cols, weight.shape[1]), jnp.float32)
    for lag_step in range(3):
        for row_step in range(3):
            for col_step in range(3):
                tap_index = (lag_step * 3 + row_step) * 3 + col_step
                window = padded[
                    lag_step : lag_step + frames,
                    row_step : row_step + rows,
                    col_step : col_step + cols,
                ]
                kernel = weight[tap_index * channels_in : (tap_index + 1) * channels_in]
                summed = summed + jnp.dot(
                    window.reshape(-1, channels_in), kernel, preferred_element_type=jnp.float32
                )
    return summed.reshape(frames, rows, cols, weight.shape[1])


def transposed_taps(padded, weight, frames, rows, cols):
    channels_out = padded.shape[-1]
    channels_in = weight.shape[0] // 27
    summed = jnp.zeros((frames * rows * cols, channels_in), jnp.float32)
    for lag_step in range(3):
        for row_step in range(3):
            for col_step in range(3):
                tap_index = (lag_step * 3 + row_step) * 3 + col_step
                window = padded[
                    2 - lag_step : 2 - lag_step + frames,
                    2 - row_step : 2 - row_step + rows,
                    2 - col_step : 2 - col_step + cols,
                ]
                kernel = weight[tap_index * channels_in : (tap_index + 1) * channels_in]
                summed = summed + lax.dot_general(
                    window.reshape(-1, channels_out),
                    kernel,
                    (((1,), (1,)), ((), ())),
                    preferred_element_type=jnp.float32,
                )
    return summed.reshape(frames, rows, cols, channels_in)


def weight_terms(padded, grads, frames, rows, cols):
    channels_in = padded.shape[-1]
    flat_grads = grads.reshape(-1, grads.shape[-1])
    blocks = []
    for row_step in range(3):
        for col_step in range(3):
            window = padded[2 : 2 + frames, row_step : row_step + rows, col_step : col_step + cols]
            blocks.append(
                lax.dot_general(
                    window.reshape(-1, channels_in),
                    flat_grads,
                    (((0,), (0,)), ((), ())),
                    preferred_element_type=jnp.float32,
                )
            )
    return jnp.concatenate(blocks, 0)


def local(
    latent,
    gain_latent,
    shift_latent,
    conv_latent,
    up_weight,
    gain_block,
    shift_block,
    conv_block,
    cotangent,
):
    per_group = C1 // GROUPS
    groups_here = latent.shape[-1] // per_group
    latent_f32 = latent.astype(jnp.float32)
    grouped = latent_f32.reshape(-1, groups_here, per_group)
    first_sums = jnp.sum(grouped, axis=(0, 2))
    second_sums = jnp.sum(grouped * grouped, axis=(0, 2))
    first_totals, second_totals = lax.psum((first_sums, second_sums), "tm")
    count_latent = grouped.shape[0] * per_group * lax.axis_size("tm")
    mean_latent = first_totals / count_latent
    inverse_latent = lax.rsqrt(second_totals / count_latent - mean_latent * mean_latent + epsilon)
    normed = (
        standardize(latent_f32, mean_latent, inverse_latent, groups_here) * gain_latent
        + shift_latent
    )
    active = jax.nn.silu(normed).astype(jnp.bfloat16)
    earlier = shifted(active, "tm", 1)
    extended = jnp.concatenate([earlier, active], 0)
    all_channels = lax.all_gather(extended, "height", axis=3, tiled=True)
    padded = jnp.pad(all_channels, ((0, 0), (1, 1), (1, 1), (0, 0)))
    latent_weight = lax.all_gather(conv_latent, "tm", axis=0, tiled=True)
    frames_latent, rows_latent, cols_latent = (latent.shape[0], latent.shape[1], latent.shape[2])
    mixed = causal_taps(padded, latent_weight, frames_latent, rows_latent, cols_latent)
    refined = (latent_f32 + mixed).astype(jnp.bfloat16)
    band_rows = rows_latent // lax.axis_size("height")
    own_band = lax.all_to_all(refined, "height", split_axis=1, concat_axis=3, tiled=True)
    flat_band = own_band.reshape(-1, own_band.shape[-1])
    expanded = jnp.dot(
        flat_band,
        lax.all_gather(up_weight, "height", axis=0, tiled=True),
        preferred_element_type=jnp.float32,
    )
    channels_block = up_weight.shape[1] // 8
    spread = expanded.reshape(frames_latent, band_rows, cols_latent, 2, 2, 2, channels_block)
    spread = spread.transpose(0, 3, 1, 4, 2, 5, 6)
    upsampled = spread.reshape(
        2 * frames_latent, 2 * band_rows, 2 * cols_latent, channels_block
    ).astype(jnp.bfloat16)
    frames_block, rows_block, cols_block = (
        upsampled.shape[0],
        upsampled.shape[1],
        upsampled.shape[2],
    )
    up_f32 = upsampled.astype(jnp.float32)
    per_block = channels_block // GROUPS
    grouped_block = up_f32.reshape(-1, GROUPS, per_block)
    block_first = jnp.sum(grouped_block, axis=(0, 2))
    block_second = jnp.sum(grouped_block * grouped_block, axis=(0, 2))
    block_first, block_second = lax.psum((block_first, block_second), ("tm", "height"))
    count_block = grouped_block.shape[0] * per_block * lax.axis_size("tm") * lax.axis_size("height")
    mean_block = block_first / count_block
    inverse_block = lax.rsqrt(block_second / count_block - mean_block * mean_block + epsilon)
    standard = standardize(up_f32, mean_block, inverse_block, GROUPS)
    normed_block = standard * gain_block + shift_block
    active_block = jax.nn.silu(normed_block).astype(jnp.bfloat16)
    before = shifted(active_block[-2:], "tm", 1)
    ext_block = jnp.concatenate([before, active_block], 0)
    beside_all = extended_2(ext_block, (("height", 1),), 1)
    padded_block = jnp.pad(beside_all, ((0, 0), (0, 0), (1, 1), (0, 0)))
    block_weight = lax.all_gather(conv_block, ("tm", "height"), axis=0, tiled=True)
    mixed_block = causal_taps(padded_block, block_weight, frames_block, rows_block, cols_block)
    decoded = (up_f32 + mixed_block).astype(jnp.bfloat16)
    after = shifted(cotangent[:2], "tm", -1)
    grad_ext = jnp.concatenate([cotangent, after], 0)
    grad_around = extended_2(grad_ext, (("height", 1),), 1)
    grad_padded = jnp.pad(grad_around, ((0, 0), (0, 0), (1, 1), (0, 0)))
    grad_active = transposed_taps(grad_padded, block_weight, frames_block, rows_block, cols_block)
    local_terms = weight_terms(padded_block, cotangent, frames_block, rows_block, cols_block)
    grad_weight = lax.psum_scatter(local_terms, ("tm", "height"), scatter_dimension=0, tiled=True)
    sigmoid = jax.nn.sigmoid(normed_block)
    grad_normed = grad_active * sigmoid * (1.0 + normed_block * (1.0 - sigmoid))
    flat_grad = grad_normed.reshape(-1, channels_block)
    flat_standard = standard.reshape(-1, channels_block)
    grad_shift, grad_gain = lax.psum(
        (jnp.sum(flat_grad, axis=0), jnp.sum(flat_grad * flat_standard, axis=0)), ("tm", "height")
    )
    first_mean = jnp.sum((gain_block * grad_shift).reshape(GROUPS, per_block), axis=1) / count_block
    second_mean = jnp.sum((gain_block * grad_gain).reshape(GROUPS, per_block), axis=1) / count_block
    grouped_grad = (grad_normed * gain_block).reshape(-1, GROUPS, per_block)
    grouped_standard = standard.reshape(-1, GROUPS, per_block)
    corrected = (
        grouped_grad - first_mean[:, None] - grouped_standard * second_mean[:, None]
    ) * inverse_block[:, None]
    grad_upsampled = (cotangent.astype(jnp.float32) + corrected.reshape(cotangent.shape)).astype(
        jnp.bfloat16
    )
    return (decoded, grad_upsampled, grad_weight, grad_gain, grad_shift)


MESH = pl.DeviceIdType.MESH
VMEM_LIMIT = 32 * 1024 * 1024
CUTS = 2
F32 = jnp.float32
BF16 = jnp.bfloat16


def group_matrix(channels, per):
    row = lax.broadcasted_iota(jnp.int32, (channels, channels), 0) // per
    col = lax.broadcasted_iota(jnp.int32, (channels, channels), 1) // per
    return (row == col).astype(F32)


def over_groups(rows, per):
    return jnp.dot(
        rows,
        group_matrix(rows.shape[-1], per),
        precision=lax.Precision.HIGHEST,
        preferred_element_type=F32,
    )


def column_shift(cells, cols, step):
    count = cells.shape[0]
    column = lax.broadcasted_iota(jnp.int32, cells.shape, 0) % cols
    edge = 0 if step == 1 else cols - 1
    return jnp.where(column == edge, 0.0, pltpu.roll(cells, step % count, 0))


def two_rows(first, second):
    width = first.shape[-1]
    row = lax.broadcasted_iota(jnp.int32, (8, width), 0)
    return jnp.where(row == 0, first, jnp.where(row == 1, second, 0.0))


def block_kernel(sizes, n_send, n_recv, *refs):
    (T, H, Fl, Rl, Cl, CH, C2, F, R, C) = sizes
    (
        latent, gain_in, shift_in, w_l, up_w, gain_b_in, shift_b_in, w_b, cot,
        decoded, grad_up, grad_w, grad_gs,
        lbuf, gall, gain_b, shift_b, wl, abuf, part, partf, parts_in, stat2, stat3, upw, wb,
        ub, std, ab, cb, cot3, gw, gy, gs, gz, tmp, lace, send_sem, recv_sem, local_sem,
    ) = refs
    d, t, h = lax.axis_index("dp"), lax.axis_index("tm"), lax.axis_index("height")
    N = T * H
    FL = T * Fl
    U = H * CH // T
    band = Rl // H
    q = lax.rem(d, 4)
    half, side = lax.rem(q, 2), q // 2
    pair = d + 1 - 2 * half
    across = d + 2 - 4 * side
    counts = [0, 0]

    def new_send():
        counts[0] += 1
        return send_sem.at[counts[0] - 1]

    def new_recv(n=1):
        counts[1] += n
        return recv_sem.at[counts[1] - 1] if n == 1 else counts[1] - n

    def at(kt, kh):
        return (d, lax.rem(t + kt, T), lax.rem(h + kh, H))

    def copy(src, dst, device, s_sem, r_sem):
        return pltpu.make_async_remote_copy(
            src_ref=src, dst_ref=dst, send_sem=s_sem, recv_sem=r_sem,
            device_id=device, device_id_type=MESH,
        )

    def go(*what):
        copy(*what).start()

    pair_dev, across_dev = (pair, t, h), (across, t, h)
    left = []

    def got(name, ref, r_sem):
        with scope(name):
            copy(ref, ref, pair_dev, send_sem.at[0], r_sem).wait_recv()

    def left_all(ref, s_sem):
        left.append((ref, s_sem))

    def scope(name):
        return jax.named_scope(name)

    peers = [(kt, kh) for kh in [*range(H // 2, H), *range(1, H // 2), 0] for kt in range(T) if kt or kh]
    shard = w_b.shape[0]

    def local_copy(k, src, dst):
        made = pltpu.make_async_copy(src, dst, local_sem.at[k])
        made.start()
        return made

    def other(i):
        where = 0
        for hh in range(H):
            where = where + jnp.where(h == hh, hh ^ (i + 1), 0)
        return where

    nearest = [other(i) for i in range(H - 1)]

    class Along:
        def __init__(self, s_sem):
            self.s, self.base = s_sem, new_recv(H - 1)

        def send(self, i, src, dst):
            to = nearest[i]
            r = recv_sem.at[self.base + lax.rem(to - h + H, H) - 1]
            go(src, dst, (d, t, to), self.s, r)

        def wait(self, name, i, ref):
            got(name, ref, recv_sem.at[self.base + lax.rem(h - nearest[i] + H, H) - 1])

    own_l = local_copy(0, latent, lbuf.at[t, h])
    cb[...] = jnp.zeros(cb.shape, BF16)
    barrier = pltpu.get_barrier_semaphore()
    for kt, kh in peers:
        pl.semaphore_signal(barrier, inc=1, device_id=at(kt, kh), device_id_type=MESH)
    pl.semaphore_signal(barrier, inc=1, device_id=pair_dev, device_id_type=MESH)
    pl.semaphore_signal(barrier, inc=1, device_id=across_dev, device_id_type=MESH)
    own_w = local_copy(2, w_b, wb.at[pl.ds(pl.multiple_of((t * H + h) * shard, shard), shard)])
    own_g = [
        local_copy(5, gain_in, gall.at[h, pl.ds(0, 1)]),
        local_copy(6, shift_in, gall.at[h, pl.ds(1, 1)]),
        local_copy(7, gain_b_in, gain_b), local_copy(8, shift_b_in, shift_b),
    ]
    own_up = local_copy(1, up_w, upw.at[pl.ds(pl.multiple_of(h * CH, CH), CH)])
    own_c = local_copy(4, cot, cb.at[pl.ds(0, F), pl.ds(1, R)])
    own_wl = local_copy(3, w_l, wl)
    abuf[...] = jnp.zeros(abuf.shape, BF16)
    ab[...] = jnp.zeros(ab.shape, BF16)
    own_l.wait()
    with scope("w_barrier"):
        pl.semaphore_wait(barrier, N + 1)

    yes = at(1, 0)
    w_half = shard // 2
    half_cols = pl.ds(pl.multiple_of(half * (C2 // 2), C2 // 2), C2 // 2)

    def w_piece(gt, gh, piece_side):
        start = pl.multiple_of((gt * H + gh) * shard + piece_side * w_half, w_half)
        return wb.at[pl.ds(start, w_half), half_cols]

    def w_both(gt, gh):
        return wb.at[pl.ds(pl.multiple_of((gt * H + gh) * shard, shard), shard), half_cols]

    up_rows, up_cols = CH // T, 2 * C2

    def up_piece(gt, gh, n=1):
        first = 2 * half + (side if n == 1 else 0)
        return upw.at[
            pl.ds(pl.multiple_of(gh * CH + gt * up_rows, up_rows), up_rows),
            pl.ds(pl.multiple_of(first * up_cols, up_cols), n * up_cols),
        ]

    mine = lbuf.at[t, h]
    lz = Along(new_send())
    ly_s, ly_r = new_send(), new_recv()
    for i in range(H - 1):
        lz.send(i, mine, mine)
    go(mine, mine, yes, ly_s, ly_r)
    own_w.wait()
    w_s = new_send()
    w_mine = w_piece(t, h, side)
    wy_r = [new_recv() for _ in range(H)]
    go(w_both(t, h), w_both(t, h), yes, w_s, wy_r[H - 1])
    for made in own_g:
        made.wait()
    gain_s, gain_r = new_send(), new_recv()
    for kh in range(1, H):
        go(gall.at[h], gall.at[h], at(0, kh), gain_s, gain_r)
    own_up.wait()
    u_s = new_send()
    uz = Along(u_s)

    def up_send(core):
        @pl.when(half == core)
        def _():
            for i in range(H - 1):
                uz.send(i, up_piece(t, h), up_piece(t, h))

    up_send(0)
    for i in range(H - 1):
        if i == 2:
            up_send(1)
        piece = lbuf.at[t, nearest[i]]
        lz.wait("w_lz", i, piece)
        go(piece, piece, yes, ly_s, ly_r)
    left_all(lbuf.at[0, pl.ds(0, H - 1)], lz.s)
    left_all(lbuf.at[0], ly_s)
    left_all(gall.at[pl.ds(0, H - 1)], gain_s)

    wx_r, wx_at = [], []
    wpair_r = new_recv()

    def w_across(gt, gh):
        wx_r.append(new_recv())
        wx_at.append((gt, gh))
        go(w_piece(gt, gh, side), w_piece(gt, gh, side), across_dev, w_s, wx_r[-1])

    def w_pair(k):
        gt, gh = wx_at[k]
        got("w_wx", w_piece(gt, gh, 1 - side), wx_r[k])
        go(w_both(gt, gh), w_both(gt, gh), pair_dev, w_s, wpair_r)


    def halo(buffer, f0, f_two, two_at, step):
        made = []
        ok_t_send = (t < T - 1) if step == 1 else (t > 0)
        ok_t_recv = (t > 0) if step == 1 else (t < T - 1)
        kt = step % T

        def part_of(fs, n_f, r0, n_r):
            return buffer.at[pl.ds(fs, n_f), pl.ds(r0, n_r)]

        for kt_, kh_, ok_s, ok_r, src, dst in (
            (kt, 0, ok_t_send, ok_t_recv, part_of(f_two, 2, 1, R), part_of(two_at, 2, 1, R)),
            (0, 1, h < H - 1, h > 0, part_of(f0, F, R, 1), part_of(f0, F, 0, 1)),
            (0, H - 1, h > 0, h < H - 1, part_of(f0, F, 1, 1), part_of(f0, F, R + 1, 1)),
            (kt, 1, ok_t_send & (h < H - 1), ok_t_recv & (h > 0),
             part_of(f_two, 2, R, 1), part_of(two_at, 2, 0, 1)),
            (kt, H - 1, ok_t_send & (h > 0), ok_t_recv & (h < H - 1),
             part_of(f_two, 2, 1, 1), part_of(two_at, 2, R + 1, 1)),
        ):
            c = copy(src, dst, at(kt_, kh_), new_send(), new_recv())
            pl.when(ok_s)(c.start)
            made.append((c, ok_s, ok_r))
        return made

    uy_r = [new_recv() for _ in range(H - 1)]
    ux_r = [new_recv(), new_recv()]
    upair_r = new_recv()

    def up_height(i):
        piece = up_piece(t, nearest[i])
        uz.wait("w_uz", i, piece)
        go(piece, piece, yes, u_s, uy_r[i])
        go(piece, piece, across_dev, u_s, ux_r[0])

    up_height(0)
    got("w_ly", lbuf.at[0], ly_r)
    got("w_gain", gall.at[pl.ds(0, H - 1)], gain_r)
    up_height(1)
    wz = Along(w_s)
    own_c.wait()
    wz.send(0, w_mine, w_mine)
    wz.send(1, w_mine, w_mine)

    per_l = H * CH // GROUPS
    cells_l = FL * Rl * Cl
    count_l = cells_l * per_l
    xs, rows = [], []
    for k in range(H):
        x = lbuf[:, k].astype(F32).reshape(cells_l, CH)
        rows += [jnp.sum(x, 0, keepdims=True), jnp.sum(x * x, 0, keepdims=True)]
    total = over_groups(jnp.concatenate(rows, 0), per_l) / count_l
    for k in range(H):
        mean = total[2 * k : 2 * k + 1]
        inv = lax.rsqrt(total[2 * k + 1 : 2 * k + 2] - mean * mean + epsilon)
        x = lbuf[:, k].astype(F32).reshape(cells_l, CH)
        v = (x - mean) * inv * gall[k, 0:1] + gall[k, 1:2]
        lane = k * CH % U
        abuf[k * CH // U, 2 : 2 + FL, 1 : 1 + Rl, :, lane : lane + CH] = (
            (v * jax.nn.sigmoid(v)).astype(BF16).reshape(FL, Rl, Cl, CH)
        )

    up_height(2)

    own_wl.wait()

    parts_of = 2
    some = FL // parts_of

    def window(m, chunk, tap):
        lag, dr = tap // 9, (tap // 3) % 3
        return abuf[chunk, pl.ds(lag + m * some, some), pl.ds(dr, Rl)].reshape(some * Rl * Cl, U)

    def w_rows(chunk, tap):
        return wl[pl.ds(pl.multiple_of((tap * T + chunk - 27 * t) * U, U), U), :]

    with scope("c_latent"):
        sums = [None] * parts_of
        for g in range(4):
            tap = jnp.where(t == 0, 3 * g, 15 + 3 * g)
            for chunk in range(T):
                k3 = jnp.concatenate([w_rows(chunk, tap + dc) for dc in range(3)], 1)
                for m in range(parts_of):
                    term = jnp.dot(window(m, chunk, tap), k3, preferred_element_type=F32)
                    sums[m] = term if sums[m] is None else sums[m] + term
        alone = jnp.where(t == 0, 12, 14)
        k2 = jnp.concatenate([w_rows(t, alone), w_rows(t, 13)], 1)
        mixed = []
        for m in range(parts_of):
            both = jnp.dot(window(m, t, alone), k2, preferred_element_type=F32)
            lone = both[:, :CH] + jnp.dot(
                window(m, 1 - t, alone), w_rows(1 - t, alone), preferred_element_type=F32
            )
            first = sums[m][:, :CH] + jnp.where(t == 0, lone, 0.0)
            last = sums[m][:, 2 * CH :] + jnp.where(t == 0, 0.0, lone)
            mixed.append(
                column_shift(first, Cl, 1) + sums[m][:, CH : 2 * CH] + both[:, CH:]
                + column_shift(last, Cl, -1)
            )
        mixed = jnp.concatenate(mixed, 0)
        partf[...] = mixed.reshape(FL, Rl, Cl, CH)
        partf[pl.ds(t * Fl, Fl)] += lbuf[t, h].astype(F32)
        part[...] = partf[...].astype(BF16)
    p_s, p_r = new_send(), new_recv()
    for kt, kh in peers:
        dev = at(kt, kh)
        go(part.at[pl.ds(dev[1] * Fl, Fl), pl.ds(dev[2] * band, band)],
           parts_in.at[kt * H + kh], dev, p_s, p_r)
    cot_halo = halo(cb, 0, 0, F, -1)
    wz.send(2, w_mine, w_mine)

    def w_height(i):
        piece = w_piece(t, nearest[i], side)
        wz.wait("w_wz", i, piece)
        go(piece, piece, yes, w_s, wy_r[i])
        w_across(t, nearest[i])

    piece = up_piece(1 - t, nearest[0])
    got("w_uy", piece, uy_r[0])
    go(piece, piece, across_dev, u_s, ux_r[1])
    piece = up_piece(1 - t, nearest[1])
    got("w_uy", piece, uy_r[1])
    go(piece, piece, across_dev, u_s, ux_r[1])
    piece = up_piece(1 - t, nearest[2])
    got("w_uy", piece, uy_r[2])
    go(piece, piece, across_dev, u_s, ux_r[1])
    got("w_wy0", w_both(1 - t, h), wy_r[H - 1])
    go(w_both(1 - t, h), w_both(1 - t, h), pair_dev, w_s, wpair_r)
    w_height(0)
    got("w_ux", upw.at[pl.ds(0, (H - 1) * up_rows), pl.ds(0, up_cols)], ux_r[0])
    for i in range(H - 1):
        piece = up_piece(t, nearest[i], 2)
        go(piece, piece, pair_dev, u_s, upair_r)
    got("w_ux", upw.at[pl.ds(0, (H - 1) * up_rows), pl.ds(0, up_cols)], ux_r[1])
    for i in range(H - 1):
        piece = up_piece(1 - t, nearest[i], 2)
        go(piece, piece, pair_dev, u_s, upair_r)
    w_height(1)
    got("w_upair", upw.at[pl.ds(0, (H - 1) * CH), pl.ds(0, 4 * C2)], upair_r)
    got("w_parts", parts_in.at[pl.ds(1, N - 1)], p_r)
    left_all(parts_in.at[pl.ds(1, N - 1)], p_s)
    left_all(upw.at[pl.ds(0, (H - 1) * CH)], u_s)

    cells_b = Fl * band * Cl
    with scope("c_up"):
        parts_own = partf[pl.ds(t * Fl, Fl), pl.ds(h * band, band)]
        expanded = jnp.zeros((cells_b, 8 * C2), F32)
        for kh in range(H):
            value = parts_own if kh == 0 else parts_in[kh].astype(F32)
            for kt in range(1, T):
                value = value + parts_in[kt * H + kh].astype(F32)
            refined = value.reshape(cells_b, CH).astype(BF16)
            source = lax.rem(h + H - kh, H)
            expanded = expanded + jnp.dot(
                refined, upw[pl.ds(pl.multiple_of(source * CH, CH), CH), :],
                preferred_element_type=F32,
            )
        expanded = expanded.astype(BF16).astype(F32)
        for f in range(Fl):
            for r in range(band):
                for p in range(2):
                    for qq in range(2):
                        for s in range(2):
                            first = (f * band + r) * Cl
                            col = ((p * 2 + qq) * 2 + s) * C2
                            for n in range(C2 // 128):
                                lace[
                                    n, pl.ds(((2 * f + p) * R + 2 * r + qq) * C + s, Cl, stride=2), :
                                ] = expanded[first : first + Cl, col + n * 128 : col + (n + 1) * 128]

        cells = F * R * C
        me = t * H + h
        up = jnp.concatenate([lace[n] for n in range(C2 // 128)], axis=1)
        stat2[me] = two_rows(jnp.sum(up, 0, keepdims=True), jnp.sum(up * up, 0, keepdims=True))
        ub[2 : 2 + F, 1 : 1 + R] = up.astype(BF16).reshape(F, R, C, C2)
    s2_s, s2_r = new_send(), new_recv()
    for kt, kh in peers:
        go(stat2.at[me], stat2.at[me], at(kt, kh), s2_s, s2_r)
    left_all(stat2.at[pl.ds(0, N - 1)], s2_s)
    up_halo = halo(ub, 2, F, 0, 1)

    w_height(2)
    with scope("w_cothalo"):
        for made, _, ok in cot_halo:
            pl.when(ok)(made.wait_recv)
    wide = cb[0:F].astype(F32).reshape(F * (R + 2) * C, C2)
    cot3[:, :, :, 0:C2] = column_shift(wide, C, -1).astype(BF16).reshape(F, R + 2, C, C2)
    cot3[:, :, :, C2 : 2 * C2] = cb[0:F]
    cot3[:, :, :, 2 * C2 :] = column_shift(wide, C, 1).astype(BF16).reshape(F, R + 2, C, C2)

    got("w_s2", stat2.at[pl.ds(0, N - 1)], s2_r)
    per_b = C2 // GROUPS
    count_b = cells * per_b * N
    total = stat2[0]
    for k in range(1, N):
        total = total + stat2[k]
    total = over_groups(total, per_b) / count_b
    mean_b = total[0:1]
    inv_b = lax.rsqrt(total[1:2] - mean_b * mean_b + epsilon)

    def activate(values):
        normed = (values - mean_b) * inv_b * gain_b[...] + shift_b[...]
        return (normed * jax.nn.sigmoid(normed)).astype(BF16)

    with scope("c_gw"):
        own = activate(ub[2 : 2 + F, 1 : 1 + R].astype(F32).reshape(cells, C2))
        ab[2 : 2 + F, 1 : 1 + R] = own.reshape(F, R, C, C2)
        for dr in range(3):
            term = lax.dot_general(
                own, cot3[:, 2 - dr : 2 - dr + R].reshape(cells, 3 * C2),
                (((0,), (0,)), ((), ())), preferred_element_type=F32,
            )
            for dc in range(3):
                gw[(dr * 3 + dc) * C2 : (dr * 3 + dc + 1) * C2, :] = (
                    term[:, dc * C2 : (dc + 1) * C2].astype(BF16)
                )
    out_rows = 9 * C2 // N
    y_rows = out_rows * H

    cut_rows = out_rows // CUTS

    def cut(c):
        return pl.ds(c * cut_rows, cut_rows)

    def g_at(gt, gh, c):
        start = (gt * H + gh) * out_rows + c * cut_rows
        return pl.ds(pl.multiple_of(start, cut_rows), cut_rows)

    def g_rows(gt, gh, c):
        return gw.at[g_at(gt, gh, c)]

    def ahead(kh):
        return lax.rem(h + kh, H)

    order = [*range(H // 2, H), *range(1, H // 2), 0]
    gy_s, gz_s, gz_r = new_send(), new_send(), new_recv()
    gy_r = {(kh, c): new_recv() for kh in order for c in range(CUTS)}
    for kh in order:
        for c in range(CUTS):
            go(g_rows(1 - t, ahead(kh), c), gy.at[kh, cut(c)], yes, gy_s, gy_r[kh, c])
    left_all(gy, gy_s)

    with scope("w_uphalo"):
        for made, _, ok in up_halo:
            pl.when(ok)(made.wait_recv)
    with scope("c_halo"):
        for rows_at, n_rows, ok in ((0, 1, h > 0), (R + 1, 1, h < H - 1)):
            @pl.when(ok)
            def _():
                v = ub[2 : 2 + F, rows_at : rows_at + n_rows].astype(F32).reshape(F * n_rows * C, C2)
                ab[2 : 2 + F, rows_at : rows_at + n_rows] = activate(v).reshape(F, n_rows, C, C2)
        for rows_at, n_rows, ok in (
            (1, R, t > 0), (0, 1, (t > 0) & (h > 0)), (R + 1, 1, (t > 0) & (h < H - 1))
        ):
            @pl.when(ok)
            def _():
                v = ub[0:2, rows_at : rows_at + n_rows].astype(F32).reshape(2 * n_rows * C, C2)
                ab[0:2, rows_at : rows_at + n_rows] = activate(v).reshape(2, n_rows, C, C2)

    def g_on(kh, c):
        got("w_gy", gy.at[kh, cut(c)], gy_r[kh, c])
        total = gy[kh, c * cut_rows : (c + 1) * cut_rows].astype(F32)
        total = total + gw[g_at(t, ahead(kh), c), :].astype(F32)
        if kh == 0:
            grad_w[c * cut_rows : (c + 1) * cut_rows] = total
        else:
            gs[kh, c * cut_rows : (c + 1) * cut_rows] = total.astype(BF16)
            go(gs.at[kh, cut(c)], gz.at[kh, cut(c)], at(0, kh), gz_s, gz_r)

    steps = [(kh, c) for kh in order for c in range(CUTS)]
    got("w_wy", w_piece(1 - t, nearest[0], side), wy_r[0])
    w_across(1 - t, nearest[0])
    got("w_wy", w_piece(1 - t, nearest[1], side), wy_r[1])
    w_across(1 - t, nearest[1])
    got("w_wy", w_piece(1 - t, nearest[2], side), wy_r[2])
    w_across(1 - t, nearest[2])
    w_pair(0)
    w_pair(1)
    g_on(*steps[0])
    w_pair(2)
    g_on(*steps[1])
    w_pair(3)
    g_on(*steps[2])
    w_pair(4)
    w_pair(5)
    left_all(gs.at[pl.ds(1, H - 1)], gz_s)
    got("w_wpair", wb.at[pl.ds(0, (N - 1) * shard), pl.ds(0, C2 // 2)], wpair_r)
    left_all(wb.at[pl.ds(0, (2 * H + 3 * N - 4) * w_half // 2)], w_s)

    with scope("c_gradtap"):
        sums = {}
        for j in range(9):
            lag, dr = j // 3, j % 3
            win = cb[2 - lag : 2 - lag + F, 2 - dr : 2 - dr + R].reshape(cells, C2)
            for dc in range(3):
                term = lax.dot_general(
                    win, wb[(j * 3 + dc) * C2 : (j * 3 + dc + 1) * C2, :],
                    (((1,), (1,)), ((), ())), preferred_element_type=F32,
                )
                key = (dc, j % 2 if dc == 1 else 0)
                sums[key] = sums[key] + term if key in sums else term
        grad_active = (
            column_shift(sums[0, 0], C, -1) + sums[1, 0] + sums[1, 1]
            + column_shift(sums[2, 0], C, 1)
        )
    standard = (ub[2 : 2 + F, 1 : 1 + R].astype(F32).reshape(cells, C2) - mean_b) * inv_b
    std[...] = standard
    normed = standard * gain_b[...] + shift_b[...]
    sigmoid = jax.nn.sigmoid(normed)
    grad_normed = grad_active * sigmoid * (1.0 + normed * (1.0 - sigmoid))
    stat3[me] = two_rows(
        jnp.sum(grad_normed * standard, 0, keepdims=True), jnp.sum(grad_normed, 0, keepdims=True)
    )
    s3_s, s3_r = new_send(), new_recv()
    for kt, kh in peers:
        go(stat3.at[me], stat3.at[me], at(kt, kh), s3_s, s3_r)
    left_all(stat3.at[pl.ds(0, N - 1)], s3_s)
    tmp[...] = grad_normed * gain_b[...]
    for step in steps[3:4]:
        g_on(*step)

    some = F // 2
    n = some * R * C
    for m in range(2):
        with scope("c_tap"):
            wide = None
            for j in range(9):
                lag, dr = j // 3, j % 3
                k3 = jnp.concatenate(
                    [wb[(j * 3 + dc) * C2 : (j * 3 + dc + 1) * C2, :] for dc in range(3)], 1
                )
                win = ab[lag + m * some : lag + (m + 1) * some, dr : dr + R].reshape(n, C2)
                term = jnp.dot(win, k3, preferred_element_type=F32)
                wide = term if wide is None else wide + term
            decoded[m * some : (m + 1) * some] = (
                (column_shift(wide[:, :C2], C, 1) + wide[:, C2 : 2 * C2]
                 + column_shift(wide[:, 2 * C2 :], C, -1)
                 + ub[2 + m * some : 2 + (m + 1) * some, 1 : 1 + R].astype(F32).reshape(n, C2))
                .astype(BF16).reshape(some, R, C, C2)
            )
        for step in steps[4:6] if m == 0 else steps[6 : -CUTS]:
            g_on(*step)

    got("w_s3", stat3.at[pl.ds(0, N - 1)], s3_r)
    total = stat3[0]
    for k in range(1, N):
        total = total + stat3[k]
    grad_gs[...] = total
    means = over_groups(total * gain_b[...], per_b) / count_b
    corrected = (tmp[...] - means[1:2] - std[...] * means[0:1]) * inv_b
    grad_up[...] = (
        cb[0:F, 1 : 1 + R].astype(F32).reshape(cells, C2) + corrected
    ).astype(BF16).reshape(F, R, C, C2)

    for step in steps[-CUTS:]:
        g_on(*step)
    got("w_gz", gz.at[pl.ds(1, H - 1)], gz_r)
    result = grad_w[...]
    for kh in range(1, H):
        result = result + gz[kh].astype(F32)
    grad_w[...] = result

    with scope("w_send"):
        for ref, s_sem in left:
            copy(ref, ref, pair_dev, s_sem, recv_sem.at[0]).wait_send()
        for made, ok, _ in cot_halo + up_halo:
            pl.when(ok)(made.wait_send)
    assert counts == [n_send, n_recv], counts


def finish_kernel(decoded, grad_up, grad_w, grad_gs, out_d, out_u, out_w, out_g, out_s, sems):
    moves = [
        pltpu.make_async_copy(src, dst, sems.at[k])
        for k, (src, dst) in enumerate((
            (decoded, out_d), (grad_up, out_u), (grad_w, out_w),
            (grad_gs.at[pl.ds(0, 1)], out_g), (grad_gs.at[pl.ds(1, 1)], out_s),
        ))
    ]
    for move in moves:
        move.start()
    for move in moves:
        move.wait()


def stay(array):
    return pltpu.with_memory_space_constraint(array, pltpu.HBM)


def local_block(shape, *args):
    (latent, gain_l, shift_l, w_l, up_w, gain_b, shift_b, w_b, cot) = args
    T, H = shape["tm"], shape["height"]
    Fl, Rl, Cl, CH = latent.shape
    F, R, C, C2 = cot.shape
    N = T * H
    U = H * CH // T
    fits = (
        shape["dp"] % 4 == 0 and T == 2 and H & (H - 1) == 0
        and CH % 128 == 0 and U % CH == 0
        and w_b.shape[0] % 32 == 0 and (CH // T) % 16 == 0
        and (9 * C2) % (16 * CUTS * N) == 0 and C2 % 256 == 0
        and Cl % 16 == 0 and w_l.shape[0] == 27 * U and F >= 2
    )
    if not fits:
        return local(*args)
    sizes = (T, H, Fl, Rl, Cl, CH, C2, F, R, C)
    n_send = 20
    n_recv = 20 + 4 * (H - 1) + (1 + CUTS) * H + N - 2
    FL = T * Fl
    band = Rl // H
    cells = F * R * C
    out_rows = 9 * C2 // N
    vmem = pl.BlockSpec(memory_space=pltpu.VMEM)
    hbm = pl.BlockSpec(memory_space=pltpu.HBM)
    flops = 2 * (FL * Rl * Cl * w_l.size + 2 * cells * 27 * C2 * C2 + cells * 9 * C2 * C2)
    outs = pl.pallas_call(
        functools.partial(block_kernel, sizes, n_send, n_recv),
        out_shape=(
            jax.ShapeDtypeStruct(cot.shape, BF16),
            jax.ShapeDtypeStruct(cot.shape, BF16),
            jax.ShapeDtypeStruct((out_rows, C2), F32),
            jax.ShapeDtypeStruct((8, C2), F32),
        ),
        in_specs=[hbm] * 9,
        out_specs=(vmem,) * 4,
        scratch_shapes=[
            pltpu.VMEM((T, H, Fl, Rl, Cl, CH), BF16),
            pltpu.VMEM((H, 2, CH), F32),
            pltpu.VMEM((1, C2), F32),
            pltpu.VMEM((1, C2), F32),
            pltpu.VMEM(w_l.shape, BF16),
            pltpu.VMEM((T, FL + 2, Rl + 2, Cl, U), BF16),
            pltpu.VMEM((FL, Rl, Cl, CH), BF16),
            pltpu.VMEM((FL, Rl, Cl, CH), F32),
            pltpu.VMEM((N, Fl, band, Cl, CH), BF16),
            pltpu.VMEM((N, 8, C2), F32),
            pltpu.VMEM((N, 8, C2), F32),
            pltpu.VMEM((H * CH, 8 * C2), BF16),
            pltpu.VMEM((27 * C2, C2), BF16),
            pltpu.VMEM((F + 2, R + 2, C, C2), BF16),
            pltpu.VMEM((cells, C2), F32),
            pltpu.VMEM((F + 2, R + 2, C, C2), BF16),
            pltpu.VMEM((F + 2, R + 2, C, C2), BF16),
            pltpu.VMEM((F, R + 2, C, 3 * C2), BF16),
            pltpu.VMEM((9 * C2, C2), BF16),
            pltpu.VMEM((H, out_rows, C2), BF16),
            pltpu.VMEM((H, out_rows, C2), BF16),
            pltpu.VMEM((H, out_rows, C2), BF16),
            pltpu.VMEM((cells, C2), F32),
            pltpu.VMEM((C2 // 128, cells, 128), F32),
            pltpu.SemaphoreType.DMA((n_send,)),
            pltpu.SemaphoreType.DMA((n_recv,)),
            pltpu.SemaphoreType.DMA((9,)),
        ],
        compiler_params=pltpu.CompilerParams(
            collective_id=0, has_side_effects=True, vmem_limit_bytes=VMEM_LIMIT
        ),
        cost_estimate=pl.CostEstimate(flops=flops, bytes_accessed=1 << 23, transcendentals=0),
    )(
        stay(latent), stay(gain_l.reshape(1, -1)), stay(shift_l.reshape(1, -1)), stay(w_l), stay(up_w),
        stay(gain_b.reshape(1, -1)), stay(shift_b.reshape(1, -1)), stay(w_b), stay(cot),
    )
    row = jax.ShapeDtypeStruct((1, C2), F32)
    done = pl.pallas_call(
        finish_kernel,
        out_shape=tuple(jax.ShapeDtypeStruct(a.shape, a.dtype) for a in outs[:3]) + (row, row),
        in_specs=[vmem] * 4,
        out_specs=(hbm,) * 5,
        scratch_shapes=[pltpu.SemaphoreType.DMA((5,))],
        compiler_params=pltpu.CompilerParams(vmem_limit_bytes=1 << 20),
        cost_estimate=pl.CostEstimate(flops=0, bytes_accessed=1 << 20, transcendentals=0),
    )(*outs)
    return done[0], done[1], done[2], done[3].reshape(C2), done[4].reshape(C2)


def solution(mesh):
    return jax.shard_map(
        functools.partial(local_block, dict(mesh.shape)),
        mesh=mesh,
        in_specs=(
            P(("dp", "tm"), None, None, "height"),
            P("height"),
            P("height"),
            P("tm", "height"),
            P("height", None),
            P(),
            P(),
            P(("tm", "height"), None),
            P(("dp", "tm"), "height", None, None),
        ),
        out_specs=(
            P(("dp", "tm"), "height", None, None),
            P(("dp", "tm"), "height", None, None),
            P(("dp", "tm", "height"), None),
            P("dp"),
            P("dp"),
        ),
        check_vma=False,
    )
```

```python
import functools

import jax
import jax.numpy as jnp
from jax import lax
from jax.experimental import pallas as pl
from jax.experimental.pallas import tpu as pltpu
from jax.sharding import PartitionSpec as P

C1 = 512
GROUPS = 32


epsilon = 1e-06


def shifted(block, axis, distance):
    devices = range(lax.axis_size(axis))
    route = [(i - distance, i) for i in devices if i - distance in devices]
    return lax.ppermute(block, axis, route)


def extended_2(cells, sides, width):
    for axis, dim in sides:
        count = lax.axis_size(axis)
        ends = count - 1
        head = lax.slice_in_dim(cells, 0, width, axis=dim)
        tail = lax.slice_in_dim(cells, cells.shape[dim] - width, cells.shape[dim], axis=dim)
        cells = jnp.concatenate(
            [
                lax.ppermute(tail, axis, [(i, (i + 1) % count) for i in range(ends)]),
                cells,
                lax.ppermute(head, axis, [((i + 1) % count, i) for i in range(ends)]),
            ],
            axis=dim,
        )
    return cells


def standardize(values, mean_value, inverse, groups):
    shape_full = values.shape
    grouped = values.reshape(shape_full[:-1] + (groups, shape_full[-1] // groups))
    return ((grouped - mean_value[:, None]) * inverse[:, None]).reshape(shape_full)


def causal_taps(padded, weight, frames, rows, cols):
    channels_in = padded.shape[-1]
    summed = jnp.zeros((frames * rows * cols, weight.shape[1]), jnp.float32)
    for lag_step in range(3):
        for row_step in range(3):
            for col_step in range(3):
                tap_index = (lag_step * 3 + row_step) * 3 + col_step
                window = padded[
                    lag_step : lag_step + frames,
                    row_step : row_step + rows,
                    col_step : col_step + cols,
                ]
                kernel = weight[tap_index * channels_in : (tap_index + 1) * channels_in]
                summed = summed + jnp.dot(
                    window.reshape(-1, channels_in), kernel, preferred_element_type=jnp.float32
                )
    return summed.reshape(frames, rows, cols, weight.shape[1])


def transposed_taps(padded, weight, frames, rows, cols):
    channels_out = padded.shape[-1]
    channels_in = weight.shape[0] // 27
    summed = jnp.zeros((frames * rows * cols, channels_in), jnp.float32)
    for lag_step in range(3):
        for row_step in range(3):
            for col_step in range(3):
                tap_index = (lag_step * 3 + row_step) * 3 + col_step
                window = padded[
                    2 - lag_step : 2 - lag_step + frames,
                    2 - row_step : 2 - row_step + rows,
                    2 - col_step : 2 - col_step + cols,
                ]
                kernel = weight[tap_index * channels_in : (tap_index + 1) * channels_in]
                summed = summed + lax.dot_general(
                    window.reshape(-1, channels_out),
                    kernel,
                    (((1,), (1,)), ((), ())),
                    preferred_element_type=jnp.float32,
                )
    return summed.reshape(frames, rows, cols, channels_in)


def weight_terms(padded, grads, frames, rows, cols):
    channels_in = padded.shape[-1]
    flat_grads = grads.reshape(-1, grads.shape[-1])
    blocks = []
    for row_step in range(3):
        for col_step in range(3):
            window = padded[2 : 2 + frames, row_step : row_step + rows, col_step : col_step + cols]
            blocks.append(
                lax.dot_general(
                    window.reshape(-1, channels_in),
                    flat_grads,
                    (((0,), (0,)), ((), ())),
                    preferred_element_type=jnp.float32,
                )
            )
    return jnp.concatenate(blocks, 0)


def local(
    latent,
    gain_latent,
    shift_latent,
    conv_latent,
    up_weight,
    gain_block,
    shift_block,
    conv_block,
    cotangent,
):
    per_group = C1 // GROUPS
    groups_here = latent.shape[-1] // per_group
    latent_f32 = latent.astype(jnp.float32)
    grouped = latent_f32.reshape(-1, groups_here, per_group)
    first_sums = jnp.sum(grouped, axis=(0, 2))
    second_sums = jnp.sum(grouped * grouped, axis=(0, 2))
    first_totals, second_totals = lax.psum((first_sums, second_sums), "tm")
    count_latent = grouped.shape[0] * per_group * lax.axis_size("tm")
    mean_latent = first_totals / count_latent
    inverse_latent = lax.rsqrt(second_totals / count_latent - mean_latent * mean_latent + epsilon)
    normed = (
        standardize(latent_f32, mean_latent, inverse_latent, groups_here) * gain_latent
        + shift_latent
    )
    active = jax.nn.silu(normed).astype(jnp.bfloat16)
    earlier = shifted(active, "tm", 1)
    extended = jnp.concatenate([earlier, active], 0)
    all_channels = lax.all_gather(extended, "height", axis=3, tiled=True)
    padded = jnp.pad(all_channels, ((0, 0), (1, 1), (1, 1), (0, 0)))
    latent_weight = lax.all_gather(conv_latent, "tm", axis=0, tiled=True)
    frames_latent, rows_latent, cols_latent = (latent.shape[0], latent.shape[1], latent.shape[2])
    mixed = causal_taps(padded, latent_weight, frames_latent, rows_latent, cols_latent)
    refined = (latent_f32 + mixed).astype(jnp.bfloat16)
    band_rows = rows_latent // lax.axis_size("height")
    own_band = lax.all_to_all(refined, "height", split_axis=1, concat_axis=3, tiled=True)
    flat_band = own_band.reshape(-1, own_band.shape[-1])
    expanded = jnp.dot(
        flat_band,
        lax.all_gather(up_weight, "height", axis=0, tiled=True),
        preferred_element_type=jnp.float32,
    )
    channels_block = up_weight.shape[1] // 8
    spread = expanded.reshape(frames_latent, band_rows, cols_latent, 2, 2, 2, channels_block)
    spread = spread.transpose(0, 3, 1, 4, 2, 5, 6)
    upsampled = spread.reshape(
        2 * frames_latent, 2 * band_rows, 2 * cols_latent, channels_block
    ).astype(jnp.bfloat16)
    frames_block, rows_block, cols_block = (
        upsampled.shape[0],
        upsampled.shape[1],
        upsampled.shape[2],
    )
    up_f32 = upsampled.astype(jnp.float32)
    per_block = channels_block // GROUPS
    grouped_block = up_f32.reshape(-1, GROUPS, per_block)
    block_first = jnp.sum(grouped_block, axis=(0, 2))
    block_second = jnp.sum(grouped_block * grouped_block, axis=(0, 2))
    block_first, block_second = lax.psum((block_first, block_second), ("tm", "height"))
    count_block = grouped_block.shape[0] * per_block * lax.axis_size("tm") * lax.axis_size("height")
    mean_block = block_first / count_block
    inverse_block = lax.rsqrt(block_second / count_block - mean_block * mean_block + epsilon)
    standard = standardize(up_f32, mean_block, inverse_block, GROUPS)
    normed_block = standard * gain_block + shift_block
    active_block = jax.nn.silu(normed_block).astype(jnp.bfloat16)
    before = shifted(active_block[-2:], "tm", 1)
    ext_block = jnp.concatenate([before, active_block], 0)
    beside_all = extended_2(ext_block, (("height", 1),), 1)
    padded_block = jnp.pad(beside_all, ((0, 0), (0, 0), (1, 1), (0, 0)))
    block_weight = lax.all_gather(conv_block, ("tm", "height"), axis=0, tiled=True)
    mixed_block = causal_taps(padded_block, block_weight, frames_block, rows_block, cols_block)
    decoded = (up_f32 + mixed_block).astype(jnp.bfloat16)
    after = shifted(cotangent[:2], "tm", -1)
    grad_ext = jnp.concatenate([cotangent, after], 0)
    grad_around = extended_2(grad_ext, (("height", 1),), 1)
    grad_padded = jnp.pad(grad_around, ((0, 0), (0, 0), (1, 1), (0, 0)))
    grad_active = transposed_taps(grad_padded, block_weight, frames_block, rows_block, cols_block)
    local_terms = weight_terms(padded_block, cotangent, frames_block, rows_block, cols_block)
    grad_weight = lax.psum_scatter(local_terms, ("tm", "height"), scatter_dimension=0, tiled=True)
    sigmoid = jax.nn.sigmoid(normed_block)
    grad_normed = grad_active * sigmoid * (1.0 + normed_block * (1.0 - sigmoid))
    flat_grad = grad_normed.reshape(-1, channels_block)
    flat_standard = standard.reshape(-1, channels_block)
    grad_shift, grad_gain = lax.psum(
        (jnp.sum(flat_grad, axis=0), jnp.sum(flat_grad * flat_standard, axis=0)), ("tm", "height")
    )
    first_mean = jnp.sum((gain_block * grad_shift).reshape(GROUPS, per_block), axis=1) / count_block
    second_mean = jnp.sum((gain_block * grad_gain).reshape(GROUPS, per_block), axis=1) / count_block
    grouped_grad = (grad_normed * gain_block).reshape(-1, GROUPS, per_block)
    grouped_standard = standard.reshape(-1, GROUPS, per_block)
    corrected = (
        grouped_grad - first_mean[:, None] - grouped_standard * second_mean[:, None]
    ) * inverse_block[:, None]
    grad_upsampled = (cotangent.astype(jnp.float32) + corrected.reshape(cotangent.shape)).astype(
        jnp.bfloat16
    )
    return (decoded, grad_upsampled, grad_weight, grad_gain, grad_shift)


MESH = pl.DeviceIdType.MESH
VMEM_LIMIT = 32 * 1024 * 1024
CUTS = 2
F32 = jnp.float32
BF16 = jnp.bfloat16


def group_matrix(channels, per):
    row = lax.broadcasted_iota(jnp.int32, (channels, channels), 0) // per
    col = lax.broadcasted_iota(jnp.int32, (channels, channels), 1) // per
    return (row == col).astype(F32)


def over_groups(rows, per):
    return jnp.dot(
        rows,
        group_matrix(rows.shape[-1], per),
        precision=lax.Precision.HIGHEST,
        preferred_element_type=F32,
    )


def column_shift(cells, cols, step):
    count = cells.shape[0]
    column = lax.broadcasted_iota(jnp.int32, cells.shape, 0) % cols
    edge = 0 if step == 1 else cols - 1
    return jnp.where(column == edge, 0.0, pltpu.roll(cells, step % count, 0))


def two_rows(first, second):
    width = first.shape[-1]
    row = lax.broadcasted_iota(jnp.int32, (8, width), 0)
    return jnp.where(row == 0, first, jnp.where(row == 1, second, 0.0))


def block_kernel(sizes, n_send, n_recv, *refs):
    (T, H, Fl, Rl, Cl, CH, C2, F, R, C) = sizes
    (
        latent, gain_in, shift_in, w_l, up_w, gain_b_in, shift_b_in, w_b, cot,
        decoded, grad_up, grad_w, grad_gs,
        lbuf, gall, gain_b, shift_b, wl, abuf, part, partf, parts_in, stat2, stat3, upw, wb,
        ub, std, ab, cb, cot3, gw, gy, gf, gs, gz, tmp, lace, send_sem, recv_sem, local_sem,
    ) = refs
    d, t, h = lax.axis_index("dp"), lax.axis_index("tm"), lax.axis_index("height")
    N = T * H
    FL = T * Fl
    U = H * CH // T
    band = Rl // H
    q = lax.rem(d, 4)
    half, side = lax.rem(q, 2), q // 2
    pair = d + 1 - 2 * half
    across = d + 2 - 4 * side
    counts = [0, 0]

    def new_send():
        counts[0] += 1
        return send_sem.at[counts[0] - 1]

    def new_recv(n=1):
        counts[1] += n
        return recv_sem.at[counts[1] - 1] if n == 1 else counts[1] - n

    def at(kt, kh):
        return (d, lax.rem(t + kt, T), lax.rem(h + kh, H))

    def copy(src, dst, device, s_sem, r_sem):
        return pltpu.make_async_remote_copy(
            src_ref=src, dst_ref=dst, send_sem=s_sem, recv_sem=r_sem,
            device_id=device, device_id_type=MESH,
        )

    def go(*what):
        copy(*what).start()

    pair_dev, across_dev = (pair, t, h), (across, t, h)
    left = []

    def got(name, ref, r_sem):
        with scope(name):
            copy(ref, ref, pair_dev, send_sem.at[0], r_sem).wait_recv()

    def left_all(ref, s_sem):
        left.append((ref, s_sem))

    def scope(name):
        return jax.named_scope(name)

    peers = [(kt, kh) for kh in [*range(H // 2, H), *range(1, H // 2), 0] for kt in range(T) if kt or kh]
    shard = w_b.shape[0]

    def local_copy(k, src, dst):
        made = pltpu.make_async_copy(src, dst, local_sem.at[k])
        made.start()
        return made

    def other(i):
        where = 0
        for hh in range(H):
            where = where + jnp.where(h == hh, hh ^ (i + 1), 0)
        return where

    nearest = [other(i) for i in range(H - 1)]

    class Along:
        def __init__(self, s_sem):
            self.s, self.base = s_sem, new_recv(H - 1)

        def send(self, i, src, dst):
            to = nearest[i]
            r = recv_sem.at[self.base + lax.rem(to - h + H, H) - 1]
            go(src, dst, (d, t, to), self.s, r)

        def wait(self, name, i, ref):
            got(name, ref, recv_sem.at[self.base + lax.rem(h - nearest[i] + H, H) - 1])

    own_l = local_copy(0, latent, lbuf.at[t, h])
    cb[...] = jnp.zeros(cb.shape, BF16)
    barrier = pltpu.get_barrier_semaphore()
    for kt, kh in peers:
        pl.semaphore_signal(barrier, inc=1, device_id=at(kt, kh), device_id_type=MESH)
    pl.semaphore_signal(barrier, inc=1, device_id=pair_dev, device_id_type=MESH)
    pl.semaphore_signal(barrier, inc=1, device_id=across_dev, device_id_type=MESH)
    own_w = local_copy(2, w_b, wb.at[pl.ds(pl.multiple_of((t * H + h) * shard, shard), shard)])
    own_g = [
        local_copy(5, gain_in, gall.at[h, pl.ds(0, 1)]),
        local_copy(6, shift_in, gall.at[h, pl.ds(1, 1)]),
        local_copy(7, gain_b_in, gain_b), local_copy(8, shift_b_in, shift_b),
    ]
    own_up = local_copy(1, up_w, upw.at[pl.ds(pl.multiple_of(h * CH, CH), CH)])
    own_c = local_copy(4, cot, cb.at[pl.ds(0, F), pl.ds(1, R)])
    own_wl = local_copy(3, w_l, wl)
    abuf[...] = jnp.zeros(abuf.shape, BF16)
    ab[...] = jnp.zeros(ab.shape, BF16)
    own_l.wait()
    with scope("w_barrier"):
        pl.semaphore_wait(barrier, N + 1)

    yes = at(1, 0)
    w_half = shard // 2
    half_cols = pl.ds(pl.multiple_of(half * (C2 // 2), C2 // 2), C2 // 2)

    def w_piece(gt, gh, piece_side):
        start = pl.multiple_of((gt * H + gh) * shard + piece_side * w_half, w_half)
        return wb.at[pl.ds(start, w_half), half_cols]

    def w_both(gt, gh):
        return wb.at[pl.ds(pl.multiple_of((gt * H + gh) * shard, shard), shard), half_cols]

    up_rows, up_cols = CH // T, 2 * C2

    def up_piece(gt, gh, n=1):
        first = 2 * half + (side if n == 1 else 0)
        return upw.at[
            pl.ds(pl.multiple_of(gh * CH + gt * up_rows, up_rows), up_rows),
            pl.ds(pl.multiple_of(first * up_cols, up_cols), n * up_cols),
        ]

    mine = lbuf.at[t, h]
    lz = Along(new_send())
    ly_s, ly_r = new_send(), new_recv()
    for i in range(H - 1):
        lz.send(i, mine, mine)
    go(mine, mine, yes, ly_s, ly_r)
    own_w.wait()
    w_s = new_send()
    w_mine = w_piece(t, h, side)
    wy_r = [new_recv() for _ in range(H)]
    go(w_both(t, h), w_both(t, h), yes, w_s, wy_r[H - 1])
    for made in own_g:
        made.wait()
    gain_s, gain_r = new_send(), new_recv()
    for kh in range(1, H):
        go(gall.at[h], gall.at[h], at(0, kh), gain_s, gain_r)
    own_up.wait()
    u_s = new_send()
    uz = Along(u_s)

    def up_send(core):
        @pl.when(half == core)
        def _():
            for i in range(H - 1):
                uz.send(i, up_piece(t, h), up_piece(t, h))

    up_send(0)
    for i in range(H - 1):
        if i == 2:
            up_send(1)
        piece = lbuf.at[t, nearest[i]]
        lz.wait("w_lz", i, piece)
        go(piece, piece, yes, ly_s, ly_r)
    left_all(lbuf.at[0, pl.ds(0, H - 1)], lz.s)
    left_all(lbuf.at[0], ly_s)
    left_all(gall.at[pl.ds(0, H - 1)], gain_s)

    wx_r, wx_at = [], []
    wpair_r = new_recv()

    def w_across(gt, gh):
        wx_r.append(new_recv())
        wx_at.append((gt, gh))
        go(w_piece(gt, gh, side), w_piece(gt, gh, side), across_dev, w_s, wx_r[-1])

    def w_pair(k):
        gt, gh = wx_at[k]
        got("w_wx", w_piece(gt, gh, 1 - side), wx_r[k])
        go(w_both(gt, gh), w_both(gt, gh), pair_dev, w_s, wpair_r)


    def halo(buffer, f0, f_two, two_at, step):
        made = []
        ok_t_send = (t < T - 1) if step == 1 else (t > 0)
        ok_t_recv = (t > 0) if step == 1 else (t < T - 1)
        kt = step % T

        def part_of(fs, n_f, r0, n_r):
            return buffer.at[pl.ds(fs, n_f), pl.ds(r0, n_r)]

        for kt_, kh_, ok_s, ok_r, src, dst in (
            (kt, 0, ok_t_send, ok_t_recv, part_of(f_two, 2, 1, R), part_of(two_at, 2, 1, R)),
            (0, 1, h < H - 1, h > 0, part_of(f0, F, R, 1), part_of(f0, F, 0, 1)),
            (0, H - 1, h > 0, h < H - 1, part_of(f0, F, 1, 1), part_of(f0, F, R + 1, 1)),
            (kt, 1, ok_t_send & (h < H - 1), ok_t_recv & (h > 0),
             part_of(f_two, 2, R, 1), part_of(two_at, 2, 0, 1)),
            (kt, H - 1, ok_t_send & (h > 0), ok_t_recv & (h < H - 1),
             part_of(f_two, 2, 1, 1), part_of(two_at, 2, R + 1, 1)),
        ):
            c = copy(src, dst, at(kt_, kh_), new_send(), new_recv())
            pl.when(ok_s)(c.start)
            made.append((c, ok_s, ok_r))
        return made

    uy_r = [new_recv() for _ in range(H - 1)]
    ux_r = [new_recv(), new_recv()]
    upair_r = new_recv()

    def up_height(i):
        piece = up_piece(t, nearest[i])
        uz.wait("w_uz", i, piece)
        go(piece, piece, yes, u_s, uy_r[i])
        go(piece, piece, across_dev, u_s, ux_r[0])

    up_height(0)
    got("w_ly", lbuf.at[0], ly_r)
    got("w_gain", gall.at[pl.ds(0, H - 1)], gain_r)
    up_height(1)
    wz = Along(w_s)
    own_c.wait()
    wz.send(0, w_mine, w_mine)
    wz.send(1, w_mine, w_mine)

    per_l = H * CH // GROUPS
    cells_l = FL * Rl * Cl
    count_l = cells_l * per_l
    xs, rows = [], []
    for k in range(H):
        x = lbuf[:, k].astype(F32).reshape(cells_l, CH)
        rows += [jnp.sum(x, 0, keepdims=True), jnp.sum(x * x, 0, keepdims=True)]
    total = over_groups(jnp.concatenate(rows, 0), per_l) / count_l
    for k in range(H):
        mean = total[2 * k : 2 * k + 1]
        inv = lax.rsqrt(total[2 * k + 1 : 2 * k + 2] - mean * mean + epsilon)
        x = lbuf[:, k].astype(F32).reshape(cells_l, CH)
        v = (x - mean) * inv * gall[k, 0:1] + gall[k, 1:2]
        lane = k * CH % U
        abuf[k * CH // U, 2 : 2 + FL, 1 : 1 + Rl, :, lane : lane + CH] = (
            (v * jax.nn.sigmoid(v)).astype(BF16).reshape(FL, Rl, Cl, CH)
        )

    up_height(2)

    own_wl.wait()

    parts_of = 2
    some = FL // parts_of

    def window(m, chunk, tap):
        lag, dr = tap // 9, (tap // 3) % 3
        return abuf[chunk, pl.ds(lag + m * some, some), pl.ds(dr, Rl)].reshape(some * Rl * Cl, U)

    def w_rows(chunk, tap):
        return wl[pl.ds(pl.multiple_of((tap * T + chunk - 27 * t) * U, U), U), :]

    with scope("c_latent"):
        sums = [None] * parts_of
        for g in range(4):
            tap = jnp.where(t == 0, 3 * g, 15 + 3 * g)
            for chunk in range(T):
                k3 = jnp.concatenate([w_rows(chunk, tap + dc) for dc in range(3)], 1)
                for m in range(parts_of):
                    term = jnp.dot(window(m, chunk, tap), k3, preferred_element_type=F32)
                    sums[m] = term if sums[m] is None else sums[m] + term
        alone = jnp.where(t == 0, 12, 14)
        k2 = jnp.concatenate([w_rows(t, alone), w_rows(t, 13)], 1)
        mixed = []
        for m in range(parts_of):
            both = jnp.dot(window(m, t, alone), k2, preferred_element_type=F32)
            lone = both[:, :CH] + jnp.dot(
                window(m, 1 - t, alone), w_rows(1 - t, alone), preferred_element_type=F32
            )
            first = sums[m][:, :CH] + jnp.where(t == 0, lone, 0.0)
            last = sums[m][:, 2 * CH :] + jnp.where(t == 0, 0.0, lone)
            mixed.append(
                column_shift(first, Cl, 1) + sums[m][:, CH : 2 * CH] + both[:, CH:]
                + column_shift(last, Cl, -1)
            )
        mixed = jnp.concatenate(mixed, 0)
        partf[...] = mixed.reshape(FL, Rl, Cl, CH)
        partf[pl.ds(t * Fl, Fl)] += lbuf[t, h].astype(F32)
        part[...] = partf[...].astype(BF16)
    p_s, p_r = new_send(), new_recv()
    for kt, kh in peers:
        dev = at(kt, kh)
        go(part.at[pl.ds(dev[1] * Fl, Fl), pl.ds(dev[2] * band, band)],
           parts_in.at[kt * H + kh], dev, p_s, p_r)
    wz.send(2, w_mine, w_mine)

    def w_height(i):
        piece = w_piece(t, nearest[i], side)
        wz.wait("w_wz", i, piece)
        go(piece, piece, yes, w_s, wy_r[i])
        w_across(t, nearest[i])

    piece = up_piece(1 - t, nearest[0])
    got("w_uy", piece, uy_r[0])
    go(piece, piece, across_dev, u_s, ux_r[1])
    piece = up_piece(1 - t, nearest[1])
    got("w_uy", piece, uy_r[1])
    go(piece, piece, across_dev, u_s, ux_r[1])
    piece = up_piece(1 - t, nearest[2])
    got("w_uy", piece, uy_r[2])
    go(piece, piece, across_dev, u_s, ux_r[1])
    got("w_wy0", w_both(1 - t, h), wy_r[H - 1])
    go(w_both(1 - t, h), w_both(1 - t, h), pair_dev, w_s, wpair_r)
    w_height(0)
    cot_halo = halo(cb, 0, 0, F, -1)
    got("w_ux", upw.at[pl.ds(0, (H - 1) * up_rows), pl.ds(0, up_cols)], ux_r[0])
    for i in range(H - 1):
        piece = up_piece(t, nearest[i], 2)
        go(piece, piece, pair_dev, u_s, upair_r)
    got("w_ux", upw.at[pl.ds(0, (H - 1) * up_rows), pl.ds(0, up_cols)], ux_r[1])
    for i in range(H - 1):
        piece = up_piece(1 - t, nearest[i], 2)
        go(piece, piece, pair_dev, u_s, upair_r)
    w_height(1)
    got("w_upair", upw.at[pl.ds(0, (H - 1) * CH), pl.ds(0, 4 * C2)], upair_r)
    got("w_parts", parts_in.at[pl.ds(1, N - 1)], p_r)
    left_all(parts_in.at[pl.ds(1, N - 1)], p_s)
    left_all(upw.at[pl.ds(0, (H - 1) * CH)], u_s)

    cells_b = Fl * band * Cl
    with scope("c_up"):
        parts_own = partf[pl.ds(t * Fl, Fl), pl.ds(h * band, band)]
        expanded = jnp.zeros((cells_b, 8 * C2), F32)
        for kh in range(H):
            value = parts_own if kh == 0 else parts_in[kh].astype(F32)
            for kt in range(1, T):
                value = value + parts_in[kt * H + kh].astype(F32)
            refined = value.reshape(cells_b, CH).astype(BF16)
            source = lax.rem(h + H - kh, H)
            expanded = expanded + jnp.dot(
                refined, upw[pl.ds(pl.multiple_of(source * CH, CH), CH), :],
                preferred_element_type=F32,
            )
        expanded = expanded.astype(BF16).astype(F32)
        for f in range(Fl):
            for r in range(band):
                for p in range(2):
                    for qq in range(2):
                        for s in range(2):
                            first = (f * band + r) * Cl
                            col = ((p * 2 + qq) * 2 + s) * C2
                            for n in range(C2 // 128):
                                lace[
                                    n, pl.ds(((2 * f + p) * R + 2 * r + qq) * C + s, Cl, stride=2), :
                                ] = expanded[first : first + Cl, col + n * 128 : col + (n + 1) * 128]

        cells = F * R * C
        me = t * H + h
        up = jnp.concatenate([lace[n] for n in range(C2 // 128)], axis=1)
        stat2[me] = two_rows(jnp.sum(up, 0, keepdims=True), jnp.sum(up * up, 0, keepdims=True))
        ub[2 : 2 + F, 1 : 1 + R] = up.astype(BF16).reshape(F, R, C, C2)
    s2_s, s2_r = new_send(), new_recv()
    for kt, kh in peers:
        go(stat2.at[me], stat2.at[me], at(kt, kh), s2_s, s2_r)
    left_all(stat2.at[pl.ds(0, N - 1)], s2_s)
    up_halo = halo(ub, 2, F, 0, 1)

    w_height(2)
    with scope("w_cothalo"):
        for made, _, ok in cot_halo:
            pl.when(ok)(made.wait_recv)
    wide = cb[0:F].astype(F32).reshape(F * (R + 2) * C, C2)
    cot3[:, :, :, 0:C2] = column_shift(wide, C, -1).astype(BF16).reshape(F, R + 2, C, C2)
    cot3[:, :, :, C2 : 2 * C2] = cb[0:F]
    cot3[:, :, :, 2 * C2 :] = column_shift(wide, C, 1).astype(BF16).reshape(F, R + 2, C, C2)

    got("w_s2", stat2.at[pl.ds(0, N - 1)], s2_r)
    per_b = C2 // GROUPS
    count_b = cells * per_b * N
    total = stat2[0]
    for k in range(1, N):
        total = total + stat2[k]
    total = over_groups(total, per_b) / count_b
    mean_b = total[0:1]
    inv_b = lax.rsqrt(total[1:2] - mean_b * mean_b + epsilon)

    def activate(values):
        normed = (values - mean_b) * inv_b * gain_b[...] + shift_b[...]
        return (normed * jax.nn.sigmoid(normed)).astype(BF16)

    with scope("c_gw"):
        own = activate(ub[2 : 2 + F, 1 : 1 + R].astype(F32).reshape(cells, C2))
        ab[2 : 2 + F, 1 : 1 + R] = own.reshape(F, R, C, C2)
        def taps_of(i):
            dr = jnp.where(t == 0, 2 - i, i)
            term = lax.dot_general(
                own, cot3[:, pl.ds(2 - dr, R)].reshape(cells, 3 * C2),
                (((0,), (0,)), ((), ())), preferred_element_type=F32,
            )
            for dc in range(3):
                gw[pl.ds(pl.multiple_of((dr * 3 + dc) * C2, C2), C2), :] = (
                    term[:, dc * C2 : (dc + 1) * C2].astype(BF16)
                )

        taps_of(0)
        taps_of(1)
    out_rows = 9 * C2 // N
    y_rows = out_rows * H

    cut_rows = out_rows // CUTS

    def cut(c):
        return pl.ds(c * cut_rows, cut_rows)

    def g_at(gt, gh, c):
        start = (gt * H + gh) * out_rows + c * cut_rows
        return pl.ds(pl.multiple_of(start, cut_rows), cut_rows)

    def g_rows(gt, gh, c):
        return gw.at[g_at(gt, gh, c)]

    def ahead(kh):
        return lax.rem(h + kh, H)

    order = [*range(H // 2, H), *range(1, H // 2), 0]
    gy_s, gz_s, gz_r = new_send(), new_send(), new_recv()
    gy_r = {(kh, c): new_recv() for kh in order for c in range(CUTS) if (kh, c) != (1, 0)}
    first_cut = (1, 0)
    steps = [(kh, c) for kh in order for c in range(CUTS) if (kh, c) != first_cut]
    for kh, c in steps:
        if (kh, c) != (0, 0):
            go(g_rows(1 - t, ahead(kh), c), gy.at[kh, cut(c)], yes, gy_s, gy_r[kh, c])
    zf_s, zf_r = new_send(), new_recv()
    go(g_rows(1 - t, ahead(1), 0), gf.at[1], at(0, 1), zf_s, zf_r)
    with scope("c_gw2"):
        taps_of(2)
    go(g_rows(t, ahead(1), 0), gf.at[0], at(0, 1), zf_s, zf_r)
    left_all(gw.at[pl.ds(0, len(steps) * cut_rows)], gy_s)
    left_all(gf, zf_s)

    def g_join():
        got("w_gf", gf, zf_r)
        total = gw[g_at(1 - t, h, 0), :].astype(F32) + gf[1].astype(F32)
        gs[0, :cut_rows] = total.astype(BF16)
        go(gs.at[0, cut(0)], gy.at[0, cut(0)], yes, gy_s, gy_r[0, 0])

    with scope("w_uphalo"):
        for made, _, ok in up_halo:
            pl.when(ok)(made.wait_recv)
    with scope("c_halo"):
        for rows_at, n_rows, ok in ((0, 1, h > 0), (R + 1, 1, h < H - 1)):
            @pl.when(ok)
            def _():
                v = ub[2 : 2 + F, rows_at : rows_at + n_rows].astype(F32).reshape(F * n_rows * C, C2)
                ab[2 : 2 + F, rows_at : rows_at + n_rows] = activate(v).reshape(F, n_rows, C, C2)
        for rows_at, n_rows, ok in (
            (1, R, t > 0), (0, 1, (t > 0) & (h > 0)), (R + 1, 1, (t > 0) & (h < H - 1))
        ):
            @pl.when(ok)
            def _():
                v = ub[0:2, rows_at : rows_at + n_rows].astype(F32).reshape(2 * n_rows * C, C2)
                ab[0:2, rows_at : rows_at + n_rows] = activate(v).reshape(2, n_rows, C, C2)

    def g_on(kh, c):
        got("w_gy", gy.at[kh, cut(c)], gy_r[kh, c])
        total = gy[kh, c * cut_rows : (c + 1) * cut_rows].astype(F32)
        total = total + gw[g_at(t, ahead(kh), c), :].astype(F32)
        if (kh, c) == (0, 0):
            total = total + gf[0].astype(F32)
        if kh == 0:
            grad_w[c * cut_rows : (c + 1) * cut_rows] = total
        else:
            gs[kh, c * cut_rows : (c + 1) * cut_rows] = total.astype(BF16)
            go(gs.at[kh, cut(c)], gz.at[kh, cut(c)], at(0, kh), gz_s, gz_r)

    got("w_wy", w_piece(1 - t, nearest[0], side), wy_r[0])
    w_across(1 - t, nearest[0])
    got("w_wy", w_piece(1 - t, nearest[1], side), wy_r[1])
    w_across(1 - t, nearest[1])
    got("w_wy", w_piece(1 - t, nearest[2], side), wy_r[2])
    w_across(1 - t, nearest[2])
    w_pair(0)
    w_pair(1)
    g_on(*steps[0])
    w_pair(2)
    g_on(*steps[1])
    w_pair(3)
    g_on(*steps[2])
    g_join()
    w_pair(4)
    w_pair(5)
    g_on(*steps[3])
    left_all(gw.at[pl.ds(0, (len(steps) - CUTS) * cut_rows)], gz_s)
    got("w_wpair", wb.at[pl.ds(0, (N - 1) * shard), pl.ds(0, C2 // 2)], wpair_r)
    left_all(wb.at[pl.ds(0, (2 * H + 3 * N - 4) * w_half // 2)], w_s)

    with scope("c_gradtap"):
        sums = {}
        for j in range(9):
            lag, dr = j // 3, j % 3
            win = cb[2 - lag : 2 - lag + F, 2 - dr : 2 - dr + R].reshape(cells, C2)
            for dc in range(3):
                term = lax.dot_general(
                    win, wb[(j * 3 + dc) * C2 : (j * 3 + dc + 1) * C2, :],
                    (((1,), (1,)), ((), ())), preferred_element_type=F32,
                )
                key = (dc, j % 2 if dc == 1 else 0)
                sums[key] = sums[key] + term if key in sums else term
        grad_active = (
            column_shift(sums[0, 0], C, -1) + sums[1, 0] + sums[1, 1]
            + column_shift(sums[2, 0], C, 1)
        )
    standard = (ub[2 : 2 + F, 1 : 1 + R].astype(F32).reshape(cells, C2) - mean_b) * inv_b
    std[...] = standard
    normed = standard * gain_b[...] + shift_b[...]
    sigmoid = jax.nn.sigmoid(normed)
    grad_normed = grad_active * sigmoid * (1.0 + normed * (1.0 - sigmoid))
    stat3[me] = two_rows(
        jnp.sum(grad_normed * standard, 0, keepdims=True), jnp.sum(grad_normed, 0, keepdims=True)
    )
    s3_s, s3_r = new_send(), new_recv()
    for kt, kh in peers:
        go(stat3.at[me], stat3.at[me], at(kt, kh), s3_s, s3_r)
    left_all(stat3.at[pl.ds(0, N - 1)], s3_s)
    tmp[...] = grad_normed * gain_b[...]
    for step in steps[4:5]:
        g_on(*step)

    some = F // 2
    n = some * R * C
    for m in range(2):
        with scope("c_tap"):
            wide = None
            for j in range(9):
                lag, dr = j // 3, j % 3
                k3 = jnp.concatenate(
                    [wb[(j * 3 + dc) * C2 : (j * 3 + dc + 1) * C2, :] for dc in range(3)], 1
                )
                win = ab[lag + m * some : lag + (m + 1) * some, dr : dr + R].reshape(n, C2)
                term = jnp.dot(win, k3, preferred_element_type=F32)
                wide = term if wide is None else wide + term
            decoded[m * some : (m + 1) * some] = (
                (column_shift(wide[:, :C2], C, 1) + wide[:, C2 : 2 * C2]
                 + column_shift(wide[:, 2 * C2 :], C, -1)
                 + ub[2 + m * some : 2 + (m + 1) * some, 1 : 1 + R].astype(F32).reshape(n, C2))
                .astype(BF16).reshape(some, R, C, C2)
            )
        for step in steps[5:5] if m == 0 else steps[5 : -CUTS]:
            g_on(*step)

    got("w_s3", stat3.at[pl.ds(0, N - 1)], s3_r)
    total = stat3[0]
    for k in range(1, N):
        total = total + stat3[k]
    grad_gs[...] = total
    means = over_groups(total * gain_b[...], per_b) / count_b
    corrected = (tmp[...] - means[1:2] - std[...] * means[0:1]) * inv_b
    grad_up[...] = (
        cb[0:F, 1 : 1 + R].astype(F32).reshape(cells, C2) + corrected
    ).astype(BF16).reshape(F, R, C, C2)

    for step in steps[-CUTS:]:
        g_on(*step)
    got("w_gz", gw.at[pl.ds(0, (len(steps) - CUTS) * cut_rows)], gz_r)
    for c in range(CUTS):
        rows = slice(c * cut_rows, (c + 1) * cut_rows)
        result = grad_w[rows]
        for kh in range(1, H):
            if (kh, c) != first_cut:
                result = result + gz[kh, rows].astype(F32)
        grad_w[rows] = result

    with scope("w_send"):
        for ref, s_sem in left:
            copy(ref, ref, pair_dev, s_sem, recv_sem.at[0]).wait_send()
        for made, ok, _ in cot_halo + up_halo:
            pl.when(ok)(made.wait_send)
    assert counts == [n_send, n_recv], counts


def finish_kernel(decoded, grad_up, grad_w, grad_gs, out_d, out_u, out_w, out_g, out_s, sems):
    moves = [
        pltpu.make_async_copy(src, dst, sems.at[k])
        for k, (src, dst) in enumerate((
            (decoded, out_d), (grad_up, out_u), (grad_w, out_w),
            (grad_gs.at[pl.ds(0, 1)], out_g), (grad_gs.at[pl.ds(1, 1)], out_s),
        ))
    ]
    for move in moves:
        move.start()
    for move in moves:
        move.wait()


def stay(array):
    return pltpu.with_memory_space_constraint(array, pltpu.HBM)


def local_block(shape, *args):
    (latent, gain_l, shift_l, w_l, up_w, gain_b, shift_b, w_b, cot) = args
    T, H = shape["tm"], shape["height"]
    Fl, Rl, Cl, CH = latent.shape
    F, R, C, C2 = cot.shape
    N = T * H
    U = H * CH // T
    fits = (
        shape["dp"] % 4 == 0 and T == 2 and H == 4
        and CH % 128 == 0 and U % CH == 0
        and w_b.shape[0] % 32 == 0 and (CH // T) % 16 == 0
        and (9 * C2) % (16 * CUTS * N) == 0 and C2 % 256 == 0
        and Cl % 16 == 0 and w_l.shape[0] == 27 * U and F >= 2
    )
    if not fits:
        return local(*args)
    sizes = (T, H, Fl, Rl, Cl, CH, C2, F, R, C)
    n_send = 21
    n_recv = 20 + 4 * (H - 1) + (1 + CUTS) * H + N - 2
    FL = T * Fl
    band = Rl // H
    cells = F * R * C
    out_rows = 9 * C2 // N
    vmem = pl.BlockSpec(memory_space=pltpu.VMEM)
    hbm = pl.BlockSpec(memory_space=pltpu.HBM)
    flops = 2 * (FL * Rl * Cl * w_l.size + 2 * cells * 27 * C2 * C2 + cells * 9 * C2 * C2)
    outs = pl.pallas_call(
        functools.partial(block_kernel, sizes, n_send, n_recv),
        out_shape=(
            jax.ShapeDtypeStruct(cot.shape, BF16),
            jax.ShapeDtypeStruct(cot.shape, BF16),
            jax.ShapeDtypeStruct((out_rows, C2), F32),
            jax.ShapeDtypeStruct((8, C2), F32),
        ),
        in_specs=[hbm] * 9,
        out_specs=(vmem,) * 4,
        scratch_shapes=[
            pltpu.VMEM((T, H, Fl, Rl, Cl, CH), BF16),
            pltpu.VMEM((H, 2, CH), F32),
            pltpu.VMEM((1, C2), F32),
            pltpu.VMEM((1, C2), F32),
            pltpu.VMEM(w_l.shape, BF16),
            pltpu.VMEM((T, FL + 2, Rl + 2, Cl, U), BF16),
            pltpu.VMEM((FL, Rl, Cl, CH), BF16),
            pltpu.VMEM((FL, Rl, Cl, CH), F32),
            pltpu.VMEM((N, Fl, band, Cl, CH), BF16),
            pltpu.VMEM((N, 8, C2), F32),
            pltpu.VMEM((N, 8, C2), F32),
            pltpu.VMEM((H * CH, 8 * C2), BF16),
            pltpu.VMEM((27 * C2, C2), BF16),
            pltpu.VMEM((F + 2, R + 2, C, C2), BF16),
            pltpu.VMEM((cells, C2), F32),
            pltpu.VMEM((F + 2, R + 2, C, C2), BF16),
            pltpu.VMEM((F + 2, R + 2, C, C2), BF16),
            pltpu.VMEM((F, R + 2, C, 3 * C2), BF16),
            pltpu.VMEM((9 * C2, C2), BF16),
            pltpu.VMEM((H, out_rows, C2), BF16),
            pltpu.VMEM((2, out_rows // CUTS, C2), BF16),
            pltpu.VMEM((H, out_rows, C2), BF16),
            pltpu.VMEM((H, out_rows, C2), BF16),
            pltpu.VMEM((cells, C2), F32),
            pltpu.VMEM((C2 // 128, cells, 128), F32),
            pltpu.SemaphoreType.DMA((n_send,)),
            pltpu.SemaphoreType.DMA((n_recv,)),
            pltpu.SemaphoreType.DMA((9,)),
        ],
        compiler_params=pltpu.CompilerParams(
            collective_id=0, has_side_effects=True, vmem_limit_bytes=VMEM_LIMIT
        ),
        cost_estimate=pl.CostEstimate(flops=flops, bytes_accessed=1 << 23, transcendentals=0),
    )(
        stay(latent), stay(gain_l.reshape(1, -1)), stay(shift_l.reshape(1, -1)), stay(w_l), stay(up_w),
        stay(gain_b.reshape(1, -1)), stay(shift_b.reshape(1, -1)), stay(w_b), stay(cot),
    )
    row = jax.ShapeDtypeStruct((1, C2), F32)
    done = pl.pallas_call(
        finish_kernel,
        out_shape=tuple(jax.ShapeDtypeStruct(a.shape, a.dtype) for a in outs[:3]) + (row, row),
        in_specs=[vmem] * 4,
        out_specs=(hbm,) * 5,
        scratch_shapes=[pltpu.SemaphoreType.DMA((5,))],
        compiler_params=pltpu.CompilerParams(vmem_limit_bytes=1 << 20),
        cost_estimate=pl.CostEstimate(flops=0, bytes_accessed=1 << 20, transcendentals=0),
    )(*outs)
    return done[0], done[1], done[2], done[3].reshape(C2), done[4].reshape(C2)


def solution(mesh):
    return jax.shard_map(
        functools.partial(local_block, dict(mesh.shape)),
        mesh=mesh,
        in_specs=(
            P(("dp", "tm"), None, None, "height"),
            P("height"),
            P("height"),
            P("tm", "height"),
            P("height", None),
            P(),
            P(),
            P(("tm", "height"), None),
            P(("dp", "tm"), "height", None, None),
        ),
        out_specs=(
            P(("dp", "tm"), "height", None, None),
            P(("dp", "tm"), "height", None, None),
            P(("dp", "tm", "height"), None),
            P("dp"),
            P("dp"),
        ),
        check_vma=False,
    )
```

```python
import functools

import jax
import jax.numpy as jnp
from jax import lax
from jax.experimental import pallas as pl
from jax.experimental.pallas import tpu as pltpu
from jax.sharding import PartitionSpec as P

C1 = 512
GROUPS = 32


epsilon = 1e-06


def shifted(block, axis, distance):
    devices = range(lax.axis_size(axis))
    route = [(i - distance, i) for i in devices if i - distance in devices]
    return lax.ppermute(block, axis, route)


def extended_2(cells, sides, width):
    for axis, dim in sides:
        count = lax.axis_size(axis)
        ends = count - 1
        head = lax.slice_in_dim(cells, 0, width, axis=dim)
        tail = lax.slice_in_dim(cells, cells.shape[dim] - width, cells.shape[dim], axis=dim)
        cells = jnp.concatenate(
            [
                lax.ppermute(tail, axis, [(i, (i + 1) % count) for i in range(ends)]),
                cells,
                lax.ppermute(head, axis, [((i + 1) % count, i) for i in range(ends)]),
            ],
            axis=dim,
        )
    return cells


def standardize(values, mean_value, inverse, groups):
    shape_full = values.shape
    grouped = values.reshape(shape_full[:-1] + (groups, shape_full[-1] // groups))
    return ((grouped - mean_value[:, None]) * inverse[:, None]).reshape(shape_full)


def causal_taps(padded, weight, frames, rows, cols):
    channels_in = padded.shape[-1]
    summed = jnp.zeros((frames * rows * cols, weight.shape[1]), jnp.float32)
    for lag_step in range(3):
        for row_step in range(3):
            for col_step in range(3):
                tap_index = (lag_step * 3 + row_step) * 3 + col_step
                window = padded[
                    lag_step : lag_step + frames,
                    row_step : row_step + rows,
                    col_step : col_step + cols,
                ]
                kernel = weight[tap_index * channels_in : (tap_index + 1) * channels_in]
                summed = summed + jnp.dot(
                    window.reshape(-1, channels_in), kernel, preferred_element_type=jnp.float32
                )
    return summed.reshape(frames, rows, cols, weight.shape[1])


def transposed_taps(padded, weight, frames, rows, cols):
    channels_out = padded.shape[-1]
    channels_in = weight.shape[0] // 27
    summed = jnp.zeros((frames * rows * cols, channels_in), jnp.float32)
    for lag_step in range(3):
        for row_step in range(3):
            for col_step in range(3):
                tap_index = (lag_step * 3 + row_step) * 3 + col_step
                window = padded[
                    2 - lag_step : 2 - lag_step + frames,
                    2 - row_step : 2 - row_step + rows,
                    2 - col_step : 2 - col_step + cols,
                ]
                kernel = weight[tap_index * channels_in : (tap_index + 1) * channels_in]
                summed = summed + lax.dot_general(
                    window.reshape(-1, channels_out),
                    kernel,
                    (((1,), (1,)), ((), ())),
                    preferred_element_type=jnp.float32,
                )
    return summed.reshape(frames, rows, cols, channels_in)


def weight_terms(padded, grads, frames, rows, cols):
    channels_in = padded.shape[-1]
    flat_grads = grads.reshape(-1, grads.shape[-1])
    blocks = []
    for row_step in range(3):
        for col_step in range(3):
            window = padded[2 : 2 + frames, row_step : row_step + rows, col_step : col_step + cols]
            blocks.append(
                lax.dot_general(
                    window.reshape(-1, channels_in),
                    flat_grads,
                    (((0,), (0,)), ((), ())),
                    preferred_element_type=jnp.float32,
                )
            )
    return jnp.concatenate(blocks, 0)


def local(
    latent,
    gain_latent,
    shift_latent,
    conv_latent,
    up_weight,
    gain_block,
    shift_block,
    conv_block,
    cotangent,
):
    per_group = C1 // GROUPS
    groups_here = latent.shape[-1] // per_group
    latent_f32 = latent.astype(jnp.float32)
    grouped = latent_f32.reshape(-1, groups_here, per_group)
    first_sums = jnp.sum(grouped, axis=(0, 2))
    second_sums = jnp.sum(grouped * grouped, axis=(0, 2))
    first_totals, second_totals = lax.psum((first_sums, second_sums), "tm")
    count_latent = grouped.shape[0] * per_group * lax.axis_size("tm")
    mean_latent = first_totals / count_latent
    inverse_latent = lax.rsqrt(second_totals / count_latent - mean_latent * mean_latent + epsilon)
    normed = (
        standardize(latent_f32, mean_latent, inverse_latent, groups_here) * gain_latent
        + shift_latent
    )
    active = jax.nn.silu(normed).astype(jnp.bfloat16)
    earlier = shifted(active, "tm", 1)
    extended = jnp.concatenate([earlier, active], 0)
    all_channels = lax.all_gather(extended, "height", axis=3, tiled=True)
    padded = jnp.pad(all_channels, ((0, 0), (1, 1), (1, 1), (0, 0)))
    latent_weight = lax.all_gather(conv_latent, "tm", axis=0, tiled=True)
    frames_latent, rows_latent, cols_latent = (latent.shape[0], latent.shape[1], latent.shape[2])
    mixed = causal_taps(padded, latent_weight, frames_latent, rows_latent, cols_latent)
    refined = (latent_f32 + mixed).astype(jnp.bfloat16)
    band_rows = rows_latent // lax.axis_size("height")
    own_band = lax.all_to_all(refined, "height", split_axis=1, concat_axis=3, tiled=True)
    flat_band = own_band.reshape(-1, own_band.shape[-1])
    expanded = jnp.dot(
        flat_band,
        lax.all_gather(up_weight, "height", axis=0, tiled=True),
        preferred_element_type=jnp.float32,
    )
    channels_block = up_weight.shape[1] // 8
    spread = expanded.reshape(frames_latent, band_rows, cols_latent, 2, 2, 2, channels_block)
    spread = spread.transpose(0, 3, 1, 4, 2, 5, 6)
    upsampled = spread.reshape(
        2 * frames_latent, 2 * band_rows, 2 * cols_latent, channels_block
    ).astype(jnp.bfloat16)
    frames_block, rows_block, cols_block = (
        upsampled.shape[0],
        upsampled.shape[1],
        upsampled.shape[2],
    )
    up_f32 = upsampled.astype(jnp.float32)
    per_block = channels_block // GROUPS
    grouped_block = up_f32.reshape(-1, GROUPS, per_block)
    block_first = jnp.sum(grouped_block, axis=(0, 2))
    block_second = jnp.sum(grouped_block * grouped_block, axis=(0, 2))
    block_first, block_second = lax.psum((block_first, block_second), ("tm", "height"))
    count_block = grouped_block.shape[0] * per_block * lax.axis_size("tm") * lax.axis_size("height")
    mean_block = block_first / count_block
    inverse_block = lax.rsqrt(block_second / count_block - mean_block * mean_block + epsilon)
    standard = standardize(up_f32, mean_block, inverse_block, GROUPS)
    normed_block = standard * gain_block + shift_block
    active_block = jax.nn.silu(normed_block).astype(jnp.bfloat16)
    before = shifted(active_block[-2:], "tm", 1)
    ext_block = jnp.concatenate([before, active_block], 0)
    beside_all = extended_2(ext_block, (("height", 1),), 1)
    padded_block = jnp.pad(beside_all, ((0, 0), (0, 0), (1, 1), (0, 0)))
    block_weight = lax.all_gather(conv_block, ("tm", "height"), axis=0, tiled=True)
    mixed_block = causal_taps(padded_block, block_weight, frames_block, rows_block, cols_block)
    decoded = (up_f32 + mixed_block).astype(jnp.bfloat16)
    after = shifted(cotangent[:2], "tm", -1)
    grad_ext = jnp.concatenate([cotangent, after], 0)
    grad_around = extended_2(grad_ext, (("height", 1),), 1)
    grad_padded = jnp.pad(grad_around, ((0, 0), (0, 0), (1, 1), (0, 0)))
    grad_active = transposed_taps(grad_padded, block_weight, frames_block, rows_block, cols_block)
    local_terms = weight_terms(padded_block, cotangent, frames_block, rows_block, cols_block)
    grad_weight = lax.psum_scatter(local_terms, ("tm", "height"), scatter_dimension=0, tiled=True)
    sigmoid = jax.nn.sigmoid(normed_block)
    grad_normed = grad_active * sigmoid * (1.0 + normed_block * (1.0 - sigmoid))
    flat_grad = grad_normed.reshape(-1, channels_block)
    flat_standard = standard.reshape(-1, channels_block)
    grad_shift, grad_gain = lax.psum(
        (jnp.sum(flat_grad, axis=0), jnp.sum(flat_grad * flat_standard, axis=0)), ("tm", "height")
    )
    first_mean = jnp.sum((gain_block * grad_shift).reshape(GROUPS, per_block), axis=1) / count_block
    second_mean = jnp.sum((gain_block * grad_gain).reshape(GROUPS, per_block), axis=1) / count_block
    grouped_grad = (grad_normed * gain_block).reshape(-1, GROUPS, per_block)
    grouped_standard = standard.reshape(-1, GROUPS, per_block)
    corrected = (
        grouped_grad - first_mean[:, None] - grouped_standard * second_mean[:, None]
    ) * inverse_block[:, None]
    grad_upsampled = (cotangent.astype(jnp.float32) + corrected.reshape(cotangent.shape)).astype(
        jnp.bfloat16
    )
    return (decoded, grad_upsampled, grad_weight, grad_gain, grad_shift)


MESH = pl.DeviceIdType.MESH
VMEM_LIMIT = 32 * 1024 * 1024
CUTS = 2
F32 = jnp.float32
BF16 = jnp.bfloat16


def group_matrix(channels, per):
    row = lax.broadcasted_iota(jnp.int32, (channels, channels), 0) // per
    col = lax.broadcasted_iota(jnp.int32, (channels, channels), 1) // per
    return (row == col).astype(F32)


def over_groups(rows, per):
    return jnp.dot(
        rows,
        group_matrix(rows.shape[-1], per),
        precision=lax.Precision.HIGHEST,
        preferred_element_type=F32,
    )


def column_shift(cells, cols, step):
    count = cells.shape[0]
    column = lax.broadcasted_iota(jnp.int32, cells.shape, 0) % cols
    edge = 0 if step == 1 else cols - 1
    return jnp.where(column == edge, 0.0, pltpu.roll(cells, step % count, 0))


def two_rows(first, second):
    width = first.shape[-1]
    row = lax.broadcasted_iota(jnp.int32, (8, width), 0)
    return jnp.where(row == 0, first, jnp.where(row == 1, second, 0.0))


def side_by_side(first, second):
    return jnp.concatenate([first, second], 1)


def block_kernel(sizes, n_send, n_recv, *refs):
    (T, H, Fl, Rl, Cl, CH, C2, F, R, C) = sizes
    (
        latent, gain_in, shift_in, w_l, up_w, gain_b_in, shift_b_in, w_b, cot,
        decoded, grad_up, grad_w, grad_gs,
        lbuf, gall, gain_b, shift_b, wl, abuf, part, partf, parts_in, stat2, stat3, upw, wb,
        ub, std, ab, cb, cot3, gw, gy, gf, gs, gz, tmp, lace, send_sem, recv_sem, local_sem,
    ) = refs
    d, t, h = lax.axis_index("dp"), lax.axis_index("tm"), lax.axis_index("height")
    N = T * H
    FL = T * Fl
    U = H * CH // T
    band = Rl // H
    q = lax.rem(d, 4)
    half, side = lax.rem(q, 2), q // 2
    pair = d + 1 - 2 * half
    across = d + 2 - 4 * side
    counts = [0, 0]

    def new_send():
        counts[0] += 1
        return send_sem.at[counts[0] - 1]

    def new_recv(n=1):
        counts[1] += n
        return recv_sem.at[counts[1] - 1] if n == 1 else counts[1] - n

    def at(kt, kh):
        return (d, lax.rem(t + kt, T), lax.rem(h + kh, H))

    def copy(src, dst, device, s_sem, r_sem):
        return pltpu.make_async_remote_copy(
            src_ref=src, dst_ref=dst, send_sem=s_sem, recv_sem=r_sem,
            device_id=device, device_id_type=MESH,
        )

    def go(*what):
        copy(*what).start()

    pair_dev, across_dev = (pair, t, h), (across, t, h)
    left = []

    def got(name, ref, r_sem):
        with scope(name):
            copy(ref, ref, pair_dev, send_sem.at[0], r_sem).wait_recv()

    def left_all(ref, s_sem):
        left.append((ref, s_sem))

    def scope(name):
        return jax.named_scope(name)

    peers = [(kt, kh) for kh in [*range(H // 2, H), *range(1, H // 2), 0] for kt in range(T) if kt or kh]
    shard = w_b.shape[0]

    def local_copy(k, src, dst):
        made = pltpu.make_async_copy(src, dst, local_sem.at[k])
        made.start()
        return made

    def other(i):
        where = 0
        for hh in range(H):
            where = where + jnp.where(h == hh, hh ^ (i + 1), 0)
        return where

    nearest = [other(i) for i in range(H - 1)]

    class Along:
        def __init__(self, s_sem):
            self.s, self.base = s_sem, new_recv(H - 1)

        def send(self, i, src, dst):
            to = nearest[i]
            r = recv_sem.at[self.base + lax.rem(to - h + H, H) - 1]
            go(src, dst, (d, t, to), self.s, r)

        def wait(self, name, i, ref):
            got(name, ref, recv_sem.at[self.base + lax.rem(h - nearest[i] + H, H) - 1])

    own_l = local_copy(0, latent, lbuf.at[t, h])
    cb[...] = jnp.zeros(cb.shape, BF16)
    barrier = pltpu.get_barrier_semaphore()
    for kt, kh in peers:
        pl.semaphore_signal(barrier, inc=1, device_id=at(kt, kh), device_id_type=MESH)
    pl.semaphore_signal(barrier, inc=1, device_id=pair_dev, device_id_type=MESH)
    pl.semaphore_signal(barrier, inc=1, device_id=across_dev, device_id_type=MESH)
    own_w = local_copy(2, w_b, wb.at[pl.ds(pl.multiple_of((t * H + h) * shard, shard), shard)])
    own_g = [
        local_copy(5, gain_in, gall.at[h, pl.ds(0, 1)]),
        local_copy(6, shift_in, gall.at[h, pl.ds(1, 1)]),
        local_copy(7, gain_b_in, gain_b), local_copy(8, shift_b_in, shift_b),
    ]
    own_up = local_copy(1, up_w, upw.at[pl.ds(pl.multiple_of(h * CH, CH), CH)])
    own_c = local_copy(4, cot, cb.at[pl.ds(0, F), pl.ds(1, R)])
    own_wl = local_copy(3, w_l, wl)
    abuf[...] = jnp.zeros(abuf.shape, BF16)
    ab[...] = jnp.zeros(ab.shape, BF16)
    own_l.wait()
    with scope("w_barrier"):
        pl.semaphore_wait(barrier, N + 1)

    yes = at(1, 0)
    w_half = shard // 2
    half_cols = pl.ds(pl.multiple_of(half * (C2 // 2), C2 // 2), C2 // 2)

    def w_piece(gt, gh, piece_side):
        start = pl.multiple_of((gt * H + gh) * shard + piece_side * w_half, w_half)
        return wb.at[pl.ds(start, w_half), half_cols]

    def w_both(gt, gh):
        return wb.at[pl.ds(pl.multiple_of((gt * H + gh) * shard, shard), shard), half_cols]

    up_rows, up_cols = CH // T, 2 * C2

    def up_piece(gt, gh, n=1):
        first = 2 * half + (side if n == 1 else 0)
        return upw.at[
            pl.ds(pl.multiple_of(gh * CH + gt * up_rows, up_rows), up_rows),
            pl.ds(pl.multiple_of(first * up_cols, up_cols), n * up_cols),
        ]

    mine = lbuf.at[t, h]
    lz = Along(new_send())
    ly_s, ly_r = new_send(), new_recv()
    for i in range(H - 1):
        lz.send(i, mine, mine)
    go(mine, mine, yes, ly_s, ly_r)
    own_w.wait()
    w_s = new_send()
    w_mine = w_piece(t, h, side)
    wy_r = [new_recv() for _ in range(H)]
    go(w_both(t, h), w_both(t, h), yes, w_s, wy_r[H - 1])
    for made in own_g:
        made.wait()
    gain_s, gain_r = new_send(), new_recv()
    for kh in range(1, H):
        go(gall.at[h], gall.at[h], at(0, kh), gain_s, gain_r)
    own_up.wait()
    u_s = new_send()
    uz = Along(u_s)

    def up_send(core):
        @pl.when(half == core)
        def _():
            for i in range(H - 1):
                uz.send(i, up_piece(t, h), up_piece(t, h))

    up_send(0)
    for i in range(H - 1):
        if i == 2:
            up_send(1)
        piece = lbuf.at[t, nearest[i]]
        lz.wait("w_lz", i, piece)
        go(piece, piece, yes, ly_s, ly_r)
    left_all(lbuf.at[0, pl.ds(0, H - 1)], lz.s)
    left_all(lbuf.at[0], ly_s)
    left_all(gall.at[pl.ds(0, H - 1)], gain_s)

    wx_r, wx_at = [], []
    wpair_r = new_recv()

    def w_across(gt, gh):
        wx_r.append(new_recv())
        wx_at.append((gt, gh))
        go(w_piece(gt, gh, side), w_piece(gt, gh, side), across_dev, w_s, wx_r[-1])

    def w_pair(k):
        gt, gh = wx_at[k]
        got("w_wx", w_piece(gt, gh, 1 - side), wx_r[k])
        go(w_both(gt, gh), w_both(gt, gh), pair_dev, w_s, wpair_r)


    def halo(buffer, f0, f_two, two_at, step):
        made = []
        ok_t_send = (t < T - 1) if step == 1 else (t > 0)
        ok_t_recv = (t > 0) if step == 1 else (t < T - 1)
        kt = step % T

        def part_of(fs, n_f, r0, n_r):
            return buffer.at[pl.ds(fs, n_f), pl.ds(r0, n_r)]

        for kt_, kh_, ok_s, ok_r, src, dst in (
            (kt, 0, ok_t_send, ok_t_recv, part_of(f_two, 2, 1, R), part_of(two_at, 2, 1, R)),
            (0, 1, h < H - 1, h > 0, part_of(f0, F, R, 1), part_of(f0, F, 0, 1)),
            (0, H - 1, h > 0, h < H - 1, part_of(f0, F, 1, 1), part_of(f0, F, R + 1, 1)),
            (kt, 1, ok_t_send & (h < H - 1), ok_t_recv & (h > 0),
             part_of(f_two, 2, R, 1), part_of(two_at, 2, 0, 1)),
            (kt, H - 1, ok_t_send & (h > 0), ok_t_recv & (h < H - 1),
             part_of(f_two, 2, 1, 1), part_of(two_at, 2, R + 1, 1)),
        ):
            c = copy(src, dst, at(kt_, kh_), new_send(), new_recv())
            pl.when(ok_s)(c.start)
            made.append((c, ok_s, ok_r))
        return made

    uy_r = [new_recv() for _ in range(H - 1)]
    ux_r = [new_recv(), new_recv()]
    upair_r = new_recv()

    def up_height(i):
        piece = up_piece(t, nearest[i])
        uz.wait("w_uz", i, piece)
        go(piece, piece, yes, u_s, uy_r[i])
        go(piece, piece, across_dev, u_s, ux_r[0])

    up_height(0)
    got("w_ly", lbuf.at[0], ly_r)
    got("w_gain", gall.at[pl.ds(0, H - 1)], gain_r)
    up_height(1)
    wz = Along(w_s)
    own_c.wait()
    wz.send(0, w_mine, w_mine)
    wz.send(1, w_mine, w_mine)

    per_l = H * CH // GROUPS
    cells_l = FL * Rl * Cl
    count_l = cells_l * per_l
    xs, rows = [], []
    for k in range(H):
        x = lbuf[:, k].astype(F32).reshape(cells_l, CH)
        rows += [jnp.sum(x, 0, keepdims=True), jnp.sum(x * x, 0, keepdims=True)]
    total = over_groups(jnp.concatenate(rows, 0), per_l) / count_l
    for k in range(H):
        mean = total[2 * k : 2 * k + 1]
        inv = lax.rsqrt(total[2 * k + 1 : 2 * k + 2] - mean * mean + epsilon)
        x = lbuf[:, k].astype(F32).reshape(cells_l, CH)
        v = (x - mean) * inv * gall[k, 0:1] + gall[k, 1:2]
        lane = k * CH % U
        abuf[k * CH // U, 2 : 2 + FL, 1 : 1 + Rl, :, lane : lane + CH] = (
            (v * jax.nn.sigmoid(v)).astype(BF16).reshape(FL, Rl, Cl, CH)
        )

    up_height(2)

    own_wl.wait()

    parts_of = 2
    some = FL // parts_of

    def window(m, chunk, tap):
        lag, dr = tap // 9, (tap // 3) % 3
        return abuf[chunk, pl.ds(lag + m * some, some), pl.ds(dr, Rl)].reshape(some * Rl * Cl, U)

    def w_rows(chunk, tap):
        return wl[pl.ds(pl.multiple_of((tap * T + chunk - 27 * t) * U, U), U), :]

    with scope("c_latent"):
        sums = [None] * parts_of
        for g in range(4):
            tap = jnp.where(t == 0, 3 * g, 15 + 3 * g)
            for chunk in range(T):
                k3 = jnp.concatenate([w_rows(chunk, tap + dc) for dc in range(3)], 1)
                for m in range(parts_of):
                    term = jnp.dot(window(m, chunk, tap), k3, preferred_element_type=F32)
                    sums[m] = term if sums[m] is None else sums[m] + term
        alone = jnp.where(t == 0, 12, 14)
        k2 = jnp.concatenate([w_rows(t, alone), w_rows(t, 13)], 1)
        mixed = []
        for m in range(parts_of):
            both = jnp.dot(window(m, t, alone), k2, preferred_element_type=F32)
            lone = both[:, :CH] + jnp.dot(
                window(m, 1 - t, alone), w_rows(1 - t, alone), preferred_element_type=F32
            )
            first = sums[m][:, :CH] + jnp.where(t == 0, lone, 0.0)
            last = sums[m][:, 2 * CH :] + jnp.where(t == 0, 0.0, lone)
            mixed.append(
                column_shift(first, Cl, 1) + sums[m][:, CH : 2 * CH] + both[:, CH:]
                + column_shift(last, Cl, -1)
            )
        mixed = jnp.concatenate(mixed, 0)
        partf[...] = mixed.reshape(FL, Rl, Cl, CH)
        partf[pl.ds(t * Fl, Fl)] += lbuf[t, h].astype(F32)
        part[...] = partf[...].astype(BF16)
    p_s, p_r = new_send(), new_recv()
    for kt, kh in peers:
        dev = at(kt, kh)
        go(part.at[pl.ds(dev[1] * Fl, Fl), pl.ds(dev[2] * band, band)],
           parts_in.at[kt * H + kh], dev, p_s, p_r)
    wz.send(2, w_mine, w_mine)

    def w_height(i):
        piece = w_piece(t, nearest[i], side)
        wz.wait("w_wz", i, piece)
        go(piece, piece, yes, w_s, wy_r[i])
        w_across(t, nearest[i])

    piece = up_piece(1 - t, nearest[0])
    got("w_uy", piece, uy_r[0])
    go(piece, piece, across_dev, u_s, ux_r[1])
    piece = up_piece(1 - t, nearest[1])
    got("w_uy", piece, uy_r[1])
    go(piece, piece, across_dev, u_s, ux_r[1])
    piece = up_piece(1 - t, nearest[2])
    got("w_uy", piece, uy_r[2])
    go(piece, piece, across_dev, u_s, ux_r[1])
    w_height(0)
    cot_halo = halo(cb, 0, 0, F, -1)
    got("w_ux", upw.at[pl.ds(0, (H - 1) * up_rows), pl.ds(0, up_cols)], ux_r[0])
    for i in range(H - 1):
        piece = up_piece(t, nearest[i], 2)
        go(piece, piece, pair_dev, u_s, upair_r)
    got("w_wy0", w_both(1 - t, h), wy_r[H - 1])
    go(w_both(1 - t, h), w_both(1 - t, h), pair_dev, w_s, wpair_r)
    got("w_ux", upw.at[pl.ds(0, (H - 1) * up_rows), pl.ds(0, up_cols)], ux_r[1])
    for i in range(H - 1):
        piece = up_piece(1 - t, nearest[i], 2)
        go(piece, piece, pair_dev, u_s, upair_r)
    w_height(1)
    got("w_upair", upw.at[pl.ds(0, (H - 1) * CH), pl.ds(0, 4 * C2)], upair_r)
    got("w_parts", parts_in.at[pl.ds(1, N - 1)], p_r)
    left_all(parts_in.at[pl.ds(1, N - 1)], p_s)
    left_all(upw.at[pl.ds(0, (H - 1) * CH)], u_s)

    cells_b = Fl * band * Cl
    with scope("c_up"):
        parts_own = partf[pl.ds(t * Fl, Fl), pl.ds(h * band, band)]
        expanded = jnp.zeros((cells_b, 8 * C2), F32)
        for kh in range(H):
            value = parts_own if kh == 0 else parts_in[kh].astype(F32)
            for kt in range(1, T):
                value = value + parts_in[kt * H + kh].astype(F32)
            refined = value.reshape(cells_b, CH).astype(BF16)
            source = lax.rem(h + H - kh, H)
            expanded = expanded + jnp.dot(
                refined, upw[pl.ds(pl.multiple_of(source * CH, CH), CH), :],
                preferred_element_type=F32,
            )
        expanded = expanded.astype(BF16).astype(F32)
        for f in range(Fl):
            for r in range(band):
                for p in range(2):
                    for qq in range(2):
                        for s in range(2):
                            first = (f * band + r) * Cl
                            col = ((p * 2 + qq) * 2 + s) * C2
                            for n in range(C2 // 128):
                                lace[
                                    n, pl.ds(((2 * f + p) * R + 2 * r + qq) * C + s, Cl, stride=2), :
                                ] = expanded[first : first + Cl, col + n * 128 : col + (n + 1) * 128]

        cells = F * R * C
        me = t * H + h
        up = jnp.concatenate([lace[n] for n in range(C2 // 128)], axis=1)
        stat2[me] = side_by_side(jnp.sum(up, 0, keepdims=True), jnp.sum(up * up, 0, keepdims=True))
        ub[2 : 2 + F, 1 : 1 + R] = up.astype(BF16).reshape(F, R, C, C2)
    s2_s, s2_r = new_send(), new_recv()
    for kt, kh in peers:
        go(stat2.at[me], stat2.at[me], at(kt, kh), s2_s, s2_r)
    left_all(stat2.at[pl.ds(0, N - 1)], s2_s)
    up_halo = halo(ub, 2, F, 0, 1)

    w_height(2)
    got("w_wy", w_piece(1 - t, nearest[0], side), wy_r[0])
    w_across(1 - t, nearest[0])
    with scope("w_cothalo"):
        for made, _, ok in cot_halo:
            pl.when(ok)(made.wait_recv)
    wide = cb[0:F].astype(F32).reshape(F * (R + 2) * C, C2)
    cot3[:, :, :, 0:C2] = column_shift(wide, C, -1).astype(BF16).reshape(F, R + 2, C, C2)
    cot3[:, :, :, C2 : 2 * C2] = cb[0:F]
    cot3[:, :, :, 2 * C2 :] = column_shift(wide, C, 1).astype(BF16).reshape(F, R + 2, C, C2)

    got("w_wy", w_piece(1 - t, nearest[1], side), wy_r[1])
    w_across(1 - t, nearest[1])
    got("w_s2", stat2.at[pl.ds(0, N - 1)], s2_r)
    per_b = C2 // GROUPS
    count_b = cells * per_b * N
    total = stat2[0]
    for k in range(1, N):
        total = total + stat2[k]
    total = over_groups(jnp.concatenate([total[:, :C2], total[:, C2:]], 0), per_b) / count_b
    mean_b = total[0:1]
    inv_b = lax.rsqrt(total[1:2] - mean_b * mean_b + epsilon)

    def activate(values):
        normed = (values - mean_b) * inv_b * gain_b[...] + shift_b[...]
        return (normed * jax.nn.sigmoid(normed)).astype(BF16)

    with scope("c_gw"):
        own = activate(ub[2 : 2 + F, 1 : 1 + R].astype(F32).reshape(cells, C2))
        ab[2 : 2 + F, 1 : 1 + R] = own.reshape(F, R, C, C2)
        def taps_of(i):
            dr = jnp.where(t == 0, 2 - i, i)
            term = lax.dot_general(
                own, cot3[:, pl.ds(2 - dr, R)].reshape(cells, 3 * C2),
                (((0,), (0,)), ((), ())), preferred_element_type=F32,
            )
            for dc in range(3):
                gw[pl.ds(pl.multiple_of((dr * 3 + dc) * C2, C2), C2), :] = (
                    term[:, dc * C2 : (dc + 1) * C2].astype(BF16)
                )

        taps_of(0)
        taps_of(1)
    out_rows = 9 * C2 // N
    y_rows = out_rows * H

    cut_rows = out_rows // CUTS

    def cut(c):
        return pl.ds(c * cut_rows, cut_rows)

    def g_at(gt, gh, c):
        start = (gt * H + gh) * out_rows + c * cut_rows
        return pl.ds(pl.multiple_of(start, cut_rows), cut_rows)

    def g_rows(gt, gh, c):
        return gw.at[g_at(gt, gh, c)]

    def ahead(kh):
        return lax.rem(h + kh, H)

    order = [*range(H // 2, H), *range(1, H // 2), 0]
    gy_s, gz_s, gz_r = new_send(), new_send(), new_recv()
    gy_r = {(kh, c): new_recv() for kh in order for c in range(CUTS) if (kh, c) != (1, 0)}
    first_cut = (1, 0)
    steps = [(kh, c) for kh in order for c in range(CUTS) if (kh, c) != first_cut]
    for kh, c in steps:
        if (kh, c) != (0, 0):
            go(g_rows(1 - t, ahead(kh), c), gy.at[kh, cut(c)], yes, gy_s, gy_r[kh, c])
    zf_s, zf_r = new_send(), new_recv()
    go(g_rows(1 - t, ahead(1), 0), gf.at[1], at(0, 1), zf_s, zf_r)
    with scope("c_gw2"):
        taps_of(2)
    go(g_rows(t, ahead(1), 0), gf.at[0], at(0, 1), zf_s, zf_r)
    left_all(gw.at[pl.ds(0, len(steps) * cut_rows)], gy_s)
    left_all(gf, zf_s)

    def g_join():
        got("w_gf", gf, zf_r)
        total = gw[g_at(1 - t, h, 0), :].astype(F32) + gf[1].astype(F32)
        gs[0, :cut_rows] = total.astype(BF16)
        go(gs.at[0, cut(0)], gy.at[0, cut(0)], yes, gy_s, gy_r[0, 0])

    with scope("w_uphalo"):
        for made, _, ok in up_halo:
            pl.when(ok)(made.wait_recv)
    with scope("c_halo"):
        for rows_at, n_rows, ok in ((0, 1, h > 0), (R + 1, 1, h < H - 1)):
            @pl.when(ok)
            def _():
                v = ub[2 : 2 + F, rows_at : rows_at + n_rows].astype(F32).reshape(F * n_rows * C, C2)
                ab[2 : 2 + F, rows_at : rows_at + n_rows] = activate(v).reshape(F, n_rows, C, C2)
        for rows_at, n_rows, ok in (
            (1, R, t > 0), (0, 1, (t > 0) & (h > 0)), (R + 1, 1, (t > 0) & (h < H - 1))
        ):
            @pl.when(ok)
            def _():
                v = ub[0:2, rows_at : rows_at + n_rows].astype(F32).reshape(2 * n_rows * C, C2)
                ab[0:2, rows_at : rows_at + n_rows] = activate(v).reshape(2, n_rows, C, C2)

    def g_on(kh, c):
        got("w_gy", gy.at[kh, cut(c)], gy_r[kh, c])
        total = gy[kh, c * cut_rows : (c + 1) * cut_rows].astype(F32)
        total = total + gw[g_at(t, ahead(kh), c), :].astype(F32)
        if (kh, c) == (0, 0):
            total = total + gf[0].astype(F32)
        if kh == 0:
            grad_w[c * cut_rows : (c + 1) * cut_rows] = total
        else:
            gs[kh, c * cut_rows : (c + 1) * cut_rows] = total.astype(BF16)
            go(gs.at[kh, cut(c)], gz.at[kh, cut(c)], at(0, kh), gz_s, gz_r)

    got("w_wy", w_piece(1 - t, nearest[2], side), wy_r[2])
    w_across(1 - t, nearest[2])
    w_pair(0)
    w_pair(1)
    g_on(*steps[0])
    w_pair(2)
    g_on(*steps[1])
    g_join()
    w_pair(3)
    w_pair(4)
    w_pair(5)
    left_all(gw.at[pl.ds(0, (len(steps) - CUTS) * cut_rows)], gz_s)
    got("w_wpair", wb.at[pl.ds(0, (N - 1) * shard), pl.ds(0, C2 // 2)], wpair_r)
    left_all(wb.at[pl.ds(0, (2 * H + 3 * N - 4) * w_half // 2)], w_s)

    with scope("c_gradtap"):
        sums = {}
        for j in range(9):
            lag, dr = j // 3, j % 3
            win = cb[2 - lag : 2 - lag + F, 2 - dr : 2 - dr + R].reshape(cells, C2)
            for dc in range(3):
                term = lax.dot_general(
                    win, wb[(j * 3 + dc) * C2 : (j * 3 + dc + 1) * C2, :],
                    (((1,), (1,)), ((), ())), preferred_element_type=F32,
                )
                key = (dc, j % 2 if dc == 1 else 0)
                sums[key] = sums[key] + term if key in sums else term
        grad_active = (
            column_shift(sums[0, 0], C, -1) + sums[1, 0] + sums[1, 1]
            + column_shift(sums[2, 0], C, 1)
        )
    standard = (ub[2 : 2 + F, 1 : 1 + R].astype(F32).reshape(cells, C2) - mean_b) * inv_b
    std[...] = standard
    normed = standard * gain_b[...] + shift_b[...]
    sigmoid = jax.nn.sigmoid(normed)
    grad_normed = grad_active * sigmoid * (1.0 + normed * (1.0 - sigmoid))
    stat3[me] = side_by_side(
        jnp.sum(grad_normed * standard, 0, keepdims=True), jnp.sum(grad_normed, 0, keepdims=True)
    )
    s3_s, s3_r = new_send(), new_recv()
    for kt, kh in peers:
        go(stat3.at[me], stat3.at[me], at(kt, kh), s3_s, s3_r)
    left_all(stat3.at[pl.ds(0, N - 1)], s3_s)
    tmp[...] = grad_normed * gain_b[...]
    for step in steps[2:5]:
        g_on(*step)

    some = F // 2
    n = some * R * C
    for m in range(2):
        with scope("c_tap"):
            wide = None
            for j in range(9):
                lag, dr = j // 3, j % 3
                k3 = jnp.concatenate(
                    [wb[(j * 3 + dc) * C2 : (j * 3 + dc + 1) * C2, :] for dc in range(3)], 1
                )
                win = ab[lag + m * some : lag + (m + 1) * some, dr : dr + R].reshape(n, C2)
                term = jnp.dot(win, k3, preferred_element_type=F32)
                wide = term if wide is None else wide + term
            decoded[m * some : (m + 1) * some] = (
                (column_shift(wide[:, :C2], C, 1) + wide[:, C2 : 2 * C2]
                 + column_shift(wide[:, 2 * C2 :], C, -1)
                 + ub[2 + m * some : 2 + (m + 1) * some, 1 : 1 + R].astype(F32).reshape(n, C2))
                .astype(BF16).reshape(some, R, C, C2)
            )
        for step in steps[5:5] if m == 0 else steps[5 : -CUTS]:
            g_on(*step)

    got("w_s3", stat3.at[pl.ds(0, N - 1)], s3_r)
    total = stat3[0]
    for k in range(1, N):
        total = total + stat3[k]
    total = two_rows(total[:, :C2], total[:, C2:])
    grad_gs[...] = total
    means = over_groups(total * gain_b[...], per_b) / count_b
    corrected = (tmp[...] - means[1:2] - std[...] * means[0:1]) * inv_b
    grad_up[...] = (
        cb[0:F, 1 : 1 + R].astype(F32).reshape(cells, C2) + corrected
    ).astype(BF16).reshape(F, R, C, C2)

    for step in steps[-CUTS:]:
        g_on(*step)
    got("w_gz", gw.at[pl.ds(0, (len(steps) - CUTS) * cut_rows)], gz_r)
    for c in range(CUTS):
        rows = slice(c * cut_rows, (c + 1) * cut_rows)
        result = grad_w[rows]
        for kh in range(1, H):
            if (kh, c) != first_cut:
                result = result + gz[kh, rows].astype(F32)
        grad_w[rows] = result

    with scope("w_send"):
        for ref, s_sem in left:
            copy(ref, ref, pair_dev, s_sem, recv_sem.at[0]).wait_send()
        for made, ok, _ in cot_halo + up_halo:
            pl.when(ok)(made.wait_send)
    assert counts == [n_send, n_recv], counts


def finish_kernel(decoded, grad_up, grad_w, grad_gs, out_d, out_u, out_w, out_g, out_s, sems):
    moves = [
        pltpu.make_async_copy(src, dst, sems.at[k])
        for k, (src, dst) in enumerate((
            (decoded, out_d), (grad_up, out_u), (grad_w, out_w),
            (grad_gs.at[pl.ds(0, 1)], out_g), (grad_gs.at[pl.ds(1, 1)], out_s),
        ))
    ]
    for move in moves:
        move.start()
    for move in moves:
        move.wait()


def stay(array):
    return pltpu.with_memory_space_constraint(array, pltpu.HBM)


def local_block(shape, *args):
    (latent, gain_l, shift_l, w_l, up_w, gain_b, shift_b, w_b, cot) = args
    T, H = shape["tm"], shape["height"]
    Fl, Rl, Cl, CH = latent.shape
    F, R, C, C2 = cot.shape
    N = T * H
    U = H * CH // T
    fits = (
        shape["dp"] % 4 == 0 and T == 2 and H == 4
        and CH % 128 == 0 and U % CH == 0
        and w_b.shape[0] % 32 == 0 and (CH // T) % 16 == 0
        and (9 * C2) % (16 * CUTS * N) == 0 and C2 % 256 == 0
        and Cl % 16 == 0 and w_l.shape[0] == 27 * U and F >= 2
    )
    if not fits:
        return local(*args)
    sizes = (T, H, Fl, Rl, Cl, CH, C2, F, R, C)
    n_send = 21
    n_recv = 20 + 4 * (H - 1) + (1 + CUTS) * H + N - 2
    FL = T * Fl
    band = Rl // H
    cells = F * R * C
    out_rows = 9 * C2 // N
    vmem = pl.BlockSpec(memory_space=pltpu.VMEM)
    hbm = pl.BlockSpec(memory_space=pltpu.HBM)
    flops = 2 * (FL * Rl * Cl * w_l.size + 2 * cells * 27 * C2 * C2 + cells * 9 * C2 * C2)
    outs = pl.pallas_call(
        functools.partial(block_kernel, sizes, n_send, n_recv),
        out_shape=(
            jax.ShapeDtypeStruct(cot.shape, BF16),
            jax.ShapeDtypeStruct(cot.shape, BF16),
            jax.ShapeDtypeStruct((out_rows, C2), F32),
            jax.ShapeDtypeStruct((8, C2), F32),
        ),
        in_specs=[hbm] * 9,
        out_specs=(vmem,) * 4,
        scratch_shapes=[
            pltpu.VMEM((T, H, Fl, Rl, Cl, CH), BF16),
            pltpu.VMEM((H, 2, CH), F32),
            pltpu.VMEM((1, C2), F32),
            pltpu.VMEM((1, C2), F32),
            pltpu.VMEM(w_l.shape, BF16),
            pltpu.VMEM((T, FL + 2, Rl + 2, Cl, U), BF16),
            pltpu.VMEM((FL, Rl, Cl, CH), BF16),
            pltpu.VMEM((FL, Rl, Cl, CH), F32),
            pltpu.VMEM((N, Fl, band, Cl, CH), BF16),
            pltpu.VMEM((N, 1, 2 * C2), F32),
            pltpu.VMEM((N, 1, 2 * C2), F32),
            pltpu.VMEM((H * CH, 8 * C2), BF16),
            pltpu.VMEM((27 * C2, C2), BF16),
            pltpu.VMEM((F + 2, R + 2, C, C2), BF16),
            pltpu.VMEM((cells, C2), F32),
            pltpu.VMEM((F + 2, R + 2, C, C2), BF16),
            pltpu.VMEM((F + 2, R + 2, C, C2), BF16),
            pltpu.VMEM((F, R + 2, C, 3 * C2), BF16),
            pltpu.VMEM((9 * C2, C2), BF16),
            pltpu.VMEM((H, out_rows, C2), BF16),
            pltpu.VMEM((2, out_rows // CUTS, C2), BF16),
            pltpu.VMEM((H, out_rows, C2), BF16),
            pltpu.VMEM((H, out_rows, C2), BF16),
            pltpu.VMEM((cells, C2), F32),
            pltpu.VMEM((C2 // 128, cells, 128), F32),
            pltpu.SemaphoreType.DMA((n_send,)),
            pltpu.SemaphoreType.DMA((n_recv,)),
            pltpu.SemaphoreType.DMA((9,)),
        ],
        compiler_params=pltpu.CompilerParams(
            collective_id=0, has_side_effects=True, vmem_limit_bytes=VMEM_LIMIT
        ),
        cost_estimate=pl.CostEstimate(flops=flops, bytes_accessed=1 << 23, transcendentals=0),
    )(
        stay(latent), stay(gain_l.reshape(1, -1)), stay(shift_l.reshape(1, -1)), stay(w_l), stay(up_w),
        stay(gain_b.reshape(1, -1)), stay(shift_b.reshape(1, -1)), stay(w_b), stay(cot),
    )
    row = jax.ShapeDtypeStruct((1, C2), F32)
    done = pl.pallas_call(
        finish_kernel,
        out_shape=tuple(jax.ShapeDtypeStruct(a.shape, a.dtype) for a in outs[:3]) + (row, row),
        in_specs=[vmem] * 4,
        out_specs=(hbm,) * 5,
        scratch_shapes=[pltpu.SemaphoreType.DMA((5,))],
        compiler_params=pltpu.CompilerParams(vmem_limit_bytes=1 << 20),
        cost_estimate=pl.CostEstimate(flops=0, bytes_accessed=1 << 20, transcendentals=0),
    )(*outs)
    return done[0], done[1], done[2], done[3].reshape(C2), done[4].reshape(C2)


def solution(mesh):
    return jax.shard_map(
        functools.partial(local_block, dict(mesh.shape)),
        mesh=mesh,
        in_specs=(
            P(("dp", "tm"), None, None, "height"),
            P("height"),
            P("height"),
            P("tm", "height"),
            P("height", None),
            P(),
            P(),
            P(("tm", "height"), None),
            P(("dp", "tm"), "height", None, None),
        ),
        out_specs=(
            P(("dp", "tm"), "height", None, None),
            P(("dp", "tm"), "height", None, None),
            P(("dp", "tm", "height"), None),
            P("dp"),
            P("dp"),
        ),
        check_vma=False,
    )
```

```python
import functools

import jax
import jax.numpy as jnp
from jax import lax
from jax.experimental import pallas as pl
from jax.experimental.pallas import tpu as pltpu
from jax.sharding import PartitionSpec as P

C1 = 512
GROUPS = 32


epsilon = 1e-06


def shifted(block, axis, distance):
    devices = range(lax.axis_size(axis))
    route = [(i - distance, i) for i in devices if i - distance in devices]
    return lax.ppermute(block, axis, route)


def extended_2(cells, sides, width):
    for axis, dim in sides:
        count = lax.axis_size(axis)
        ends = count - 1
        head = lax.slice_in_dim(cells, 0, width, axis=dim)
        tail = lax.slice_in_dim(cells, cells.shape[dim] - width, cells.shape[dim], axis=dim)
        cells = jnp.concatenate(
            [
                lax.ppermute(tail, axis, [(i, (i + 1) % count) for i in range(ends)]),
                cells,
                lax.ppermute(head, axis, [((i + 1) % count, i) for i in range(ends)]),
            ],
            axis=dim,
        )
    return cells


def standardize(values, mean_value, inverse, groups):
    shape_full = values.shape
    grouped = values.reshape(shape_full[:-1] + (groups, shape_full[-1] // groups))
    return ((grouped - mean_value[:, None]) * inverse[:, None]).reshape(shape_full)


def causal_taps(padded, weight, frames, rows, cols):
    channels_in = padded.shape[-1]
    summed = jnp.zeros((frames * rows * cols, weight.shape[1]), jnp.float32)
    for lag_step in range(3):
        for row_step in range(3):
            for col_step in range(3):
                tap_index = (lag_step * 3 + row_step) * 3 + col_step
                window = padded[
                    lag_step : lag_step + frames,
                    row_step : row_step + rows,
                    col_step : col_step + cols,
                ]
                kernel = weight[tap_index * channels_in : (tap_index + 1) * channels_in]
                summed = summed + jnp.dot(
                    window.reshape(-1, channels_in), kernel, preferred_element_type=jnp.float32
                )
    return summed.reshape(frames, rows, cols, weight.shape[1])


def transposed_taps(padded, weight, frames, rows, cols):
    channels_out = padded.shape[-1]
    channels_in = weight.shape[0] // 27
    summed = jnp.zeros((frames * rows * cols, channels_in), jnp.float32)
    for lag_step in range(3):
        for row_step in range(3):
            for col_step in range(3):
                tap_index = (lag_step * 3 + row_step) * 3 + col_step
                window = padded[
                    2 - lag_step : 2 - lag_step + frames,
                    2 - row_step : 2 - row_step + rows,
                    2 - col_step : 2 - col_step + cols,
                ]
                kernel = weight[tap_index * channels_in : (tap_index + 1) * channels_in]
                summed = summed + lax.dot_general(
                    window.reshape(-1, channels_out),
                    kernel,
                    (((1,), (1,)), ((), ())),
                    preferred_element_type=jnp.float32,
                )
    return summed.reshape(frames, rows, cols, channels_in)


def weight_terms(padded, grads, frames, rows, cols):
    channels_in = padded.shape[-1]
    flat_grads = grads.reshape(-1, grads.shape[-1])
    blocks = []
    for row_step in range(3):
        for col_step in range(3):
            window = padded[2 : 2 + frames, row_step : row_step + rows, col_step : col_step + cols]
            blocks.append(
                lax.dot_general(
                    window.reshape(-1, channels_in),
                    flat_grads,
                    (((0,), (0,)), ((), ())),
                    preferred_element_type=jnp.float32,
                )
            )
    return jnp.concatenate(blocks, 0)


def local(
    latent,
    gain_latent,
    shift_latent,
    conv_latent,
    up_weight,
    gain_block,
    shift_block,
    conv_block,
    cotangent,
):
    per_group = C1 // GROUPS
    groups_here = latent.shape[-1] // per_group
    latent_f32 = latent.astype(jnp.float32)
    grouped = latent_f32.reshape(-1, groups_here, per_group)
    first_sums = jnp.sum(grouped, axis=(0, 2))
    second_sums = jnp.sum(grouped * grouped, axis=(0, 2))
    first_totals, second_totals = lax.psum((first_sums, second_sums), "tm")
    count_latent = grouped.shape[0] * per_group * lax.axis_size("tm")
    mean_latent = first_totals / count_latent
    inverse_latent = lax.rsqrt(second_totals / count_latent - mean_latent * mean_latent + epsilon)
    normed = (
        standardize(latent_f32, mean_latent, inverse_latent, groups_here) * gain_latent
        + shift_latent
    )
    active = jax.nn.silu(normed).astype(jnp.bfloat16)
    earlier = shifted(active, "tm", 1)
    extended = jnp.concatenate([earlier, active], 0)
    all_channels = lax.all_gather(extended, "height", axis=3, tiled=True)
    padded = jnp.pad(all_channels, ((0, 0), (1, 1), (1, 1), (0, 0)))
    latent_weight = lax.all_gather(conv_latent, "tm", axis=0, tiled=True)
    frames_latent, rows_latent, cols_latent = (latent.shape[0], latent.shape[1], latent.shape[2])
    mixed = causal_taps(padded, latent_weight, frames_latent, rows_latent, cols_latent)
    refined = (latent_f32 + mixed).astype(jnp.bfloat16)
    band_rows = rows_latent // lax.axis_size("height")
    own_band = lax.all_to_all(refined, "height", split_axis=1, concat_axis=3, tiled=True)
    flat_band = own_band.reshape(-1, own_band.shape[-1])
    expanded = jnp.dot(
        flat_band,
        lax.all_gather(up_weight, "height", axis=0, tiled=True),
        preferred_element_type=jnp.float32,
    )
    channels_block = up_weight.shape[1] // 8
    spread = expanded.reshape(frames_latent, band_rows, cols_latent, 2, 2, 2, channels_block)
    spread = spread.transpose(0, 3, 1, 4, 2, 5, 6)
    upsampled = spread.reshape(
        2 * frames_latent, 2 * band_rows, 2 * cols_latent, channels_block
    ).astype(jnp.bfloat16)
    frames_block, rows_block, cols_block = (
        upsampled.shape[0],
        upsampled.shape[1],
        upsampled.shape[2],
    )
    up_f32 = upsampled.astype(jnp.float32)
    per_block = channels_block // GROUPS
    grouped_block = up_f32.reshape(-1, GROUPS, per_block)
    block_first = jnp.sum(grouped_block, axis=(0, 2))
    block_second = jnp.sum(grouped_block * grouped_block, axis=(0, 2))
    block_first, block_second = lax.psum((block_first, block_second), ("tm", "height"))
    count_block = grouped_block.shape[0] * per_block * lax.axis_size("tm") * lax.axis_size("height")
    mean_block = block_first / count_block
    inverse_block = lax.rsqrt(block_second / count_block - mean_block * mean_block + epsilon)
    standard = standardize(up_f32, mean_block, inverse_block, GROUPS)
    normed_block = standard * gain_block + shift_block
    active_block = jax.nn.silu(normed_block).astype(jnp.bfloat16)
    before = shifted(active_block[-2:], "tm", 1)
    ext_block = jnp.concatenate([before, active_block], 0)
    beside_all = extended_2(ext_block, (("height", 1),), 1)
    padded_block = jnp.pad(beside_all, ((0, 0), (0, 0), (1, 1), (0, 0)))
    block_weight = lax.all_gather(conv_block, ("tm", "height"), axis=0, tiled=True)
    mixed_block = causal_taps(padded_block, block_weight, frames_block, rows_block, cols_block)
    decoded = (up_f32 + mixed_block).astype(jnp.bfloat16)
    after = shifted(cotangent[:2], "tm", -1)
    grad_ext = jnp.concatenate([cotangent, after], 0)
    grad_around = extended_2(grad_ext, (("height", 1),), 1)
    grad_padded = jnp.pad(grad_around, ((0, 0), (0, 0), (1, 1), (0, 0)))
    grad_active = transposed_taps(grad_padded, block_weight, frames_block, rows_block, cols_block)
    local_terms = weight_terms(padded_block, cotangent, frames_block, rows_block, cols_block)
    grad_weight = lax.psum_scatter(local_terms, ("tm", "height"), scatter_dimension=0, tiled=True)
    sigmoid = jax.nn.sigmoid(normed_block)
    grad_normed = grad_active * sigmoid * (1.0 + normed_block * (1.0 - sigmoid))
    flat_grad = grad_normed.reshape(-1, channels_block)
    flat_standard = standard.reshape(-1, channels_block)
    grad_shift, grad_gain = lax.psum(
        (jnp.sum(flat_grad, axis=0), jnp.sum(flat_grad * flat_standard, axis=0)), ("tm", "height")
    )
    first_mean = jnp.sum((gain_block * grad_shift).reshape(GROUPS, per_block), axis=1) / count_block
    second_mean = jnp.sum((gain_block * grad_gain).reshape(GROUPS, per_block), axis=1) / count_block
    grouped_grad = (grad_normed * gain_block).reshape(-1, GROUPS, per_block)
    grouped_standard = standard.reshape(-1, GROUPS, per_block)
    corrected = (
        grouped_grad - first_mean[:, None] - grouped_standard * second_mean[:, None]
    ) * inverse_block[:, None]
    grad_upsampled = (cotangent.astype(jnp.float32) + corrected.reshape(cotangent.shape)).astype(
        jnp.bfloat16
    )
    return (decoded, grad_upsampled, grad_weight, grad_gain, grad_shift)


MESH = pl.DeviceIdType.MESH
VMEM_LIMIT = 32 * 1024 * 1024
CUTS = 2
F32 = jnp.float32
BF16 = jnp.bfloat16


def group_matrix(channels, per):
    row = lax.broadcasted_iota(jnp.int32, (channels, channels), 0) // per
    col = lax.broadcasted_iota(jnp.int32, (channels, channels), 1) // per
    return (row == col).astype(F32)


def over_groups(rows, per):
    return jnp.dot(
        rows,
        group_matrix(rows.shape[-1], per),
        precision=lax.Precision.HIGHEST,
        preferred_element_type=F32,
    )


def column_shift(cells, cols, step):
    count = cells.shape[0]
    column = lax.broadcasted_iota(jnp.int32, cells.shape, 0) % cols
    edge = 0 if step == 1 else cols - 1
    return jnp.where(column == edge, 0.0, pltpu.roll(cells, step % count, 0))


def two_rows(first, second):
    width = first.shape[-1]
    row = lax.broadcasted_iota(jnp.int32, (8, width), 0)
    return jnp.where(row == 0, first, jnp.where(row == 1, second, 0.0))


def side_by_side(first, second):
    return jnp.concatenate([first, second], 1)


def block_kernel(sizes, n_send, n_recv, *refs):
    (T, H, Fl, Rl, Cl, CH, C2, F, R, C) = sizes
    (
        latent, gain_in, shift_in, w_l, up_w, gain_b_in, shift_b_in, w_b, cot,
        decoded, grad_up, grad_w, grad_gs,
        lbuf, gall, gain_b, shift_b, wl, abuf, part, partf, parts_in, stat2, stat3, upw, wb,
        ub, std, ab, cb, cot3, gw, gy, gf, gs, gz, tmp, lace, send_sem, recv_sem, local_sem,
    ) = refs
    d, t, h = lax.axis_index("dp"), lax.axis_index("tm"), lax.axis_index("height")
    N = T * H
    FL = T * Fl
    U = H * CH // T
    band = Rl // H
    q = lax.rem(d, 4)
    half, side = lax.rem(q, 2), q // 2
    pair = d + 1 - 2 * half
    across = d + 2 - 4 * side
    counts = [0, 0]

    def new_send():
        counts[0] += 1
        return send_sem.at[counts[0] - 1]

    def new_recv(n=1):
        counts[1] += n
        return recv_sem.at[counts[1] - 1] if n == 1 else counts[1] - n

    def at(kt, kh):
        return (d, lax.rem(t + kt, T), lax.rem(h + kh, H))

    def copy(src, dst, device, s_sem, r_sem):
        return pltpu.make_async_remote_copy(
            src_ref=src, dst_ref=dst, send_sem=s_sem, recv_sem=r_sem,
            device_id=device, device_id_type=MESH,
        )

    def go(*what):
        copy(*what).start()

    pair_dev, across_dev = (pair, t, h), (across, t, h)
    left = []

    def got(name, ref, r_sem):
        with scope(name):
            copy(ref, ref, pair_dev, send_sem.at[0], r_sem).wait_recv()

    def left_all(ref, s_sem):
        left.append((ref, s_sem))

    def scope(name):
        return jax.named_scope(name)

    peers = [(kt, kh) for kh in [*range(H // 2, H), *range(1, H // 2), 0] for kt in range(T) if kt or kh]
    shard = w_b.shape[0]

    def local_copy(k, src, dst):
        made = pltpu.make_async_copy(src, dst, local_sem.at[k])
        made.start()
        return made

    def other(i):
        where = 0
        for hh in range(H):
            where = where + jnp.where(h == hh, hh ^ (i + 1), 0)
        return where

    nearest = [other(i) for i in range(H - 1)]

    class Along:
        def __init__(self, s_sem):
            self.s, self.base = s_sem, new_recv(H - 1)

        def send(self, i, src, dst):
            to = nearest[i]
            r = recv_sem.at[self.base + lax.rem(to - h + H, H) - 1]
            go(src, dst, (d, t, to), self.s, r)

        def wait(self, name, i, ref):
            got(name, ref, recv_sem.at[self.base + lax.rem(h - nearest[i] + H, H) - 1])

    own_l = local_copy(0, latent, lbuf.at[t, h])
    cb[...] = jnp.zeros(cb.shape, BF16)
    barrier = pltpu.get_barrier_semaphore()
    for kt, kh in peers:
        pl.semaphore_signal(barrier, inc=1, device_id=at(kt, kh), device_id_type=MESH)
    pl.semaphore_signal(barrier, inc=1, device_id=pair_dev, device_id_type=MESH)
    pl.semaphore_signal(barrier, inc=1, device_id=across_dev, device_id_type=MESH)
    own_w = local_copy(2, w_b, wb.at[pl.ds(pl.multiple_of((t * H + h) * shard, shard), shard)])
    own_g = [
        local_copy(5, gain_in, gall.at[h, pl.ds(0, 1)]),
        local_copy(6, shift_in, gall.at[h, pl.ds(1, 1)]),
        local_copy(7, gain_b_in, gain_b), local_copy(8, shift_b_in, shift_b),
    ]
    own_up = local_copy(1, up_w, upw.at[pl.ds(pl.multiple_of(h * CH, CH), CH)])
    own_c = local_copy(4, cot, cb.at[pl.ds(0, F), pl.ds(1, R)])
    own_wl = local_copy(3, w_l, wl)
    own_l.wait()
    with scope("w_barrier"):
        pl.semaphore_wait(barrier, N + 1)

    yes = at(1, 0)
    w_half = shard // 2
    half_cols = pl.ds(pl.multiple_of(half * (C2 // 2), C2 // 2), C2 // 2)

    def w_piece(gt, gh, piece_side):
        start = pl.multiple_of((gt * H + gh) * shard + piece_side * w_half, w_half)
        return wb.at[pl.ds(start, w_half), half_cols]

    def w_both(gt, gh):
        return wb.at[pl.ds(pl.multiple_of((gt * H + gh) * shard, shard), shard), half_cols]

    up_rows, up_cols = CH // T, 2 * C2

    def up_piece(gt, gh, n=1):
        first = 2 * half + (side if n == 1 else 0)
        return upw.at[
            pl.ds(pl.multiple_of(gh * CH + gt * up_rows, up_rows), up_rows),
            pl.ds(pl.multiple_of(first * up_cols, up_cols), n * up_cols),
        ]

    mine = lbuf.at[t, h]
    lz = Along(new_send())
    ly_s, ly_r = new_send(), new_recv()
    for i in range(H - 1):
        lz.send(i, mine, mine)
    go(mine, mine, yes, ly_s, ly_r)
    own_w.wait()
    w_s = new_send()
    w_mine = w_piece(t, h, side)
    wy_r = [new_recv() for _ in range(H)]
    go(w_both(t, h), w_both(t, h), yes, w_s, wy_r[H - 1])
    for made in own_g:
        made.wait()
    gain_s, gain_r = new_send(), new_recv()
    for kh in range(1, H):
        go(gall.at[h], gall.at[h], at(0, kh), gain_s, gain_r)
    own_up.wait()
    u_s = new_send()
    uz = Along(u_s)

    def up_send(core):
        @pl.when(half == core)
        def _():
            for i in range(H - 1):
                uz.send(i, up_piece(t, h), up_piece(t, h))

    up_send(0)
    abuf[...] = jnp.zeros(abuf.shape, BF16)
    ab[...] = jnp.zeros(ab.shape, BF16)
    for i in range(H - 1):
        if i == 2:
            up_send(1)
        piece = lbuf.at[t, nearest[i]]
        lz.wait("w_lz", i, piece)
        go(piece, piece, yes, ly_s, ly_r)
    left_all(lbuf.at[0, pl.ds(0, H - 1)], lz.s)
    left_all(lbuf.at[0], ly_s)
    left_all(gall.at[pl.ds(0, H - 1)], gain_s)

    wx_r, wx_at = [], []
    wpair_r = new_recv()

    def w_across(gt, gh):
        wx_r.append(new_recv())
        wx_at.append((gt, gh))
        go(w_piece(gt, gh, side), w_piece(gt, gh, side), across_dev, w_s, wx_r[-1])

    def w_pair(k):
        gt, gh = wx_at[k]
        got("w_wx", w_piece(gt, gh, 1 - side), wx_r[k])
        go(w_both(gt, gh), w_both(gt, gh), pair_dev, w_s, wpair_r)


    def halo(buffer, f0, f_two, two_at, step):
        made = []
        ok_t_send = (t < T - 1) if step == 1 else (t > 0)
        ok_t_recv = (t > 0) if step == 1 else (t < T - 1)
        kt = step % T

        def part_of(fs, n_f, r0, n_r):
            return buffer.at[pl.ds(fs, n_f), pl.ds(r0, n_r)]

        for kt_, kh_, ok_s, ok_r, src, dst in (
            (kt, 0, ok_t_send, ok_t_recv, part_of(f_two, 2, 1, R), part_of(two_at, 2, 1, R)),
            (0, 1, h < H - 1, h > 0, part_of(f0, F, R, 1), part_of(f0, F, 0, 1)),
            (0, H - 1, h > 0, h < H - 1, part_of(f0, F, 1, 1), part_of(f0, F, R + 1, 1)),
            (kt, 1, ok_t_send & (h < H - 1), ok_t_recv & (h > 0),
             part_of(f_two, 2, R, 1), part_of(two_at, 2, 0, 1)),
            (kt, H - 1, ok_t_send & (h > 0), ok_t_recv & (h < H - 1),
             part_of(f_two, 2, 1, 1), part_of(two_at, 2, R + 1, 1)),
        ):
            c = copy(src, dst, at(kt_, kh_), new_send(), new_recv())
            pl.when(ok_s)(c.start)
            made.append((c, ok_s, ok_r))
        return made

    uy_r = [new_recv() for _ in range(H - 1)]
    ux_r = [new_recv()]
    ux_last_r = [new_recv() for _ in range(H - 1)]
    upair_r = new_recv()

    def up_height(i):
        piece = up_piece(t, nearest[i])
        uz.wait("w_uz", i, piece)
        go(piece, piece, yes, u_s, uy_r[i])
        go(piece, piece, across_dev, u_s, ux_r[0])

    up_height(0)
    got("w_ly", lbuf.at[0], ly_r)
    got("w_gain", gall.at[pl.ds(0, H - 1)], gain_r)
    up_height(1)
    wz = Along(w_s)
    own_c.wait()
    wz.send(0, w_mine, w_mine)
    wz.send(1, w_mine, w_mine)

    per_l = H * CH // GROUPS
    cells_l = FL * Rl * Cl
    count_l = cells_l * per_l
    xs, rows = [], []
    for k in range(H):
        x = lbuf[:, k].astype(F32).reshape(cells_l, CH)
        rows += [jnp.sum(x, 0, keepdims=True), jnp.sum(x * x, 0, keepdims=True)]
    total = over_groups(jnp.concatenate(rows, 0), per_l) / count_l
    for k in range(H):
        mean = total[2 * k : 2 * k + 1]
        inv = lax.rsqrt(total[2 * k + 1 : 2 * k + 2] - mean * mean + epsilon)
        x = lbuf[:, k].astype(F32).reshape(cells_l, CH)
        v = (x - mean) * inv * gall[k, 0:1] + gall[k, 1:2]
        lane = k * CH % U
        abuf[k * CH // U, 2 : 2 + FL, 1 : 1 + Rl, :, lane : lane + CH] = (
            (v * jax.nn.sigmoid(v)).astype(BF16).reshape(FL, Rl, Cl, CH)
        )

    up_height(2)

    own_wl.wait()

    parts_of = 2
    some = FL // parts_of

    def window(m, chunk, tap):
        lag, dr = tap // 9, (tap // 3) % 3
        return abuf[chunk, pl.ds(lag + m * some, some), pl.ds(dr, Rl)].reshape(some * Rl * Cl, U)

    def w_rows(chunk, tap):
        return wl[pl.ds(pl.multiple_of((tap * T + chunk - 27 * t) * U, U), U), :]

    with scope("c_latent"):
        sums = [None] * parts_of
        for g in range(4):
            tap = jnp.where(t == 0, 3 * g, 15 + 3 * g)
            for chunk in range(T):
                k3 = jnp.concatenate([w_rows(chunk, tap + dc) for dc in range(3)], 1)
                for m in range(parts_of):
                    term = jnp.dot(window(m, chunk, tap), k3, preferred_element_type=F32)
                    sums[m] = term if sums[m] is None else sums[m] + term
        alone = jnp.where(t == 0, 12, 14)
        k2 = jnp.concatenate([w_rows(t, alone), w_rows(t, 13)], 1)
        mixed = []
        for m in range(parts_of):
            both = jnp.dot(window(m, t, alone), k2, preferred_element_type=F32)
            lone = both[:, :CH] + jnp.dot(
                window(m, 1 - t, alone), w_rows(1 - t, alone), preferred_element_type=F32
            )
            first = sums[m][:, :CH] + jnp.where(t == 0, lone, 0.0)
            last = sums[m][:, 2 * CH :] + jnp.where(t == 0, 0.0, lone)
            mixed.append(
                column_shift(first, Cl, 1) + sums[m][:, CH : 2 * CH] + both[:, CH:]
                + column_shift(last, Cl, -1)
            )
        mixed = jnp.concatenate(mixed, 0)
        partf[...] = mixed.reshape(FL, Rl, Cl, CH)
        partf[pl.ds(t * Fl, Fl)] += lbuf[t, h].astype(F32)
        part[...] = partf[...].astype(BF16)
    p_s, p_r = new_send(), new_recv()
    for kt, kh in peers:
        dev = at(kt, kh)
        go(part.at[pl.ds(dev[1] * Fl, Fl), pl.ds(dev[2] * band, band)],
           parts_in.at[kt * H + kh], dev, p_s, p_r)
    wz.send(2, w_mine, w_mine)

    def w_height(i):
        piece = w_piece(t, nearest[i], side)
        wz.wait("w_wz", i, piece)
        go(piece, piece, yes, w_s, wy_r[i])
        w_across(t, nearest[i])

    piece = up_piece(1 - t, nearest[0])
    got("w_uy", piece, uy_r[0])
    go(piece, piece, across_dev, u_s, ux_last_r[0])
    piece = up_piece(1 - t, nearest[1])
    got("w_uy", piece, uy_r[1])
    go(piece, piece, across_dev, u_s, ux_last_r[1])
    piece = up_piece(1 - t, nearest[2])
    got("w_uy", piece, uy_r[2])
    go(piece, piece, across_dev, u_s, ux_last_r[2])
    w_height(0)
    cot_halo = halo(cb, 0, 0, F, -1)
    got("w_ux", upw.at[pl.ds(0, (H - 1) * up_rows), pl.ds(0, up_cols)], ux_r[0])
    for i in range(H - 1):
        piece = up_piece(t, nearest[i], 2)
        go(piece, piece, pair_dev, u_s, upair_r)
    got("w_wy0", w_both(1 - t, h), wy_r[H - 1])
    go(w_both(1 - t, h), w_both(1 - t, h), pair_dev, w_s, wpair_r)
    for i in range(H - 1):
        got("w_ux", up_piece(1 - t, nearest[i]), ux_last_r[i])
        piece = up_piece(1 - t, nearest[i], 2)
        go(piece, piece, pair_dev, u_s, upair_r)
    w_height(1)
    got("w_upair", upw.at[pl.ds(0, (H - 1) * CH), pl.ds(0, 4 * C2)], upair_r)
    got("w_parts", parts_in.at[pl.ds(1, N - 1)], p_r)
    left_all(parts_in.at[pl.ds(1, N - 1)], p_s)
    left_all(upw.at[pl.ds(0, (H - 1) * CH)], u_s)

    cells_b = Fl * band * Cl
    with scope("c_up"):
        parts_own = partf[pl.ds(t * Fl, Fl), pl.ds(h * band, band)]
        expanded = jnp.zeros((cells_b, 8 * C2), F32)
        for kh in range(H):
            value = parts_own if kh == 0 else parts_in[kh].astype(F32)
            for kt in range(1, T):
                value = value + parts_in[kt * H + kh].astype(F32)
            refined = value.reshape(cells_b, CH).astype(BF16)
            source = lax.rem(h + H - kh, H)
            expanded = expanded + jnp.dot(
                refined, upw[pl.ds(pl.multiple_of(source * CH, CH), CH), :],
                preferred_element_type=F32,
            )
        expanded = expanded.astype(BF16).astype(F32)
        for f in range(Fl):
            for r in range(band):
                for p in range(2):
                    for qq in range(2):
                        for s in range(2):
                            first = (f * band + r) * Cl
                            col = ((p * 2 + qq) * 2 + s) * C2
                            for n in range(C2 // 128):
                                lace[
                                    n, pl.ds(((2 * f + p) * R + 2 * r + qq) * C + s, Cl, stride=2), :
                                ] = expanded[first : first + Cl, col + n * 128 : col + (n + 1) * 128]

        cells = F * R * C
        me = t * H + h
        up = jnp.concatenate([lace[n] for n in range(C2 // 128)], axis=1)
        stat2[me] = side_by_side(jnp.sum(up, 0, keepdims=True), jnp.sum(up * up, 0, keepdims=True))
        ub[2 : 2 + F, 1 : 1 + R] = up.astype(BF16).reshape(F, R, C, C2)
    s2_s, s2_r = new_send(), new_recv()
    for kt, kh in peers:
        go(stat2.at[me], stat2.at[me], at(kt, kh), s2_s, s2_r)
    left_all(stat2.at[pl.ds(0, N - 1)], s2_s)
    up_halo = halo(ub, 2, F, 0, 1)

    w_height(2)
    got("w_wy", w_piece(1 - t, nearest[0], side), wy_r[0])
    w_across(1 - t, nearest[0])
    with scope("w_cothalo"):
        for made, _, ok in cot_halo:
            pl.when(ok)(made.wait_recv)
    wide = cb[0:F].astype(F32).reshape(F * (R + 2) * C, C2)
    cot3[:, :, :, 0:C2] = column_shift(wide, C, -1).astype(BF16).reshape(F, R + 2, C, C2)
    cot3[:, :, :, C2 : 2 * C2] = cb[0:F]
    cot3[:, :, :, 2 * C2 :] = column_shift(wide, C, 1).astype(BF16).reshape(F, R + 2, C, C2)

    got("w_wy", w_piece(1 - t, nearest[1], side), wy_r[1])
    w_across(1 - t, nearest[1])
    got("w_s2", stat2.at[pl.ds(0, N - 1)], s2_r)
    per_b = C2 // GROUPS
    count_b = cells * per_b * N
    total = stat2[0]
    for k in range(1, N):
        total = total + stat2[k]
    total = over_groups(jnp.concatenate([total[:, :C2], total[:, C2:]], 0), per_b) / count_b
    mean_b = total[0:1]
    inv_b = lax.rsqrt(total[1:2] - mean_b * mean_b + epsilon)

    def activate(values):
        normed = (values - mean_b) * inv_b * gain_b[...] + shift_b[...]
        return (normed * jax.nn.sigmoid(normed)).astype(BF16)

    with scope("c_gw"):
        own = activate(ub[2 : 2 + F, 1 : 1 + R].astype(F32).reshape(cells, C2))
        ab[2 : 2 + F, 1 : 1 + R] = own.reshape(F, R, C, C2)
        def taps_of(i):
            dr = jnp.where(t == 0, 2 - i, i)
            term = lax.dot_general(
                own, cot3[:, pl.ds(2 - dr, R)].reshape(cells, 3 * C2),
                (((0,), (0,)), ((), ())), preferred_element_type=F32,
            )
            for dc in range(3):
                gw[pl.ds(pl.multiple_of((dr * 3 + dc) * C2, C2), C2), :] = (
                    term[:, dc * C2 : (dc + 1) * C2].astype(BF16)
                )

        taps_of(0)
        taps_of(1)
    out_rows = 9 * C2 // N
    y_rows = out_rows * H

    cut_rows = out_rows // CUTS

    def cut(c):
        return pl.ds(c * cut_rows, cut_rows)

    def g_at(gt, gh, c):
        start = (gt * H + gh) * out_rows + c * cut_rows
        return pl.ds(pl.multiple_of(start, cut_rows), cut_rows)

    def g_rows(gt, gh, c):
        return gw.at[g_at(gt, gh, c)]

    def ahead(kh):
        return lax.rem(h + kh, H)

    order = [*range(H // 2, H), *range(1, H // 2), 0]
    gy_s, gz_s, gz_r = new_send(), new_send(), new_recv()
    gy_r = {(kh, c): new_recv() for kh in order for c in range(CUTS) if (kh, c) != (1, 0)}
    first_cut = (1, 0)
    steps = [(kh, c) for kh in order for c in range(CUTS) if (kh, c) != first_cut]
    for kh, c in steps:
        if (kh, c) != (0, 0):
            go(g_rows(1 - t, ahead(kh), c), gy.at[kh, cut(c)], yes, gy_s, gy_r[kh, c])
    zf_s, zf_r = new_send(), new_recv()
    go(g_rows(1 - t, ahead(1), 0), gf.at[1], at(0, 1), zf_s, zf_r)
    with scope("c_gw2"):
        taps_of(2)
    go(g_rows(t, ahead(1), 0), gf.at[0], at(0, 1), zf_s, zf_r)
    left_all(gw.at[pl.ds(0, len(steps) * cut_rows)], gy_s)
    left_all(gf, zf_s)

    def g_join():
        got("w_gf", gf, zf_r)
        total = gw[g_at(1 - t, h, 0), :].astype(F32) + gf[1].astype(F32)
        gs[0, :cut_rows] = total.astype(BF16)
        go(gs.at[0, cut(0)], gy.at[0, cut(0)], yes, gy_s, gy_r[0, 0])

    with scope("w_uphalo"):
        for made, _, ok in up_halo:
            pl.when(ok)(made.wait_recv)
    with scope("c_halo"):
        for rows_at, n_rows, ok in ((0, 1, h > 0), (R + 1, 1, h < H - 1)):
            @pl.when(ok)
            def _():
                v = ub[2 : 2 + F, rows_at : rows_at + n_rows].astype(F32).reshape(F * n_rows * C, C2)
                ab[2 : 2 + F, rows_at : rows_at + n_rows] = activate(v).reshape(F, n_rows, C, C2)
        for rows_at, n_rows, ok in (
            (1, R, t > 0), (0, 1, (t > 0) & (h > 0)), (R + 1, 1, (t > 0) & (h < H - 1))
        ):
            @pl.when(ok)
            def _():
                v = ub[0:2, rows_at : rows_at + n_rows].astype(F32).reshape(2 * n_rows * C, C2)
                ab[0:2, rows_at : rows_at + n_rows] = activate(v).reshape(2, n_rows, C, C2)

    def g_on(kh, c):
        got("w_gy", gy.at[kh, cut(c)], gy_r[kh, c])
        total = gy[kh, c * cut_rows : (c + 1) * cut_rows].astype(F32)
        total = total + gw[g_at(t, ahead(kh), c), :].astype(F32)
        if (kh, c) == (0, 0):
            total = total + gf[0].astype(F32)
        if kh == 0:
            grad_w[c * cut_rows : (c + 1) * cut_rows] = total
        else:
            gs[kh, c * cut_rows : (c + 1) * cut_rows] = total.astype(BF16)
            go(gs.at[kh, cut(c)], gz.at[kh, cut(c)], at(0, kh), gz_s, gz_r)

    got("w_wy", w_piece(1 - t, nearest[2], side), wy_r[2])
    w_across(1 - t, nearest[2])
    w_pair(0)
    w_pair(1)
    g_on(*steps[0])
    w_pair(2)
    g_on(*steps[1])
    g_join()
    w_pair(3)
    w_pair(4)
    w_pair(5)
    left_all(gw.at[pl.ds(0, (len(steps) - CUTS) * cut_rows)], gz_s)
    got("w_wpair", wb.at[pl.ds(0, (N - 1) * shard), pl.ds(0, C2 // 2)], wpair_r)
    left_all(wb.at[pl.ds(0, (2 * H + 3 * N - 4) * w_half // 2)], w_s)

    with scope("c_gradtap"):
        sums = {}
        for j in range(9):
            lag, dr = j // 3, j % 3
            win = cb[2 - lag : 2 - lag + F, 2 - dr : 2 - dr + R].reshape(cells, C2)
            for dc in range(3):
                term = lax.dot_general(
                    win, wb[(j * 3 + dc) * C2 : (j * 3 + dc + 1) * C2, :],
                    (((1,), (1,)), ((), ())), preferred_element_type=F32,
                )
                key = (dc, j % 2 if dc == 1 else 0)
                sums[key] = sums[key] + term if key in sums else term
        grad_active = (
            column_shift(sums[0, 0], C, -1) + sums[1, 0] + sums[1, 1]
            + column_shift(sums[2, 0], C, 1)
        )
    standard = (ub[2 : 2 + F, 1 : 1 + R].astype(F32).reshape(cells, C2) - mean_b) * inv_b
    std[...] = standard
    normed = standard * gain_b[...] + shift_b[...]
    sigmoid = jax.nn.sigmoid(normed)
    grad_normed = grad_active * sigmoid * (1.0 + normed * (1.0 - sigmoid))
    stat3[me] = side_by_side(
        jnp.sum(grad_normed * standard, 0, keepdims=True), jnp.sum(grad_normed, 0, keepdims=True)
    )
    s3_s, s3_r = new_send(), new_recv()
    for kt, kh in peers:
        go(stat3.at[me], stat3.at[me], at(kt, kh), s3_s, s3_r)
    left_all(stat3.at[pl.ds(0, N - 1)], s3_s)
    tmp[...] = grad_normed * gain_b[...]
    for step in steps[2:5]:
        g_on(*step)

    some = F // 2
    n = some * R * C
    for m in range(2):
        with scope("c_tap"):
            wide = None
            for j in range(9):
                lag, dr = j // 3, j % 3
                k3 = jnp.concatenate(
                    [wb[(j * 3 + dc) * C2 : (j * 3 + dc + 1) * C2, :] for dc in range(3)], 1
                )
                win = ab[lag + m * some : lag + (m + 1) * some, dr : dr + R].reshape(n, C2)
                term = jnp.dot(win, k3, preferred_element_type=F32)
                wide = term if wide is None else wide + term
            decoded[m * some : (m + 1) * some] = (
                (column_shift(wide[:, :C2], C, 1) + wide[:, C2 : 2 * C2]
                 + column_shift(wide[:, 2 * C2 :], C, -1)
                 + ub[2 + m * some : 2 + (m + 1) * some, 1 : 1 + R].astype(F32).reshape(n, C2))
                .astype(BF16).reshape(some, R, C, C2)
            )
        for step in steps[5:5] if m == 0 else steps[5 : -CUTS]:
            g_on(*step)

    got("w_s3", stat3.at[pl.ds(0, N - 1)], s3_r)
    total = stat3[0]
    for k in range(1, N):
        total = total + stat3[k]
    total = two_rows(total[:, :C2], total[:, C2:])
    grad_gs[...] = total
    means = over_groups(total * gain_b[...], per_b) / count_b
    corrected = (tmp[...] - means[1:2] - std[...] * means[0:1]) * inv_b
    grad_up[...] = (
        cb[0:F, 1 : 1 + R].astype(F32).reshape(cells, C2) + corrected
    ).astype(BF16).reshape(F, R, C, C2)

    for step in steps[-CUTS:]:
        g_on(*step)
    got("w_gz", gw.at[pl.ds(0, (len(steps) - CUTS) * cut_rows)], gz_r)
    for c in range(CUTS):
        rows = slice(c * cut_rows, (c + 1) * cut_rows)
        result = grad_w[rows]
        for kh in range(1, H):
            if (kh, c) != first_cut:
                result = result + gz[kh, rows].astype(F32)
        grad_w[rows] = result

    with scope("w_send"):
        for ref, s_sem in left:
            copy(ref, ref, pair_dev, s_sem, recv_sem.at[0]).wait_send()
        for made, ok, _ in cot_halo + up_halo:
            pl.when(ok)(made.wait_send)
    assert counts == [n_send, n_recv], counts


def finish_kernel(decoded, grad_up, grad_w, grad_gs, out_d, out_u, out_w, out_g, out_s, sems):
    moves = [
        pltpu.make_async_copy(src, dst, sems.at[k])
        for k, (src, dst) in enumerate((
            (decoded, out_d), (grad_up, out_u), (grad_w, out_w),
            (grad_gs.at[pl.ds(0, 1)], out_g), (grad_gs.at[pl.ds(1, 1)], out_s),
        ))
    ]
    for move in moves:
        move.start()
    for move in moves:
        move.wait()


def stay(array):
    return pltpu.with_memory_space_constraint(array, pltpu.HBM)


def local_block(shape, *args):
    (latent, gain_l, shift_l, w_l, up_w, gain_b, shift_b, w_b, cot) = args
    T, H = shape["tm"], shape["height"]
    Fl, Rl, Cl, CH = latent.shape
    F, R, C, C2 = cot.shape
    N = T * H
    U = H * CH // T
    fits = (
        shape["dp"] % 4 == 0 and T == 2 and H == 4
        and CH % 128 == 0 and U % CH == 0
        and w_b.shape[0] % 32 == 0 and (CH // T) % 16 == 0
        and (9 * C2) % (16 * CUTS * N) == 0 and C2 % 256 == 0
        and Cl % 16 == 0 and w_l.shape[0] == 27 * U and F >= 2
    )
    if not fits:
        return local(*args)
    sizes = (T, H, Fl, Rl, Cl, CH, C2, F, R, C)
    n_send = 21
    n_recv = 19 + 5 * (H - 1) + (1 + CUTS) * H + N - 2
    FL = T * Fl
    band = Rl // H
    cells = F * R * C
    out_rows = 9 * C2 // N
    vmem = pl.BlockSpec(memory_space=pltpu.VMEM)
    hbm = pl.BlockSpec(memory_space=pltpu.HBM)
    flops = 2 * (FL * Rl * Cl * w_l.size + 2 * cells * 27 * C2 * C2 + cells * 9 * C2 * C2)
    outs = pl.pallas_call(
        functools.partial(block_kernel, sizes, n_send, n_recv),
        out_shape=(
            jax.ShapeDtypeStruct(cot.shape, BF16),
            jax.ShapeDtypeStruct(cot.shape, BF16),
            jax.ShapeDtypeStruct((out_rows, C2), F32),
            jax.ShapeDtypeStruct((8, C2), F32),
        ),
        in_specs=[hbm] * 9,
        out_specs=(vmem,) * 4,
        scratch_shapes=[
            pltpu.VMEM((T, H, Fl, Rl, Cl, CH), BF16),
            pltpu.VMEM((H, 2, CH), F32),
            pltpu.VMEM((1, C2), F32),
            pltpu.VMEM((1, C2), F32),
            pltpu.VMEM(w_l.shape, BF16),
            pltpu.VMEM((T, FL + 2, Rl + 2, Cl, U), BF16),
            pltpu.VMEM((FL, Rl, Cl, CH), BF16),
            pltpu.VMEM((FL, Rl, Cl, CH), F32),
            pltpu.VMEM((N, Fl, band, Cl, CH), BF16),
            pltpu.VMEM((N, 1, 2 * C2), F32),
            pltpu.VMEM((N, 1, 2 * C2), F32),
            pltpu.VMEM((H * CH, 8 * C2), BF16),
            pltpu.VMEM((27 * C2, C2), BF16),
            pltpu.VMEM((F + 2, R + 2, C, C2), BF16),
            pltpu.VMEM((cells, C2), F32),
            pltpu.VMEM((F + 2, R + 2, C, C2), BF16),
            pltpu.VMEM((F + 2, R + 2, C, C2), BF16),
            pltpu.VMEM((F, R + 2, C, 3 * C2), BF16),
            pltpu.VMEM((9 * C2, C2), BF16),
            pltpu.VMEM((H, out_rows, C2), BF16),
            pltpu.VMEM((2, out_rows // CUTS, C2), BF16),
            pltpu.VMEM((H, out_rows, C2), BF16),
            pltpu.VMEM((H, out_rows, C2), BF16),
            pltpu.VMEM((cells, C2), F32),
            pltpu.VMEM((C2 // 128, cells, 128), F32),
            pltpu.SemaphoreType.DMA((n_send,)),
            pltpu.SemaphoreType.DMA((n_recv,)),
            pltpu.SemaphoreType.DMA((9,)),
        ],
        compiler_params=pltpu.CompilerParams(
            collective_id=0, has_side_effects=True, vmem_limit_bytes=VMEM_LIMIT
        ),
        cost_estimate=pl.CostEstimate(flops=flops, bytes_accessed=1 << 23, transcendentals=0),
    )(
        stay(latent), stay(gain_l.reshape(1, -1)), stay(shift_l.reshape(1, -1)), stay(w_l), stay(up_w),
        stay(gain_b.reshape(1, -1)), stay(shift_b.reshape(1, -1)), stay(w_b), stay(cot),
    )
    row = jax.ShapeDtypeStruct((1, C2), F32)
    done = pl.pallas_call(
        finish_kernel,
        out_shape=tuple(jax.ShapeDtypeStruct(a.shape, a.dtype) for a in outs[:3]) + (row, row),
        in_specs=[vmem] * 4,
        out_specs=(hbm,) * 5,
        scratch_shapes=[pltpu.SemaphoreType.DMA((5,))],
        compiler_params=pltpu.CompilerParams(vmem_limit_bytes=1 << 20),
        cost_estimate=pl.CostEstimate(flops=0, bytes_accessed=1 << 20, transcendentals=0),
    )(*outs)
    return done[0], done[1], done[2], done[3].reshape(C2), done[4].reshape(C2)


def solution(mesh):
    return jax.shard_map(
        functools.partial(local_block, dict(mesh.shape)),
        mesh=mesh,
        in_specs=(
            P(("dp", "tm"), None, None, "height"),
            P("height"),
            P("height"),
            P("tm", "height"),
            P("height", None),
            P(),
            P(),
            P(("tm", "height"), None),
            P(("dp", "tm"), "height", None, None),
        ),
        out_specs=(
            P(("dp", "tm"), "height", None, None),
            P(("dp", "tm"), "height", None, None),
            P(("dp", "tm", "height"), None),
            P("dp"),
            P("dp"),
        ),
        check_vma=False,
    )
```
